128 devices in a mesh: tp: 2 (over core), dp: 64 (over z, y, x).
Axes of the slice: x: 4, y: 4, z: 4, core: 2. Of those that a mesh axis runs over, the one named last changes fastest.
Arguments:
- x_saved: bfloat16 [64, 2048, 1024], P('dp', 'tp')
- dy_out: bfloat16 [64, 2048, 1024], P('dp', 'tp')
- ln_params: float32 [4, 1024], replicated
- w_qkv: bfloat16 [1024, 16, 3, 64], P(None, 'tp')
- w_out: bfloat16 [1024, 1024], P('tp')
- w_up: bfloat16 [1024, 4096], P(None, 'tp')
- w_down: bfloat16 [4096, 1024], P('tp')
Outputs:
- output 1: bfloat16 [64, 2048, 1024], P('dp', 'tp')
- output 2: float32 [4, 1024], replicated
- output 3: float32 [1024, 16, 3, 64], P('dp', 'tp')
- output 4: float32 [1024, 1024], P(('tp', 'dp'))
- output 5: float32 [1024, 4096], P('dp', 'tp')
- output 6: float32 [4096, 1024], P(('tp', 'dp'))
All inputs are finite; a program needn't handle non-finite values.
Results may differ from the reference program's by a relative error of at most 0.00983313.
Values are sent between devices in bfloat16 or wider.
A program may use at most 1 GiB of HBM per device.

```python
import jax
import jax.numpy as jnp
from jax import lax

NUM_SEQS = 64
SEQ_LEN = 2048
D_MODEL = 1024
NUM_HEADS = 16
KV_HEADS = 16
HEAD_DIM = 64
FF_DIM = 4096
Q_PER_GROUP = NUM_HEADS // KV_HEADS
NORM_EPS = 1e-5
ROPE_BASE = 10000.0


def layer_norm(x_rows, norm_gain, norm_shift):
    row_mean = jnp.mean(x_rows, axis=-1, keepdims=True)
    centered = x_rows - row_mean
    row_var = jnp.mean(centered * centered, axis=-1, keepdims=True)
    return (centered * lax.rsqrt(row_var + NORM_EPS) * norm_gain + norm_shift).astype(jnp.bfloat16)


def rope_tables(positions):
    half_dim = HEAD_DIM // 2
    inv_freq = ROPE_BASE ** (-2.0 * jnp.arange(half_dim, dtype=jnp.float32) / HEAD_DIM)
    angles = positions.astype(jnp.float32)[:, None] * inv_freq[None, :]
    return jnp.cos(angles), jnp.sin(angles)


def apply_rope(tensor, cos_t, sin_t):
    half_dim = tensor.shape[-1] // 2
    t_f32 = tensor.astype(jnp.float32)
    lo_half = t_f32[..., :half_dim]
    hi_half = t_f32[..., half_dim:]
    return jnp.concatenate([lo_half * cos_t - hi_half * sin_t, hi_half * cos_t + lo_half * sin_t], axis=-1).astype(jnp.bfloat16)


def attention(qkv_proj):
    positions = jnp.arange(SEQ_LEN)
    cos_t, sin_t = rope_tables(positions)
    rotated = apply_rope(qkv_proj[:, :, :Q_PER_GROUP + 1, :], cos_t[:, None, None, :], sin_t[:, None, None, :])
    query_rot = rotated[:, :, :Q_PER_GROUP, :]
    key_rot = rotated[:, :, Q_PER_GROUP, :]
    values = qkv_proj[:, :, Q_PER_GROUP + 1, :]
    scores = jnp.einsum('tgqh,sgh->gqts', query_rot.astype(jnp.float32), key_rot.astype(jnp.float32)) * (HEAD_DIM ** -0.5)
    causal = positions[:, None] >= positions[None, :]
    attn_probs = jax.nn.softmax(jnp.where(causal, scores, -1e30), axis=-1).astype(jnp.bfloat16)
    return jnp.einsum('gqts,sgh->tgqh', attn_probs.astype(jnp.float32), values.astype(jnp.float32)).astype(jnp.bfloat16)


def layer_forward(x_seq, ln_params, w_qkv, w_out, w_up, w_down):
    x_f32 = x_seq.astype(jnp.float32)
    h_attn = layer_norm(x_f32, ln_params[0], ln_params[1])
    h_mlp = layer_norm(x_f32, ln_params[2], ln_params[3])
    qkv_proj = jnp.dot(h_attn.astype(jnp.float32), w_qkv.reshape(D_MODEL, -1), preferred_element_type=jnp.float32).astype(jnp.bfloat16)
    context = attention(qkv_proj.reshape(SEQ_LEN, KV_HEADS, Q_PER_GROUP + 2, HEAD_DIM))
    attn_out = jnp.dot(context.reshape(SEQ_LEN, NUM_HEADS * HEAD_DIM).astype(jnp.float32), w_out, preferred_element_type=jnp.float32)
    hidden = jnp.dot(h_mlp.astype(jnp.float32), w_up, preferred_element_type=jnp.float32).astype(jnp.bfloat16)
    gelu_out = jax.nn.gelu(hidden.astype(jnp.float32), approximate=False).astype(jnp.bfloat16)
    mlp_out = jnp.dot(gelu_out.astype(jnp.float32), w_down, preferred_element_type=jnp.float32)
    return x_f32 + attn_out + mlp_out


def setup_inputs(seed: int = 0) -> dict:
    key_list = jax.random.split(jax.random.key(seed), 8)
    act_shape = (NUM_SEQS, SEQ_LEN, D_MODEL)
    x_saved = jax.random.normal(key_list[0], act_shape, jnp.float32)
    shared_dir = jax.random.normal(key_list[1], (NUM_SEQS, 1, D_MODEL), jnp.float32)
    dy_out = 0.6 * shared_dir + 0.8 * jax.random.normal(key_list[2], act_shape, jnp.float32)
    ln_base = jnp.array([1.0, 0.0, 1.0, 0.0], jnp.float32)[:, None]
    ln_spread = jnp.array([0.3, 0.5, 0.3, 0.5], jnp.float32)[:, None]
    ln_params = ln_base + ln_spread * jax.random.normal(key_list[3], (4, D_MODEL), jnp.float32)
    w_qkv = jax.random.normal(key_list[4], (D_MODEL, KV_HEADS, Q_PER_GROUP + 2, HEAD_DIM), jnp.float32) * D_MODEL ** -0.5
    w_out = jax.random.normal(key_list[5], (NUM_HEADS * HEAD_DIM, D_MODEL), jnp.float32) * (NUM_HEADS * HEAD_DIM) ** -0.5
    w_up = jax.random.normal(key_list[6], (D_MODEL, FF_DIM), jnp.float32) * D_MODEL ** -0.5
    w_down = jax.random.normal(key_list[7], (FF_DIM, D_MODEL), jnp.float32) * FF_DIM ** -0.5
    return {'x_saved': x_saved.astype(jnp.bfloat16), 'dy_out': dy_out.astype(jnp.bfloat16), 'ln_params': ln_params, 'w_qkv': w_qkv.astype(jnp.bfloat16), 'w_out': w_out.astype(jnp.bfloat16), 'w_up': w_up.astype(jnp.bfloat16), 'w_down': w_down.astype(jnp.bfloat16)}


def reference(x_saved, dy_out, ln_params, w_qkv, w_out, w_up, w_down):
    weights = (ln_params, w_qkv.astype(jnp.float32), w_out.astype(jnp.float32), w_up.astype(jnp.float32), w_down.astype(jnp.float32))

    def seq_step(grad_sums, seq_pair):
        x_seq, dy_seq = seq_pair
        _, pull_back = jax.vjp(layer_forward, x_seq, *weights)
        grads = pull_back(dy_seq.astype(jnp.float32))
        return tuple(grad_total + grad_part for grad_total, grad_part in zip(grad_sums, grads[1:])), grads[0]

    zero_sums = tuple(jnp.zeros_like(weight) for weight in weights)
    grad_sums, grad_x = lax.scan(seq_step, zero_sums, (x_saved, dy_out))
    return (grad_x, grad_sums[0], grad_sums[1], grad_sums[2], grad_sums[3], grad_sums[4])
```

```python
import math

import jax
import jax.numpy as jnp
from jax import lax
from jax.experimental import pallas as pl
from jax.experimental.pallas import tpu as pltpu
from jax.sharding import PartitionSpec as P

NORM_EPS = 1e-5
ROPE_BASE = 10000.0
F32, BF16 = jnp.float32, jnp.bfloat16
LOG2E = math.log2(math.e)
T = 2048
HALF = T // 2
TILE = 256
TT = 512
FC = 512
AXIS_STRIDE = {'z': 16, 'y': 4, 'x': 1}


def dot(a, b):
    return jnp.dot(a, b, preferred_element_type=F32)


def dot_nt(a, b):
    return lax.dot_general(a, b, (((1,), (1,)), ((), ())), preferred_element_type=F32)


def rope_tables():
    inv_freq = ROPE_BASE ** (-2.0 * jnp.arange(32, dtype=F32) / 64)
    angles = inv_freq[:, None] * jnp.arange(T, dtype=F32)[None, :]
    return jnp.cos(angles), jnp.sin(angles)


def normed(x_ref):
    x = x_ref[...].astype(F32)
    centered = x - jnp.mean(x, axis=-1, keepdims=True)
    var = jnp.mean(centered * centered, axis=-1, keepdims=True)
    return centered * lax.rsqrt(var + NORM_EPS)


def token_kernel(x_ref, dy_ref, ln_ref, wqkv_ref, wout_ref, wup_ref, wdown_ref,
                 ha_ref, qkv_ref, dctx_ref, dhm_ref, gup_ref, gdown_ref,
                 hm_s, hm_t, dh_s, up_acc, down_acc, sems):
    step = pl.program_id(0)
    last = pl.num_programs(0) - 1
    width = wup_ref.shape[1]

    def flush(c):
        cols = pl.ds(c * FC, FC)
        return (pltpu.make_async_copy(up_acc.at[:, cols], gup_ref.at[:, cols], sems.at[0, c]),
                pltpu.make_async_copy(down_acc.at[cols, :], gdown_ref.at[cols, :], sems.at[1, c]))

    norm = normed(x_ref)
    hm = (norm * ln_ref[2:3, :] + ln_ref[3:4, :]).astype(BF16)
    ha = (norm * ln_ref[0:1, :] + ln_ref[1:2, :]).astype(BF16)
    hm_s[...] = hm
    hm_t[...] = hm.T
    ha_ref[...] = ha.T

    @pl.when(step == 0)
    def _():
        up_acc[...] = jnp.zeros_like(up_acc)
        down_acc[...] = jnp.zeros_like(down_acc)

    for c in range(width // FC):
        cols = pl.ds(c * FC, FC)
        u = dot(hm_s[...], wup_ref[:, cols]).astype(BF16).astype(F32)
        dg = dot_nt(dy_ref[...], wdown_ref[cols, :]).astype(BF16).astype(F32)
        cdf = 0.5 * (1.0 + lax.erf(u * math.sqrt(0.5)))
        gelu = (u * cdf).astype(BF16)
        pdf = jnp.exp(-0.5 * u * u) * (1.0 / math.sqrt(2.0 * math.pi))
        dh = (dg * (cdf + u * pdf)).astype(BF16)
        dh_s[:, cols] = dh
        down_acc[cols, :] += dot(gelu.T, dy_ref[...])
        up_acc[:, cols] += dot(hm_t[...], dh)

        @pl.when(step == last)
        def _():
            for copy in flush(c):
                copy.start()
    dhm_ref[...] = dot_nt(dh_s[...], wup_ref[...]).astype(BF16)
    qkv_ref[...] = dot(wqkv_ref[...], ha_ref[...]).astype(BF16)
    dctx_ref[...] = dot_nt(wout_ref[...], dy_ref[...]).astype(BF16)

    @pl.when(step == last)
    def _():
        for c in range(width // FC):
            for copy in flush(c):
                copy.wait()


def token_part(x, dy, ln, wqkv_t, wout, wup, wdown):
    D = x.shape[1]
    width = wup.shape[1]
    whole = lambda a: pl.BlockSpec(a.shape, lambda i: (0, 0), pipeline_mode=pl.Buffered(1))
    tok = pl.BlockSpec((TT, D), lambda i: (i, 0))
    col = lambda n: pl.BlockSpec((n, TT), lambda i: (0, i))
    S = jax.ShapeDtypeStruct
    return pl.pallas_call(
        token_kernel,
        grid=(T // TT,),
        in_specs=[tok, tok] + [whole(a) for a in (ln, wqkv_t, wout, wup, wdown)],
        out_specs=[col(D), col(wqkv_t.shape[0]), col(wout.shape[0]), tok, pl.BlockSpec(memory_space=pl.ANY), pl.BlockSpec(memory_space=pl.ANY)],
        out_shape=[S((D, T), BF16), S((wqkv_t.shape[0], T), BF16), S((wout.shape[0], T), BF16), S((T, D), BF16),
                   S((D, width), F32), S((width, D), F32)],
        scratch_shapes=[pltpu.VMEM((TT, D), BF16), pltpu.VMEM((D, TT), BF16), pltpu.VMEM((TT, width), BF16),
                        pltpu.VMEM((D, width), F32), pltpu.VMEM((width, D), F32), pltpu.SemaphoreType.DMA((2, width // FC))],
        compiler_params=pltpu.CompilerParams(dimension_semantics=("arbitrary",), vmem_limit_bytes=63 << 20),
        cost_estimate=pl.CostEstimate(flops=52 * 10**9, bytes_accessed=60 << 20, transcendentals=2 * T * width),
        name="token_part",
    )(x, dy, ln, wqkv_t, wout, wup, wdown)


def attention_kernel(qkv_ref, dctx_ref, cos_ref, sin_ref, dqkv_ref, ctx_ref,
                     q_t, k_t, q_n, k_n, v_n, do_n, p_s, dp_s, dk_acc, dv_acc):
    step = pl.program_id(1)

    @pl.when(step == 0)
    def _():
        for t0 in range(0, T, TILE):
            cols = pl.ds(t0, TILE)
            cos, sin = cos_ref[:, cols], sin_ref[:, cols]
            for head in range(2):
                base = head * 192
                for slot, ref, factor in ((0, q_t, 0.125), (1, k_t, 1.0)):
                    lo = qkv_ref[pl.ds(base + slot * 64, 32), cols].astype(F32)
                    hi = qkv_ref[pl.ds(base + slot * 64 + 32, 32), cols].astype(F32)
                    rot = jnp.concatenate([lo * cos - hi * sin, hi * cos + lo * sin], axis=0).astype(BF16)
                    if factor != 1.0:
                        rot = rot * jnp.asarray(factor, BF16)
                    ref[pl.ds(head * 64, 64), cols] = rot
            q_n[cols, :] = q_t[:, cols].T
            k_n[cols, :] = k_t[:, cols].T
            v_pair = jnp.concatenate([qkv_ref[pl.ds(128, 64), cols], qkv_ref[pl.ds(320, 64), cols]], axis=0)
            v_n[cols, :] = v_pair.T
            do_n[cols, :] = dctx_ref[:, cols].T

    lane = lax.broadcasted_iota(jnp.int32, (TILE, 128), 1)

    def split_lanes(x):
        zero = jnp.zeros_like(x)
        return jnp.concatenate([jnp.where(lane < 64, x, zero), jnp.where(lane < 64, zero, x)], axis=0)

    def split_rows(x):
        zero = jnp.zeros((64, TILE), x.dtype)
        return jnp.concatenate([jnp.concatenate([x[:64], zero], axis=1), jnp.concatenate([zero, x[64:]], axis=1)], axis=0)

    def fold_rows(x, op):
        parts = [x[r * 8:(r + 1) * 8] for r in range(TILE // 8)]
        while len(parts) > 1:
            parts = [op(a, b) for a, b in zip(parts[::2], parts[1::2])]
        return parts[0]

    def row_block(i, base):
        cols = pl.ds(i * TILE, TILE)
        state = {}

        def scores():
            q_split = split_rows(q_t[:, cols])
            top = None
            for j in range(i + 1):
                s = dot(k_n[pl.ds(j * TILE, TILE), :], q_split)
                if j == i:
                    key = lax.broadcasted_iota(jnp.int32, (TILE, 2 * TILE), 0)
                    query = lax.broadcasted_iota(jnp.int32, (TILE, 2 * TILE), 1) % TILE
                    s = jnp.where(query >= key, s, -1e30)
                p_s[pl.ds((base + j) * TILE, TILE), :] = s
                m = fold_rows(s, jnp.maximum)
                top = m if top is None else jnp.maximum(top, m)
            state['max'] = jnp.max(top, axis=0, keepdims=True)

        def weights():
            do_split = split_rows(dctx_ref[:, cols])
            total = dot_sum = None
            for j in range(i + 1):
                rows = pl.ds((base + j) * TILE, TILE)
                dp = dot(v_n[pl.ds(j * TILE, TILE), :], do_split).astype(BF16)
                dp_s[rows, :] = dp
                p = jnp.exp2((p_s[rows, :] - state['max']) * LOG2E)
                p_s[rows, :] = p
                a, b = fold_rows(p, jnp.add), fold_rows(p * dp.astype(F32), jnp.add)
                total = a if total is None else total + a
                dot_sum = b if dot_sum is None else dot_sum + b
            inv = 1.0 / jnp.sum(total, axis=0, keepdims=True)
            state['inv'] = inv
            state['delta'] = jnp.sum(dot_sum, axis=0, keepdims=True) * inv

        def grads():
            q_pair = split_lanes(q_n[cols, :])
            do_pair = split_lanes(do_n[cols, :])
            inv, delta = state['inv'], state['delta']
            ctx = [None, None]
            dq = [None, None]
            for j in range(i + 1):
                rows = pl.ds((base + j) * TILE, TILE)
                keys = pl.ds(j * TILE, TILE)
                p = p_s[rows, :] * inv
                p_bf = p.astype(BF16)
                ds_bf = (p * (dp_s[rows, :].astype(F32) - delta)).astype(BF16)
                for head in range(2):
                    half = slice(head * TILE, (head + 1) * TILE)
                    o = dot(qkv_ref[pl.ds(head * 192 + 128, 64), keys], p_bf[:, half])
                    g = dot(k_t[pl.ds(head * 64, 64), keys], ds_bf[:, half])
                    ctx[head] = o if ctx[head] is None else ctx[head] + o
                    dq[head] = g if dq[head] is None else dq[head] + g
                dv = dot(p_bf, do_pair)
                dk = dot(ds_bf, q_pair)
                if i == T // TILE - 1:
                    dv_acc[keys, :] = dv
                    dk_acc[keys, :] = dk
                else:
                    dv_acc[keys, :] += dv
                    dk_acc[keys, :] += dk
            cos, sin = cos_ref[:, cols], sin_ref[:, cols]
            for head in range(2):
                ctx_ref[pl.ds(head * 64, 64), cols] = ctx[head].astype(BF16)
                write_rotated(head * 192, (dq[head] * 0.125).astype(BF16), cos, sin, cols)
        return scores, weights, grads

    def write_rotated(base, grad, cos, sin, cols):
        lo, hi = grad[:32].astype(F32), grad[32:].astype(F32)
        back = jnp.concatenate([lo * cos + hi * sin, hi * cos - lo * sin], axis=0)
        dqkv_ref[pl.ds(base, 64), cols] = back.astype(BF16)

    blocks = T // TILE
    for m in range(blocks // 2):
        @pl.when(step == m)
        def _(m=m):
            long = row_block(blocks - 1 - m, 0)
            short = row_block(m, blocks - m)
            for a, b in zip(long, short):
                a()
                b()

    @pl.when(step == blocks // 2 - 1)
    def _():
        for t0 in range(0, T, TILE):
            cols = pl.ds(t0, TILE)
            cos, sin = cos_ref[:, cols], sin_ref[:, cols]
            dk = dk_acc[cols, :].astype(BF16).T
            dv = dv_acc[cols, :].astype(BF16).T
            for head in range(2):
                write_rotated(head * 192 + 64, dk[head * 64:(head + 1) * 64], cos, sin, cols)
                dqkv_ref[pl.ds(head * 192 + 128, 64), cols] = dv[head * 64:(head + 1) * 64]


def attention(qkv_t, dctx_t, cos_t, sin_t):
    pairs = dctx_t.shape[0] // 128
    tiles = T // TILE + 1
    return pl.pallas_call(
        attention_kernel,
        grid=(pairs, T // TILE // 2),
        in_specs=[pl.BlockSpec((384, T), lambda p, m: (p, 0)), pl.BlockSpec((128, T), lambda p, m: (p, 0)),
                  pl.BlockSpec((32, T), lambda p, m: (0, 0)), pl.BlockSpec((32, T), lambda p, m: (0, 0))],
        out_specs=[pl.BlockSpec((384, T), lambda p, m: (p, 0)), pl.BlockSpec((128, T), lambda p, m: (p, 0))],
        out_shape=[jax.ShapeDtypeStruct(qkv_t.shape, BF16), jax.ShapeDtypeStruct(dctx_t.shape, BF16)],
        scratch_shapes=[pltpu.VMEM((128, T), BF16)] * 2 + [pltpu.VMEM((T, 128), BF16)] * 4
        + [pltpu.VMEM((tiles * TILE, 2 * TILE), F32), pltpu.VMEM((tiles * TILE, 2 * TILE), BF16)]
        + [pltpu.VMEM((T, 128), F32)] * 2,
        compiler_params=pltpu.CompilerParams(dimension_semantics=("arbitrary", "arbitrary"), vmem_limit_bytes=60 << 20),
        cost_estimate=pl.CostEstimate(flops=int(6 * 2 * 8 * T * T * 64 // 2 * 3), bytes_accessed=20 << 20, transcendentals=8 * T * T // 2),
        name="attention",
    )(qkv_t, dctx_t, cos_t, sin_t)


def wout_kernel(ctx_ref, dy_ref, out_ref):
    out_ref[...] = dot(ctx_ref[...], dy_ref[...])


def wqkv_kernel(ha_ref, dqkv_ref, out_ref):
    out_ref[...] = dot_nt(ha_ref[...], dqkv_ref[...])


def dha_kernel(place_ref, dqkv_ref, w_ref, out_ref):
    out_ref[...] = dot(dqkv_ref[...].T, w_ref[...]).astype(BF16)


def weight_products(ctx_t, dy, ha_t, dqkv_t):
    D, rows, cols = dy.shape[1], ctx_t.shape[0], dqkv_t.shape[0]
    params = pltpu.CompilerParams(dimension_semantics=("arbitrary",), vmem_limit_bytes=40 << 20)
    g_wout = pl.pallas_call(
        wout_kernel, grid=(D // 256,),
        in_specs=[pl.BlockSpec((rows, T), lambda i: (0, 0)), pl.BlockSpec((T, 256), lambda i: (0, i))],
        out_specs=pl.BlockSpec((rows, 256), lambda i: (0, i)),
        out_shape=jax.ShapeDtypeStruct((rows, D), F32), compiler_params=params,
        cost_estimate=pl.CostEstimate(flops=2 * rows * T * D, bytes_accessed=8 << 20, transcendentals=0), name="wout_grad",
    )(ctx_t, dy)
    g_wqkv = pl.pallas_call(
        wqkv_kernel, grid=(cols // 256,),
        in_specs=[pl.BlockSpec((D, T), lambda i: (0, 0)), pl.BlockSpec((256, T), lambda i: (i, 0))],
        out_specs=pl.BlockSpec((D, 256), lambda i: (0, i)),
        out_shape=jax.ShapeDtypeStruct((D, cols), F32), compiler_params=params,
        cost_estimate=pl.CostEstimate(flops=2 * cols * T * D, bytes_accessed=16 << 20, transcendentals=0), name="wqkv_grad",
    )(ha_t, dqkv_t)
    return g_wout, g_wqkv


def dha_part(dqkv_t, wqkv_t, place):
    cols, D = wqkv_t.shape
    return pl.pallas_call(
        dha_kernel,
        grid_spec=pltpu.PrefetchScalarGridSpec(
            num_scalar_prefetch=1, grid=(HALF // TT,),
            in_specs=[pl.BlockSpec((cols, TT), lambda i, place: (0, place[0] * (HALF // TT) + i)), pl.BlockSpec((cols, D), lambda i, place: (0, 0))],
            out_specs=pl.BlockSpec((TT, D), lambda i, place: (i, 0))),
        out_shape=jax.ShapeDtypeStruct((HALF, D), BF16),
        compiler_params=pltpu.CompilerParams(dimension_semantics=("arbitrary",), vmem_limit_bytes=40 << 20),
        cost_estimate=pl.CostEstimate(flops=2 * cols * HALF * D, bytes_accessed=8 << 20, transcendentals=0), name="dha",
    )(jnp.reshape(place, (1,)), dqkv_t, wqkv_t)


def norm_back_kernel(x_ref, dy_ref, a_own, a_other, m_own, m_other, ln_ref, out_ref, gln_ref):
    x = x_ref[...].astype(F32)
    centered = x - jnp.mean(x, axis=-1, keepdims=True)
    rstd = lax.rsqrt(jnp.mean(centered * centered, axis=-1, keepdims=True) + NORM_EPS)
    xhat = centered * rstd
    da = (a_own[...].astype(F32) + a_other[...].astype(F32)).astype(BF16).astype(F32)
    dm = (m_own[...].astype(F32) + m_other[...].astype(F32)).astype(BF16).astype(F32)
    g = da * ln_ref[0:1, :] + dm * ln_ref[2:3, :]
    mean_g = jnp.mean(g, axis=-1, keepdims=True)
    mean_gx = jnp.mean(g * xhat, axis=-1, keepdims=True)
    out_ref[...] = (dy_ref[...].astype(F32) + rstd * (g - mean_g - xhat * mean_gx)).astype(BF16)
    sums = jnp.concatenate([jnp.sum(v, axis=0, keepdims=True) for v in (da * xhat, da, dm * xhat, dm)], axis=0)

    @pl.when(pl.program_id(0) == 0)
    def _():
        gln_ref[...] = sums

    @pl.when(pl.program_id(0) > 0)
    def _():
        gln_ref[...] += sums


def norm_back(x, dy, a_own, a_other, m_own, m_other, ln):
    rows, D = x.shape
    tok = pl.BlockSpec((256, D), lambda i: (i, 0))
    small = pl.BlockSpec((4, D), lambda i: (0, 0))
    return pl.pallas_call(
        norm_back_kernel, grid=(rows // 256,),
        in_specs=[tok] * 6 + [small], out_specs=[tok, small],
        out_shape=[jax.ShapeDtypeStruct((rows, D), BF16), jax.ShapeDtypeStruct((4, D), F32)],
        compiler_params=pltpu.CompilerParams(dimension_semantics=("arbitrary",), vmem_limit_bytes=40 << 20),
        cost_estimate=pl.CostEstimate(flops=40 * rows * D, bytes_accessed=14 << 20, transcendentals=0), name="norm_back",
    )(x, dy, a_own, a_other, m_own, m_other, ln)


def shift_chips(value, axis, step):
    stride = AXIS_STRIDE[axis]
    pairs = []
    for chip in range(64):
        place = (chip // stride) % 4
        pairs.append((chip, chip + (((place + step) % 4) - place) * stride))
    return lax.ppermute(value, 'dp', pairs)


def reduce_ring(blocks, axis):
    place = (lax.axis_index('dp') // AXIS_STRIDE[axis]) % 4

    def half(ahead, which):
        return lax.dynamic_slice_in_dim(blocks, (place + ahead) % 4, 1, 0)[0, which]

    up = shift_chips(jnp.stack([half(2, 0), half(1, 1)]), axis, 1)
    down = shift_chips(jnp.stack([half(2, 1), half(3, 0)]), axis, -1)
    up_last = shift_chips(half(1, 0) + up[0], axis, 1)
    down_last = shift_chips(half(3, 1) + down[0], axis, -1)
    return jnp.stack([half(0, 0) + up_last + down[1], half(0, 1) + down_last + up[1]])


def reduce_scatter_torus(grad, order):
    rows = grad.shape[0] // 64
    grad = grad.reshape(4, 4, 4, 2, rows // 2, grad.shape[1])
    left = ['z', 'y', 'x']
    for axis in order:
        place = left.index(axis)
        grad = jnp.moveaxis(grad, (place, len(left)), (0, 1))
        grad = jnp.moveaxis(reduce_ring(grad, axis), 0, len(left) - 1)
        left.pop(place)
    return grad.reshape(rows, -1)


def swap_cores(value):
    return lax.ppermute(value, 'tp', [(0, 1), (1, 0)])


def sum_all(value):
    value = value + swap_cores(value)
    for axis in ('x', 'y', 'z'):
        near, far, back = (shift_chips(value, axis, step) for step in (1, 2, 3))
        place = (lax.axis_index('dp') // AXIS_STRIDE[axis]) % 4
        ring = jnp.stack([value, near, far, back])
        value = sum(lax.dynamic_index_in_dim(ring, (place - k) % 4, 0, keepdims=False) for k in range(4))
    return value


def solution(mesh):
    def local_step(x_loc, dy_loc, ln_params, w_qkv, w_out, w_up, w_down):
        D = x_loc.shape[2]
        core = lax.axis_index('tp')
        x_loc, dy_loc = x_loc[0], dy_loc[0]
        wqkv_t = w_qkv.transpose(1, 2, 3, 0).reshape(-1, D)

        def whole(own):
            other = swap_cores(own)
            first = core == 0
            return jnp.concatenate([jnp.where(first, own, other), jnp.where(first, other, own)], axis=0)

        x_full, dy_full = whole(x_loc), whole(dy_loc)
        ha_t, qkv_t, dctx_t, dhm, g_wup, g_wdown = token_part(x_full, dy_full, ln_params, wqkv_t, w_out, w_up, w_down)
        grad_wup = reduce_scatter_torus(g_wup, ('x', 'y', 'z'))
        grad_wdown = reduce_scatter_torus(g_wdown, ('y', 'z', 'x'))

        def part(full, place):
            return lax.dynamic_slice_in_dim(full, place * HALF, HALF, 0)

        dhm_other = swap_cores(part(dhm, 1 - core))
        cos_t, sin_t = rope_tables()
        dqkv_t, ctx_t = attention(qkv_t, dctx_t, cos_t, sin_t)
        g_wout, g_wqkv = weight_products(ctx_t, dy_full, ha_t, dqkv_t)
        grad_wout = reduce_scatter_torus(g_wout, ('z', 'x', 'y'))
        grad_wqkv = reduce_scatter_torus(g_wqkv, ('z', 'x', 'y')).reshape(16, 8, 3, 64)
        dha_other = swap_cores(dha_part(dqkv_t, wqkv_t, 1 - core))
        dha_own = dha_part(dqkv_t, wqkv_t, core)
        grad_x, g_ln = norm_back(x_loc, dy_loc, dha_own, dha_other, part(dhm, core), dhm_other, ln_params)
        return grad_x[None], sum_all(g_ln), grad_wqkv, grad_wout, grad_wup, grad_wdown

    act_spec = P('dp', 'tp', None)
    in_specs = (act_spec, act_spec, P(None, None), P(None, 'tp', None, None), P('tp', None), P(None, 'tp'), P('tp', None))
    out_specs = (act_spec, P(None, None), P('dp', 'tp', None, None), P(('tp', 'dp'), None), P('dp', 'tp'), P(('tp', 'dp'), None))
    return jax.shard_map(local_step, mesh=mesh, in_specs=in_specs, out_specs=out_specs, check_vma=False)
```

```python
import math

import jax
import jax.numpy as jnp
import numpy as np
from jax import lax
from jax.experimental import pallas as pl
from jax.experimental.pallas import tpu as pltpu
from jax.sharding import PartitionSpec as P

NORM_EPS = 1e-5
ROPE_BASE = 10000.0
F32, BF16 = jnp.float32, jnp.bfloat16
LOG2E = math.log2(math.e)
T = 2048
HALF = T // 2
TILE = 256
SMALL = 128
TT = 512
FC = 512
LANES = 128
VMEM_LIMIT = 63 << 20
AXES = ('z', 'y', 'x')
AXIS_STRIDE = {'z': 16, 'y': 4, 'x': 1}
RING = 4


def dot(a, b):
    return jnp.dot(a, b, preferred_element_type=F32)


def dot_nt(a, b):
    return lax.dot_general(a, b, (((1,), (1,)), ((), ())), preferred_element_type=F32)


def rope_tables():
    inv_freq = ROPE_BASE ** (-2.0 * jnp.arange(32, dtype=F32) / 64)
    angles = inv_freq[:, None] * jnp.arange(T, dtype=F32)[None, :]
    return jnp.cos(angles), jnp.sin(angles)


def ring_place(axis):
    return lax.rem(lax.div(lax.axis_index('dp'), AXIS_STRIDE[axis]), RING)


def ring_chip(axis, ahead):
    place = ring_place(axis)
    return {'dp': lax.axis_index('dp') + (lax.rem(place + ahead, RING) - place) * AXIS_STRIDE[axis]}


def other_core():
    return {'tp': 1 - lax.axis_index('tp')}


def send_to(device, src, dst, send_sem, recv_sem):
    return pltpu.make_async_remote_copy(src_ref=src, dst_ref=dst, send_sem=send_sem, recv_sem=recv_sem,
                                        device_id=device, device_id_type=pl.DeviceIdType.MESH)


def greet(devices):
    barrier = pltpu.get_barrier_semaphore()
    for device in devices:
        pl.semaphore_signal(barrier, inc=1, device_id=device, device_id_type=pl.DeviceIdType.MESH)
    pl.semaphore_wait(barrier, len(devices))


class TorusSum:
    COUNT = 30

    @staticmethod
    def half_shape(rows, width, by_cols):
        return (rows, width // 2) if by_cols else (rows // 2, width)

    @staticmethod
    def scratch(rows, width, by_cols=False):
        half, whole = TorusSum.half_shape(rows, width, by_cols), (rows, width)
        shapes = []
        for lead in ((RING, RING), (RING,), ()):
            shapes += [pltpu.VMEM(lead + half, F32)] * 8 + [pltpu.VMEM(lead + whole, F32)]
        return shapes + [pltpu.SemaphoreType.DMA((18,)), pltpu.SemaphoreType.DMA((18,)), pltpu.SemaphoreType.DMA((3,))]

    def __init__(self, grad, order, rows, col, width, refs, by_cols=False, in_vmem=False):
        self.grad, self.order, self.col, self.by_cols, self.in_vmem = grad, order, col, by_cols, in_vmem
        self.whole, self.half = (rows, width), TorusSum.half_shape(rows, width, by_cols)
        self.cols = pl.ds(col, width)
        self.refs, (self.send, self.recv, self.load) = refs, refs[27:]
        self.kept = [[axis for axis in AXES if axis not in order[:n]] for n in range(3)]

    def bufs(self, phase):
        return self.refs[9 * phase:9 * phase + 9]

    def part(self, which, col=0):
        shape = self.whole if which == 2 else self.half
        start = [0, col]
        if which == 1:
            start[self.by_cols] += self.half[self.by_cols]
        return tuple(pl.ds(first, size) for first, size in zip(start, shape))

    def block(self, phase, ahead, which):
        index = lax.rem(ring_place(self.order[phase]) + ahead, RING)
        lead = tuple(index if axis == self.order[phase] else slice(None) for axis in self.kept[phase])
        if phase == 0:
            return self.grad.at[lead + self.part(which, self.col)]
        return self.refs[9 * phase - 1].at[lead + self.part(which)]

    def load_copy(self, n):
        ahead, which = ((1, 0), (3, 1), (0, 2))[n]
        return pltpu.make_async_copy(self.block(0, ahead, which), self.bufs(0)[6 + n], self.load.at[n])

    def copy(self, phase, n):
        bufs = self.bufs(phase)
        src = bufs[2 + n] if n >= 4 else self.block(phase, *((2, 0), (1, 1), (2, 1), (3, 0))[n])
        chip = ring_chip(self.order[phase], (1, 1, 3, 3, 1, 3)[n])
        return send_to(chip, src, bufs[n], self.send.at[6 * phase + n], self.recv.at[6 * phase + n])

    def loads(self, phase):
        return phase == 0 and not self.in_vmem

    def start(self, phase):
        for n in (0, 2, 1, 3):
            self.copy(phase, n).start()
        if self.loads(phase):
            for n in range(3):
                self.load_copy(n).start()

    def add(self, phase):
        bufs = self.bufs(phase)
        own = self.block(phase, 1, 0), self.block(phase, 3, 1)
        if self.loads(phase):
            own = bufs[6], bufs[7]
            self.load_copy(0).wait()
            self.load_copy(1).wait()
        self.copy(phase, 0).wait_recv()
        self.copy(phase, 2).wait_recv()

        def rows(at):
            bufs[6][at] = own[0][at] + bufs[0][at]
            bufs[7][at] = own[1][at] + bufs[2][at]
        self.each(phase, rows)

    def each(self, phase, body):
        if phase == 0:
            def step(n, carry):
                body(n)
                return carry
            lax.fori_loop(0, RING, step, 0)
        else:
            body(slice(None))

    def pass_on(self, phase):
        self.copy(phase, 4).start()
        self.copy(phase, 5).start()

    def finish(self, phase):
        bufs = self.bufs(phase)
        lead = (slice(None),) * (2 - phase)
        low, high = bufs[8].at[lead + self.part(0)], bufs[8].at[lead + self.part(1)]
        own = self.block(phase, 0, 0), self.block(phase, 0, 1)
        if self.loads(phase):
            own = low, high
            self.load_copy(2).wait()
        for n in (1, 3, 4, 5):
            self.copy(phase, n).wait_recv()

        def rows(at):
            low[at] = own[0][at] + bufs[3][at] + bufs[4][at]
            high[at] = own[1][at] + bufs[1][at] + bufs[5][at]
        self.each(phase, rows)

    def drain(self):
        for phase in range(3):
            for n in range(6):
                self.copy(phase, n).wait_send()

    @property
    def result(self):
        return self.refs[26]


def plan_columns(rows, tiles, by_cols=False):
    plan, col = [], 0
    for order, count in zip((('x', 'y', 'z'), ('y', 'z', 'x'), ('z', 'x', 'y')), tiles):
        plan.append((order, rows, col, count * LANES, by_cols))
        col += count * LANES
    return plan


def plan_scratch(plans):
    return [shape for plan in plans for _, rows, _, width, by_cols in plan for shape in TorusSum.scratch(rows, width, by_cols)]


def plan_sums(grads, plans, refs, in_vmem=False):
    groups = []
    for grad, plan in zip(grads, plans):
        groups.append([])
        for order, rows, col, width, by_cols in plan:
            groups[-1].append(TorusSum(grad, order, rows, col, width, refs[:TorusSum.COUNT], by_cols, in_vmem))
            refs = refs[TorusSum.COUNT:]
    return groups


PLAN_UP = plan_columns(16, (5, 5, 6))
PLAN_DOWN = plan_columns(32, (3, 3, 2))
PLAN_QKV = plan_columns(16, (4, 4, 4))
PLAN_OUT = plan_columns(8, (2, 2, 4), True)


def normed(x):
    x = x.astype(F32)
    centered = x - jnp.mean(x, axis=-1, keepdims=True)
    rstd = lax.rsqrt(jnp.mean(centered * centered, axis=-1, keepdims=True) + NORM_EPS)
    return centered * rstd, rstd


def token_kernel(x_hbm, dy_hbm, ln_ref, wqkv_hbm, wout_hbm, wup_hbm, wdown_hbm,
                 ha_ref, qkv_ref, dctx_ref, dhm_ref, dy_ref, gup_ref, gdown_ref,
                 xs, dys, wqkv, wout, wup, wdown, hm_s, hm_t, dh_s, up_acc, down_acc,
                 row_load, w_load, chunk_load, flush_sem, send, recv):
    step = pl.program_id(0)
    first, last = step == 0, step == pl.num_programs(0) - 1
    width = wup.shape[1]
    chunks = width // FC
    rows = pl.ds(pl.multiple_of(step * TT, TT), TT)

    def chunk(c):
        return pl.ds(c * FC, FC)

    def flush(c):
        return (pltpu.make_async_copy(up_acc.at[:, chunk(c)], gup_ref.at[:, chunk(c)], flush_sem.at[0, c]),
                pltpu.make_async_copy(down_acc.at[chunk(c), :], gdown_ref.at[chunk(c), :], flush_sem.at[1, c]))

    def row_loads(n):
        part = pl.ds(n * TT, TT)
        return [pltpu.make_async_copy(src.at[part], dst.at[part], row_load.at[k, n]) for k, (src, dst) in enumerate(((x_hbm, xs), (dy_hbm, dys)))]

    def chunk_loads(c):
        return (pltpu.make_async_copy(wup_hbm.at[:, chunk(c)], wup.at[:, chunk(c)], chunk_load.at[0, c]),
                pltpu.make_async_copy(wdown_hbm.at[chunk(c), :], wdown.at[chunk(c), :], chunk_load.at[1, c]))

    w_loads = [pltpu.make_async_copy(src, dst, w_load.at[k]) for k, (src, dst) in enumerate(((wqkv_hbm, wqkv), (wout_hbm, wout)))]
    swaps = [send_to(other_core(), src, dst.at[pl.ds(HALF, HALF)], send.at[k], recv.at[k]) for k, (src, dst) in enumerate(((x_hbm, xs), (dy_hbm, dys)))]

    @pl.when(first)
    def _():
        for copy in [*row_loads(0), *(copy for c in range(chunks) for copy in chunk_loads(c)), *w_loads, *row_loads(1)]:
            copy.start()
        up_acc[:] = jnp.zeros_like(up_acc)
        down_acc[:] = jnp.zeros_like(down_acc)
        greet([other_core()])
        for copy in swaps:
            copy.start()

    for n in range(HALF // TT):
        @pl.when(step == n)
        def _(n=n):
            for copy in row_loads(n):
                copy.wait()

    @pl.when(step == HALF // TT)
    def _():
        for copy in swaps:
            copy.wait_recv()

    norm, _ = normed(xs[rows, :])
    hm = (norm * ln_ref[pl.ds(2, 1), :] + ln_ref[pl.ds(3, 1), :]).astype(BF16)
    ha_ref[:] = (norm * ln_ref[pl.ds(0, 1), :] + ln_ref[pl.ds(1, 1), :]).astype(BF16).T
    hm_s[:] = hm
    hm_t[:] = hm.T
    dy_ref[:] = dys[rows, :]

    for c in range(chunks):
        @pl.when(first)
        def _(c=c):
            for copy in chunk_loads(c):
                copy.wait()
        cols = chunk(c)
        u = dot(hm_s[:], wup[:, cols]).astype(BF16).astype(F32)
        dg = dot_nt(dys[rows, :], wdown[cols, :]).astype(BF16).astype(F32)
        cdf = 0.5 * (1.0 + lax.erf(u * math.sqrt(0.5)))
        gelu = (u * cdf).astype(BF16)
        pdf = jnp.exp(-0.5 * u * u) * (1.0 / math.sqrt(2.0 * math.pi))
        dh = (dg * (cdf + u * pdf)).astype(BF16)
        dh_s[:, cols] = dh
        down_acc[cols, :] += dot(gelu.T, dys[rows, :])
        up_acc[:, cols] += dot(hm_t[:], dh)

        @pl.when(last)
        def _(c=c):
            for copy in flush(c):
                copy.start()
    dhm_ref[:] = dot_nt(dh_s[:], wup[:]).astype(BF16)

    @pl.when(first)
    def _():
        for copy in w_loads:
            copy.wait()
    qkv_ref[:] = dot(wqkv[:], ha_ref[:]).astype(BF16)
    dctx_ref[:] = dot_nt(wout[:], dys[rows, :]).astype(BF16)

    @pl.when(last)
    def _():
        for copy in swaps:
            copy.wait_send()
        for c in range(chunks):
            for copy in flush(c):
                copy.wait()


def token_part(x, dy, ln, wqkv_t, wout, wup, wdown):
    D, width = wup.shape
    S, V, dma = jax.ShapeDtypeStruct, pltpu.VMEM, pltpu.SemaphoreType.DMA
    hbm = pl.BlockSpec(memory_space=pl.ANY)
    steps, halves = T // TT, HALF // TT

    def tile(i):
        core = lax.axis_index('tp')
        return jnp.where(i < halves, core * halves + i, (1 - core) * halves + i - halves)

    def tok(size):
        return pl.BlockSpec((TT, size), lambda i: (tile(i), 0))

    def col(size):
        return pl.BlockSpec((size, TT), lambda i: (0, tile(i)))

    return pl.pallas_call(
        token_kernel,
        grid=(steps,),
        in_specs=[hbm, hbm, pl.BlockSpec(memory_space=pltpu.VMEM)] + [hbm] * 4,
        out_specs=[col(D), col(wqkv_t.shape[0]), col(wout.shape[0]), tok(D), tok(D), hbm, hbm],
        out_shape=[S((D, T), BF16), S((wqkv_t.shape[0], T), BF16), S((wout.shape[0], T), BF16), S((T, D), BF16), S((T, D), BF16),
                   S((D, width), F32), S((width, D), F32)],
        scratch_shapes=[V((T, D), BF16)] * 2 + [V(w.shape, BF16) for w in (wqkv_t, wout, wup, wdown)]
        + [V((TT, D), BF16), V((D, TT), BF16), V((TT, width), BF16), V((D, width), F32), V((width, D), F32)]
        + [dma((2, halves)), dma((2,)), dma((2, width // FC)), dma((2, width // FC)), dma((2,)), dma((2,))],
        compiler_params=pltpu.CompilerParams(dimension_semantics=("arbitrary",), vmem_limit_bytes=VMEM_LIMIT,
                                             collective_id=2, has_side_effects=True),
        cost_estimate=pl.CostEstimate(flops=52 * 10**9, bytes_accessed=60 << 20, transcendentals=2 * T * width),
        name="token_part",
    )(x, dy, ln, wqkv_t, wout, wup, wdown)


SCHEDULE = {
    0: (('up', 'start', 0),),
    3: (('up', 'add', 0), ('up', 'pass_on', 0), ('down', 'start', 0)),
    5: (('up', 'finish', 0), ('up', 'start', 1)),
    8: (('down', 'add', 0), ('up', 'add', 1), ('down', 'pass_on', 0), ('up', 'pass_on', 1)),
    10: (('down', 'finish', 0), ('up', 'finish', 1), ('down', 'start', 1), ('up', 'start', 2)),
    12: (('down', 'add', 1), ('up', 'add', 2), ('down', 'pass_on', 1), ('up', 'pass_on', 2)),
    13: (('down', 'finish', 1), ('up', 'finish', 2), ('down', 'start', 2)),
    14: (('down', 'add', 2), ('down', 'pass_on', 2)),
}


def attention_kernel(qkv_ref, dctx_ref, cos_ref, sin_ref, up_ref, down_ref, dqkv_ref, ctx_ref, up_out, down_out,
                     q_t, k_t, q_n, k_n, v_n, do_n, p_s, dp_s, dk_acc, dv_acc, *sum_refs):
    step = pl.program_id(1)
    now = pl.program_id(0) * pl.num_programs(1) + step
    sums = dict(zip(('up', 'down'), plan_sums((up_ref, down_ref), (PLAN_UP, PLAN_DOWN), sum_refs)))

    for when, stages in SCHEDULE.items():
        @pl.when(now == when)
        def _(when=when, stages=stages):
            if when == 0:
                greet([ring_chip(axis, ahead) for axis in AXES for ahead in (1, 3)])
            for group, stage, phase in stages:
                for one in sums[group]:
                    getattr(one, stage)(phase)

    @pl.when(step == 0)
    def _():
        for t0 in range(0, T, TILE):
            cols = pl.ds(t0, TILE)
            cos, sin = cos_ref[:, cols], sin_ref[:, cols]
            for head in range(2):
                base = head * 192
                for slot, ref, factor in ((0, q_t, 0.125), (1, k_t, 1.0)):
                    lo = qkv_ref[pl.ds(base + slot * 64, 32), cols].astype(F32)
                    hi = qkv_ref[pl.ds(base + slot * 64 + 32, 32), cols].astype(F32)
                    rot = jnp.concatenate([lo * cos - hi * sin, hi * cos + lo * sin], axis=0).astype(BF16)
                    if factor != 1.0:
                        rot = rot * jnp.asarray(factor, BF16)
                    ref[pl.ds(head * 64, 64), cols] = rot
            q_n[cols, :] = q_t[:, cols].T
            k_n[cols, :] = k_t[:, cols].T
            v_pair = jnp.concatenate([qkv_ref[pl.ds(128, 64), cols], qkv_ref[pl.ds(320, 64), cols]], axis=0)
            v_n[cols, :] = v_pair.T
            do_n[cols, :] = dctx_ref[:, cols].T

    lane = lax.broadcasted_iota(jnp.int32, (TILE, 128), 1)

    def split_lanes(x):
        zero = jnp.zeros_like(x)
        return jnp.concatenate([jnp.where(lane < 64, x, zero), jnp.where(lane < 64, zero, x)], axis=0)

    def split_rows(x):
        zero = jnp.zeros((64, TILE), x.dtype)
        return jnp.concatenate([jnp.concatenate([x[:64], zero], axis=1), jnp.concatenate([zero, x[64:]], axis=1)], axis=0)

    def fold_rows(x, op):
        parts = [x[r * 8:(r + 1) * 8] for r in range(TILE // 8)]
        while len(parts) > 1:
            parts = [op(a, b) for a, b in zip(parts[::2], parts[1::2])]
        return parts[0]

    def row_block(i, base):
        cols = pl.ds(i * TILE, TILE)
        state = {}

        def scores():
            q_split = split_rows(q_t[:, cols])
            top = None
            for j in range(i + 1):
                s = dot(k_n[pl.ds(j * TILE, TILE), :], q_split)
                if j == i:
                    key = lax.broadcasted_iota(jnp.int32, (TILE, 2 * TILE), 0)
                    query = lax.broadcasted_iota(jnp.int32, (TILE, 2 * TILE), 1) % TILE
                    s = jnp.where(query >= key, s, -1e30)
                p_s[pl.ds((base + j) * TILE, TILE), :] = s
                m = fold_rows(s, jnp.maximum)
                top = m if top is None else jnp.maximum(top, m)
            state['max'] = jnp.max(top, axis=0, keepdims=True)

        def weights():
            do_split = split_rows(dctx_ref[:, cols])
            total = dot_sum = None
            for j in range(i + 1):
                rows = pl.ds((base + j) * TILE, TILE)
                dp = dot(v_n[pl.ds(j * TILE, TILE), :], do_split).astype(BF16)
                dp_s[rows, :] = dp
                p = jnp.exp2((p_s[rows, :] - state['max']) * LOG2E)
                p_s[rows, :] = p
                a, b = fold_rows(p, jnp.add), fold_rows(p * dp.astype(F32), jnp.add)
                total = a if total is None else total + a
                dot_sum = b if dot_sum is None else dot_sum + b
            inv = 1.0 / jnp.sum(total, axis=0, keepdims=True)
            state['inv'] = inv
            state['delta'] = jnp.sum(dot_sum, axis=0, keepdims=True) * inv

        def grads():
            q_pair = split_lanes(q_n[cols, :])
            do_pair = split_lanes(do_n[cols, :])
            inv, delta = state['inv'], state['delta']
            ctx = [None, None]
            dq = [None, None]
            for j in range(i + 1):
                rows = pl.ds((base + j) * TILE, TILE)
                keys = pl.ds(j * TILE, TILE)
                p = p_s[rows, :] * inv
                p_bf = p.astype(BF16)
                ds_bf = (p * (dp_s[rows, :].astype(F32) - delta)).astype(BF16)
                for head in range(2):
                    half = slice(head * TILE, (head + 1) * TILE)
                    o = dot(qkv_ref[pl.ds(head * 192 + 128, 64), keys], p_bf[:, half])
                    g = dot(k_t[pl.ds(head * 64, 64), keys], ds_bf[:, half])
                    ctx[head] = o if ctx[head] is None else ctx[head] + o
                    dq[head] = g if dq[head] is None else dq[head] + g
                dv = dot(p_bf, do_pair)
                dk = dot(ds_bf, q_pair)
                if i == T // TILE - 1:
                    dv_acc[keys, :] = dv
                    dk_acc[keys, :] = dk
                else:
                    dv_acc[keys, :] += dv
                    dk_acc[keys, :] += dk
            cos, sin = cos_ref[:, cols], sin_ref[:, cols]
            for head in range(2):
                ctx_ref[pl.ds(head * 64, 64), cols] = ctx[head].astype(BF16)
                write_rotated(head * 192, (dq[head] * 0.125).astype(BF16), cos, sin, cols)
        return scores, weights, grads

    def write_rotated(base, grad, cos, sin, cols):
        lo, hi = grad[:32].astype(F32), grad[32:].astype(F32)
        back = jnp.concatenate([lo * cos + hi * sin, hi * cos - lo * sin], axis=0)
        dqkv_ref[pl.ds(base, 64), cols] = back.astype(BF16)

    blocks = T // TILE
    for m in range(blocks // 2):
        @pl.when(step == m)
        def _(m=m):
            long = row_block(blocks - 1 - m, 0)
            short = row_block(m, blocks - m)
            for a, b in zip(long, short):
                a()
                b()

    @pl.when(step == blocks // 2 - 1)
    def _():
        for t0 in range(0, T, TILE):
            cols = pl.ds(t0, TILE)
            cos, sin = cos_ref[:, cols], sin_ref[:, cols]
            dk = dk_acc[cols, :].astype(BF16).T
            dv = dv_acc[cols, :].astype(BF16).T
            for head in range(2):
                write_rotated(head * 192 + 64, dk[head * 64:(head + 1) * 64], cos, sin, cols)
                dqkv_ref[pl.ds(head * 192 + 128, 64), cols] = dv[head * 64:(head + 1) * 64]

    @pl.when(now == 15)
    def _():
        for one in sums['down']:
            one.finish(2)
        for group, out in (('up', up_out), ('down', down_out)):
            for one in sums[group]:
                out[:, one.cols] = one.result[:]
                one.drain()


def attention(qkv_t, dctx_t, cos_t, sin_t, g_up, g_down):
    pairs = dctx_t.shape[0] // 128
    tiles = T // TILE + 1
    S, V = jax.ShapeDtypeStruct, pltpu.VMEM
    up_share, down_share = (g_up.shape[0] // 64, g_up.shape[1]), (g_down.shape[0] // 64, g_down.shape[1])
    hbm = pl.BlockSpec(memory_space=pl.ANY)

    def by_pair(rows):
        return pl.BlockSpec((rows, T), lambda p, m: (p, 0))

    def fixed(shape):
        return pl.BlockSpec(shape, lambda p, m: (0, 0))

    return pl.pallas_call(
        attention_kernel,
        grid=(pairs, T // TILE // 2),
        in_specs=[by_pair(384), by_pair(128), fixed(cos_t.shape), fixed(sin_t.shape), hbm, hbm],
        out_specs=[by_pair(384), by_pair(128), fixed(up_share), fixed(down_share)],
        out_shape=[S(qkv_t.shape, BF16), S(dctx_t.shape, BF16), S(up_share, F32), S(down_share, F32)],
        scratch_shapes=[V((128, T), BF16)] * 2 + [V((T, 128), BF16)] * 4 + [V((tiles * TILE, 2 * TILE), F32), V((tiles * TILE, 2 * TILE), BF16)]
        + [V((T, 128), F32)] * 2 + plan_scratch((PLAN_UP, PLAN_DOWN)),
        compiler_params=pltpu.CompilerParams(dimension_semantics=("arbitrary", "arbitrary"), vmem_limit_bytes=VMEM_LIMIT,
                                             collective_id=0, has_side_effects=True),
        cost_estimate=pl.CostEstimate(flops=int(6 * 2 * 8 * T * T * 64 // 2 * 3), bytes_accessed=20 << 20, transcendentals=8 * T * T // 2),
        name="attention",
    )(qkv_t, dctx_t, cos_t, sin_t, *(g.reshape((RING,) * 3 + (-1, g.shape[1])) for g in (g_up, g_down)))


def tail_kernel(hat_hbm, dqkv_hbm, ctx_hbm, dy_hbm, w_hbm, x_hbm, dhm_hbm, ln_ref, gx_ref, gln_ref, gqkv_ref, gout_ref,
                hat, dqkv, ctx, dy, w, x, dhm_own, dhm_in, dha_own, dha_out, dha_in, g_qkv, g_out, pair_s, ring_s,
                load, send, recv, ring_send, ring_recv, *sum_refs):
    core = lax.axis_index('tp')
    own, away = core * HALF, (1 - core) * HALF
    qkv_sums, out_sums = plan_sums((g_qkv, g_out), (PLAN_QKV, PLAN_OUT), sum_refs, True)
    every = qkv_sums + out_sums
    block = dqkv.shape[0] // len(qkv_sums)

    def rows_of(ref, start, size):
        return ref.at[pl.ds(start, size)]

    pieces = [(hat_hbm, hat)] + [(rows_of(dqkv_hbm, n * block, block), rows_of(dqkv, n * block, block)) for n in range(3)]
    pieces += [(ctx_hbm, ctx), (dy_hbm, dy), (w_hbm, w), (x_hbm, x), (rows_of(dhm_hbm, own, HALF), dhm_own)]
    loads = [pltpu.make_async_copy(src, dst, load.at[n]) for n, (src, dst) in enumerate(pieces)]
    for copy in loads:
        copy.start()
    greet([ring_chip(axis, ahead) for axis in AXES for ahead in (1, 2, 3)] + [other_core()])
    dhm_copy = send_to(other_core(), rows_of(dhm_hbm, away, HALF), dhm_in, send.at[0], recv.at[0])
    dha_copy = send_to(other_core(), dha_out, dha_in, send.at[1], recv.at[1])
    pair_copy = send_to(other_core(), pair_s.at[0], pair_s.at[1], send.at[2], recv.at[2])
    dhm_copy.start()

    loads[0].wait()
    for n, one in enumerate(qkv_sums):
        loads[1 + n].wait()

        def columns(k, carry, n=n):
            first = pl.multiple_of(n * block + k * TILE, TILE)
            product = dot_nt(hat[:], dqkv[pl.ds(first, TILE), :])
            g_qkv[:, :, :, :, pl.ds(first, TILE)] = product.reshape(g_qkv.shape[:4] + (TILE,))
            return carry
        lax.fori_loop(0, block // TILE, columns, 0)
        one.start(0)
    loads[4].wait()
    loads[5].wait()

    def out_columns(k, carry):
        cols = pl.ds(pl.multiple_of(k * TILE, TILE), TILE)
        g_out[:, :, :, :, cols] = dot(ctx[:], dy[:, cols]).reshape(g_out.shape[:4] + (TILE,))
        return carry
    lax.fori_loop(0, dy.shape[1] // TILE, out_columns, 0)
    for one in out_sums:
        one.start(0)

    loads[6].wait()
    for first, target in ((away, dha_out), (own, dha_own)):
        def tokens(k, carry, first=first, target=target):
            cols = pl.ds(pl.multiple_of(first + k * TILE, TILE), TILE)
            target[pl.ds(pl.multiple_of(k * TILE, TILE), TILE), :] = dot(dqkv[:, cols].T, w[:]).astype(BF16)
            return carry
        lax.fori_loop(0, HALF // TILE, tokens, 0)
        if target is dha_out:
            dha_copy.start()

    def stages(sums, phase, *names):
        for name in names:
            for one in sums:
                getattr(one, name)(phase)

    stages(qkv_sums, 0, 'add', 'pass_on')
    loads[7].wait()
    loads[8].wait()
    dhm_copy.wait_recv()
    dha_copy.wait_recv()
    pair_s[0] = jnp.zeros_like(pair_s[0])

    def norm_back(k, carry):
        at = pl.ds(pl.multiple_of(k * SMALL, SMALL), SMALL)
        norm, rstd = normed(x[at, :])
        da = (dha_own[at, :].astype(F32) + dha_in[at, :].astype(F32)).astype(BF16).astype(F32)
        dm = (dhm_own[at, :].astype(F32) + dhm_in[at, :].astype(F32)).astype(BF16).astype(F32)
        g = da * ln_ref[pl.ds(0, 1), :] + dm * ln_ref[pl.ds(2, 1), :]
        mean_g = jnp.mean(g, axis=-1, keepdims=True)
        mean_gn = jnp.mean(g * norm, axis=-1, keepdims=True)
        residual = dy[pl.ds(pl.multiple_of(own + k * SMALL, SMALL), SMALL), :].astype(F32)
        gx_ref[at, :] = (residual + rstd * (g - mean_g - norm * mean_gn)).astype(BF16)
        for row, value in enumerate((da * norm, da, dm * norm, dm)):
            pair_s[0, pl.ds(row, 1), :] += jnp.sum(value, axis=0, keepdims=True)
        return carry

    half = HALF // SMALL // 2
    lax.fori_loop(0, half, norm_back, 0)
    stages(out_sums, 0, 'add', 'pass_on')
    stages(qkv_sums, 0, 'finish')
    stages(qkv_sums, 1, 'start')
    lax.fori_loop(half, 2 * half, norm_back, 0)
    pair_copy.start()
    stages(out_sums, 0, 'finish')
    stages(out_sums, 1, 'start')
    stages(qkv_sums, 1, 'add', 'pass_on')
    stages(out_sums, 1, 'add', 'pass_on')

    def ring_copies(phase):
        place = ring_place(AXES[phase])
        return [send_to(ring_chip(AXES[phase], ahead), ring_s.at[phase, place], ring_s.at[phase, place],
                        ring_send.at[phase, ahead], ring_recv.at[phase, ahead]) for ahead in (1, 2, 3)]

    def ring_start(phase, value):
        ring_s[phase, ring_place(AXES[phase])] = value
        for copy in ring_copies(phase):
            copy.start()

    def ring_sum(phase):
        for copy in ring_copies(phase):
            copy.wait_recv()
        return ring_s[phase, 0] + ring_s[phase, 1] + ring_s[phase, 2] + ring_s[phase, 3]

    pair_copy.wait_recv()
    ring_start(0, pair_s[0] + pair_s[1])
    stages(every, 1, 'finish')
    stages(every, 2, 'start')
    ring_start(1, ring_sum(0))
    stages(every, 2, 'add', 'pass_on')
    ring_start(2, ring_sum(1))
    stages(every, 2, 'finish')
    gln_ref[:] = ring_sum(2)[:gln_ref.shape[0]]
    for out, sums in ((gqkv_ref, qkv_sums), (gout_ref, out_sums)):
        for one in sums:
            out[:, one.cols] = one.result[:]
            one.drain()
    for copy in (dhm_copy, dha_copy, pair_copy):
        copy.wait_send()
    for phase in range(3):
        for copy in ring_copies(phase):
            copy.wait_send()


def tail(ha_t, dqkv_t, ctx_t, dy, wqkv_t, x, dhm, ln):
    D, C = ha_t.shape[0], ctx_t.shape[0]
    S, V = jax.ShapeDtypeStruct, pltpu.VMEM
    hbm, vmem = pl.BlockSpec(memory_space=pl.ANY), pl.BlockSpec(memory_space=pltpu.VMEM)
    own = V((HALF, D), BF16)
    chips = (RING,) * 3
    dma = pltpu.SemaphoreType.DMA
    return pl.pallas_call(
        tail_kernel,
        in_specs=[hbm] * 7 + [vmem],
        out_specs=[vmem] * 4,
        out_shape=[S((HALF, D), BF16), S(ln.shape, F32), S((D // 64, 3 * C), F32), S((C // 64, D), F32)],
        scratch_shapes=[V(a.shape, BF16) for a in (ha_t, dqkv_t, ctx_t, dy, wqkv_t)] + [own] * 6
        + [V(chips + (D // 64, 3 * C), F32), V(chips + (C // 64, D), F32), V((2, 8, D), F32), V((3, RING, 8, D), F32)]
        + [dma((9,)), dma((3,)), dma((3,)), dma((3, RING)), dma((3, RING))] + plan_scratch((PLAN_QKV, PLAN_OUT)),
        compiler_params=pltpu.CompilerParams(vmem_limit_bytes=VMEM_LIMIT, collective_id=1, has_side_effects=True),
        cost_estimate=pl.CostEstimate(flops=15 * 10**9, bytes_accessed=30 << 20, transcendentals=0),
        name="tail",
    )(ha_t, dqkv_t, ctx_t, dy, wqkv_t, x, dhm, ln)


def solution(mesh):
    def local_step(x_loc, dy_loc, ln_params, w_qkv, w_out, w_up, w_down):
        x_loc, dy_loc = x_loc[0], dy_loc[0]
        wqkv_t = w_qkv.transpose(1, 2, 3, 0).reshape(-1, x_loc.shape[1])
        cos_t, sin_t = rope_tables()
        ha_t, qkv_t, dctx_t, dhm, dy, g_wup, g_wdown = token_part(x_loc, dy_loc, ln_params, wqkv_t, w_out, w_up, w_down)
        dqkv_t, ctx_t, grad_wup, grad_wdown = attention(qkv_t, dctx_t, cos_t, sin_t, g_wup, g_wdown)
        grad_x, grad_ln, grad_wqkv, grad_wout = tail(ha_t, dqkv_t, ctx_t, dy, wqkv_t, x_loc, dhm, ln_params)
        return grad_x[None], grad_ln, grad_wqkv.reshape((-1,) + w_qkv.shape[1:]), grad_wout, grad_wup, grad_wdown

    act_spec = P('dp', 'tp')
    in_specs = (act_spec, act_spec, P(), P(None, 'tp'), P('tp'), P(None, 'tp'), P('tp'))
    out_specs = (act_spec, P(), P('dp', 'tp'), P(('tp', 'dp')), P('dp', 'tp'), P(('tp', 'dp')))
    return jax.shard_map(local_step, mesh=mesh, in_specs=in_specs, out_specs=out_specs, check_vma=False)
```

```python
import math

import jax
import jax.numpy as jnp
import numpy as np
from jax import lax
from jax.experimental import pallas as pl
from jax.experimental.pallas import tpu as pltpu
from jax.sharding import PartitionSpec as P

NORM_EPS = 1e-5
ROPE_BASE = 10000.0
F32, BF16 = jnp.float32, jnp.bfloat16
LOG2E = math.log2(math.e)
T = 2048
HALF = T // 2
TILE = 256
SMALL = 128
TT = 512
FC = 1024
LANES = 128
VMEM_LIMIT = 63 << 20
AXES = ('z', 'y', 'x')
AXIS_STRIDE = {'z': 16, 'y': 4, 'x': 1}
RING = 4


def dot(a, b):
    return jnp.dot(a, b, preferred_element_type=F32)


def dot_nt(a, b):
    return lax.dot_general(a, b, (((1,), (1,)), ((), ())), preferred_element_type=F32)


def rope_tables():
    inv_freq = ROPE_BASE ** (-2.0 * jnp.arange(32, dtype=F32) / 64)
    angles = inv_freq[:, None] * jnp.arange(T, dtype=F32)[None, :]
    return jnp.cos(angles), jnp.sin(angles)


def ring_place(axis):
    return lax.rem(lax.div(lax.axis_index('dp'), AXIS_STRIDE[axis]), RING)


def ring_chip(axis, ahead):
    place = ring_place(axis)
    return {'dp': lax.axis_index('dp') + (lax.rem(place + ahead, RING) - place) * AXIS_STRIDE[axis]}


def other_core():
    return {'tp': 1 - lax.axis_index('tp')}


def send_to(device, src, dst, send_sem, recv_sem):
    return pltpu.make_async_remote_copy(src_ref=src, dst_ref=dst, send_sem=send_sem, recv_sem=recv_sem,
                                        device_id=device, device_id_type=pl.DeviceIdType.MESH)


def greet(devices):
    barrier = pltpu.get_barrier_semaphore()
    for device in devices:
        pl.semaphore_signal(barrier, inc=1, device_id=device, device_id_type=pl.DeviceIdType.MESH)
    pl.semaphore_wait(barrier, len(devices))


class TorusSum:
    COUNT = 30

    @staticmethod
    def half_shape(rows, width, by_cols):
        return (rows, width // 2) if by_cols else (rows // 2, width)

    @staticmethod
    def scratch(rows, width, by_cols=False):
        half, whole = TorusSum.half_shape(rows, width, by_cols), (rows, width)
        shapes = []
        for lead in ((RING, RING), (RING,), ()):
            shapes += [pltpu.VMEM(lead + half, F32)] * 8 + [pltpu.VMEM(lead + whole, F32)]
        return shapes + [pltpu.SemaphoreType.DMA((18,)), pltpu.SemaphoreType.DMA((18,)), pltpu.SemaphoreType.DMA((3,))]

    def __init__(self, grad, order, rows, col, width, refs, by_cols=False, in_vmem=False):
        self.grad, self.order, self.col, self.by_cols, self.in_vmem = grad, order, col, by_cols, in_vmem
        self.whole, self.half = (rows, width), TorusSum.half_shape(rows, width, by_cols)
        self.cols = pl.ds(col, width)
        self.refs, (self.send, self.recv, self.load) = refs, refs[27:]
        self.kept = [[axis for axis in AXES if axis not in order[:n]] for n in range(3)]

    def bufs(self, phase):
        return self.refs[9 * phase:9 * phase + 9]

    def part(self, which, col=0):
        shape = self.whole if which == 2 else self.half
        start = [0, col]
        if which == 1:
            start[self.by_cols] += self.half[self.by_cols]
        return tuple(pl.ds(first, size) for first, size in zip(start, shape))

    def block(self, phase, ahead, which):
        index = lax.rem(ring_place(self.order[phase]) + ahead, RING)
        lead = tuple(index if axis == self.order[phase] else slice(None) for axis in self.kept[phase])
        if phase == 0:
            return self.grad.at[lead + self.part(which, self.col)]
        return self.refs[9 * phase - 1].at[lead + self.part(which)]

    def load_copy(self, n):
        ahead, which = ((1, 0), (3, 1), (0, 2))[n]
        return pltpu.make_async_copy(self.block(0, ahead, which), self.bufs(0)[6 + n], self.load.at[n])

    def copy(self, phase, n):
        bufs = self.bufs(phase)
        src = bufs[2 + n] if n >= 4 else self.block(phase, *((2, 0), (1, 1), (2, 1), (3, 0))[n])
        chip = ring_chip(self.order[phase], (1, 1, 3, 3, 1, 3)[n])
        return send_to(chip, src, bufs[n], self.send.at[6 * phase + n], self.recv.at[6 * phase + n])

    def loads(self, phase):
        return phase == 0 and not self.in_vmem

    def start(self, phase):
        for n in (0, 2, 1, 3):
            self.copy(phase, n).start()
        if self.loads(phase):
            for n in range(3):
                self.load_copy(n).start()

    def add(self, phase):
        bufs = self.bufs(phase)
        own = self.block(phase, 1, 0), self.block(phase, 3, 1)
        if self.loads(phase):
            own = bufs[6], bufs[7]
            self.load_copy(0).wait()
            self.load_copy(1).wait()
        self.copy(phase, 0).wait_recv()
        self.copy(phase, 2).wait_recv()

        def rows(at):
            bufs[6][at] = own[0][at] + bufs[0][at]
            bufs[7][at] = own[1][at] + bufs[2][at]
        self.each(phase, rows)

    def each(self, phase, body):
        if phase == 0:
            def step(n, carry):
                body(n)
                return carry
            lax.fori_loop(0, RING, step, 0)
        else:
            body(slice(None))

    def pass_on(self, phase):
        self.copy(phase, 4).start()
        self.copy(phase, 5).start()

    def finish(self, phase):
        bufs = self.bufs(phase)
        lead = (slice(None),) * (2 - phase)
        low, high = bufs[8].at[lead + self.part(0)], bufs[8].at[lead + self.part(1)]
        own = self.block(phase, 0, 0), self.block(phase, 0, 1)
        if self.loads(phase):
            own = low, high
            self.load_copy(2).wait()
        for n in (1, 3, 4, 5):
            self.copy(phase, n).wait_recv()

        def rows(at):
            low[at] = own[0][at] + bufs[3][at] + bufs[4][at]
            high[at] = own[1][at] + bufs[1][at] + bufs[5][at]
        self.each(phase, rows)

    def drain(self):
        for phase in range(3):
            for n in range(6):
                self.copy(phase, n).wait_send()

    @property
    def result(self):
        return self.refs[26]


def plan_columns(rows, tiles, by_cols=False):
    plan, col = [], 0
    for order, count in zip((('x', 'y', 'z'), ('y', 'z', 'x'), ('z', 'x', 'y')), tiles):
        plan.append((order, rows, col, count * LANES, by_cols))
        col += count * LANES
    return plan


def plan_scratch(plans):
    return [shape for plan in plans for _, rows, _, width, by_cols in plan for shape in TorusSum.scratch(rows, width, by_cols)]


def plan_sums(grads, plans, refs, in_vmem=False):
    groups = []
    for grad, plan in zip(grads, plans):
        groups.append([])
        for order, rows, col, width, by_cols in plan:
            groups[-1].append(TorusSum(grad, order, rows, col, width, refs[:TorusSum.COUNT], by_cols, in_vmem))
            refs = refs[TorusSum.COUNT:]
    return groups


PLAN_UP = plan_columns(16, (5, 5, 6))
PLAN_DOWN = plan_columns(32, (3, 3, 2))
PLAN_QKV = plan_columns(16, (4, 4, 4))
PLAN_OUT = plan_columns(8, (2, 2, 4), True)


def normed(x):
    x = x.astype(F32)
    centered = x - jnp.mean(x, axis=-1, keepdims=True)
    rstd = lax.rsqrt(jnp.mean(centered * centered, axis=-1, keepdims=True) + NORM_EPS)
    return centered * rstd, rstd


def token_kernel(x_hbm, dy_hbm, ln_ref, wqkv_hbm, wout_hbm, wup_hbm, wdown_hbm,
                 ha_ref, qkv_ref, dctx_ref, dhm_ref, dy_ref, gup_ref, gdown_ref,
                 xs, dys, wqkv, wout, wup, wdown, ha_s, hm_s, hm_t, dh_s, up_acc, down_acc,
                 row_load, w_load, chunk_load, flush_sem, dy_sem, send, recv):
    step = pl.program_id(0)
    first, last = step == 0, step == pl.num_programs(0) - 1
    width = wup.shape[1]
    chunks = width // FC
    rows = pl.ds(pl.multiple_of(step * TT, TT), TT)

    def chunk(c):
        return pl.ds(pl.multiple_of(c * FC, FC), FC)

    def flush(c):
        return (pltpu.make_async_copy(up_acc.at[:, chunk(c)], gup_ref.at[:, chunk(c)], flush_sem.at[0, c]),
                pltpu.make_async_copy(down_acc.at[chunk(c), :], gdown_ref.at[chunk(c), :], flush_sem.at[1, c]))

    def row_loads(n):
        part = pl.ds(n * TT, TT)
        return [pltpu.make_async_copy(src.at[part], dst.at[part], row_load.at[k, n]) for k, (src, dst) in enumerate(((x_hbm, xs), (dy_hbm, dys)))]

    def chunk_loads(c):
        return (pltpu.make_async_copy(wup_hbm.at[:, chunk(c)], wup.at[:, chunk(c)], chunk_load.at[0, c]),
                pltpu.make_async_copy(wdown_hbm.at[chunk(c), :], wdown.at[chunk(c), :], chunk_load.at[1, c]))

    core = lax.axis_index('tp')
    dy_saves = [pltpu.make_async_copy(dys.at[pl.ds(n * HALF, HALF)], dy_ref.at[pl.ds(place * HALF, HALF)], dy_sem.at[n])
                for n, place in enumerate((core, 1 - core))]
    w_loads = [pltpu.make_async_copy(src, dst, w_load.at[k]) for k, (src, dst) in enumerate(((wqkv_hbm, wqkv), (wout_hbm, wout)))]
    swaps = [send_to(other_core(), src, dst.at[pl.ds(HALF, HALF)], send.at[k], recv.at[k]) for k, (src, dst) in enumerate(((x_hbm, xs), (dy_hbm, dys)))]

    @pl.when(first)
    def _():
        for copy in [*row_loads(0), *(copy for c in range(chunks) for copy in chunk_loads(c)), *w_loads, *row_loads(1)]:
            copy.start()
        up_acc[:] = jnp.zeros_like(up_acc)
        down_acc[:] = jnp.zeros_like(down_acc)
        greet([other_core()])
        for copy in swaps:
            copy.start()

    def norms(n):
        norm, _ = normed(xs[pl.ds(pl.multiple_of(n * TT, TT), TT), :])
        hm = (norm * ln_ref[pl.ds(2, 1), :] + ln_ref[pl.ds(3, 1), :]).astype(BF16)
        ha_s[:] = (norm * ln_ref[pl.ds(0, 1), :] + ln_ref[pl.ds(1, 1), :]).astype(BF16).T
        hm_s[:] = hm
        hm_t[:] = hm.T

    @pl.when(first)
    def _():
        for copy in row_loads(0):
            copy.wait()
        norms(0)

    ha_ref[:] = ha_s[:]

    def columns(c, carry):
        @pl.when(first)
        def _():
            for copy in chunk_loads(c):
                copy.wait()
        cols = chunk(c)
        u = dot(hm_s[:], wup[:, cols]).astype(BF16).astype(F32)
        dg = dot_nt(dys[rows, :], wdown[cols, :]).astype(BF16).astype(F32)
        cdf = 0.5 * (1.0 + lax.erf(u * math.sqrt(0.5)))
        gelu = (u * cdf).astype(BF16)
        pdf = jnp.exp(-0.5 * u * u) * (1.0 / math.sqrt(2.0 * math.pi))
        dh = (dg * (cdf + u * pdf)).astype(BF16)
        dh_s[:, cols] = dh
        down_acc[cols, :] += dot(gelu.T, dys[rows, :])
        up_acc[:, cols] += dot(hm_t[:], dh)

        @pl.when(last)
        def _():
            for copy in flush(c):
                copy.start()
        return carry
    lax.fori_loop(0, chunks, columns, 0)
    @pl.when(first)
    def _():
        for copy in w_loads:
            copy.wait()
    for n in range(1, HALF // TT):
        @pl.when(step == n - 1)
        def _(n=n):
            for copy in row_loads(n):
                copy.wait()

    @pl.when(step == HALF // TT - 1)
    def _():
        for copy in swaps:
            copy.wait_recv()
        for copy in dy_saves:
            copy.start()

    dhm_ref[:] = dot_nt(dh_s[:], wup[:]).astype(BF16)
    norms(jnp.minimum(step + 1, pl.num_programs(0) - 1))
    qkv_ref[:] = dot(wqkv[:], ha_ref[:]).astype(BF16)
    dctx_ref[:] = dot_nt(wout[:], dys[rows, :]).astype(BF16)

    @pl.when(last)
    def _():
        for copy in swaps:
            copy.wait_send()
        for copy in dy_saves:
            copy.wait()
        for c in range(chunks):
            for copy in flush(c):
                copy.wait()


def token_part(x, dy, ln, wqkv_t, wout, wup, wdown):
    D, width = wup.shape
    S, V, dma = jax.ShapeDtypeStruct, pltpu.VMEM, pltpu.SemaphoreType.DMA
    hbm = pl.BlockSpec(memory_space=pl.ANY)
    steps, halves = T // TT, HALF // TT

    def tile(i):
        core = lax.axis_index('tp')
        return jnp.where(i < halves, core * halves + i, (1 - core) * halves + i - halves)

    def tok(size):
        return pl.BlockSpec((TT, size), lambda i: (tile(i), 0))

    def col(size):
        return pl.BlockSpec((size, TT), lambda i: (0, tile(i)))

    return pl.pallas_call(
        token_kernel,
        grid=(steps,),
        in_specs=[hbm, hbm, pl.BlockSpec(memory_space=pltpu.VMEM)] + [hbm] * 4,
        out_specs=[col(D), col(wqkv_t.shape[0]), col(wout.shape[0]), tok(D), hbm, hbm, hbm],
        out_shape=[S((D, T), BF16), S((wqkv_t.shape[0], T), BF16), S((wout.shape[0], T), BF16), S((T, D), BF16), S((T, D), BF16),
                   S((D, width), F32), S((width, D), F32)],
        scratch_shapes=[V((T, D), BF16)] * 2 + [V(w.shape, BF16) for w in (wqkv_t, wout, wup, wdown)]
        + [V((D, TT), BF16), V((TT, D), BF16), V((D, TT), BF16), V((TT, width), BF16), V((D, width), F32), V((width, D), F32)]
        + [dma((2, halves)), dma((2,)), dma((2, width // FC)), dma((2, width // FC)), dma((2,)), dma((2,)), dma((2,))],
        compiler_params=pltpu.CompilerParams(dimension_semantics=("arbitrary",), vmem_limit_bytes=VMEM_LIMIT,
                                             collective_id=2, has_side_effects=True),
        cost_estimate=pl.CostEstimate(flops=52 * 10**9, bytes_accessed=60 << 20, transcendentals=2 * T * width),
        name="token_part",
    )(x, dy, ln, wqkv_t, wout, wup, wdown)


def attention_pair(qkv_ref, dctx_ref, cos_ref, sin_ref, dqkv_ref, ctx_ref, q_t, k_t, q_n, k_n, v_n, do_n, p_s, dp_s, dk_acc, dv_acc, slot):
    lane = lax.broadcasted_iota(jnp.int32, (TILE, PAIR), 1)
    key = lax.broadcasted_iota(jnp.int32, (TILE, 2 * TILE), 0)
    query = lax.broadcasted_iota(jnp.int32, (TILE, 2 * TILE), 1) % TILE

    def tile_at(j):
        return pl.ds(j * TILE, TILE)

    def head_rows(head, part):
        return pl.ds((3 * head + part) * HEAD, HEAD)

    def halves(x):
        return x[:HEAD // 2].astype(F32), x[HEAD // 2:].astype(F32)

    def rotate(x, cols, sign):
        cos, sin = cos_ref[:, cols], sin_ref[:, cols] * sign
        lo, hi = halves(x)
        return jnp.concatenate([lo * cos - hi * sin, hi * cos + lo * sin], axis=0).astype(BF16)

    def prepare(j):
        cols = tile_at(j)
        for head in range(2):
            rows = pl.ds(head * HEAD, HEAD)
            q_t[rows, cols] = rotate(qkv_ref[head_rows(head, 0), cols], cols, 1.0) * jnp.asarray(HEAD ** -0.5, BF16)
            k_t[rows, cols] = rotate(qkv_ref[head_rows(head, 1), cols], cols, 1.0)
        q_n[cols, :] = q_t[:, cols].T
        k_n[cols, :] = k_t[:, cols].T
        v_n[cols, :] = jnp.concatenate([qkv_ref[head_rows(head, 2), cols] for head in range(2)], axis=0).T
        do_n[cols, :] = dctx_ref[:, cols].T

    def split_lanes(x):
        zero = jnp.zeros_like(x)
        return jnp.concatenate([jnp.where(lane < HEAD, x, zero), jnp.where(lane < HEAD, zero, x)], axis=0)

    def split_rows(x):
        zero = jnp.zeros((HEAD, TILE), x.dtype)
        return jnp.concatenate([jnp.concatenate([x[:HEAD], zero], axis=1), jnp.concatenate([zero, x[HEAD:]], axis=1)], axis=0)

    def fold(x, op):
        parts = [x[r:r + 8] for r in range(0, TILE, 8)]
        while len(parts) > 1:
            parts = [op(a, b) for a, b in zip(parts[::2], parts[1::2])]
        return parts[0]

    def gather(old, new, op):
        return new if old is None else op(old, new)

    blocks = list(reversed(range(T // TILE)))
    before = {i: sum(b + 1 for b in blocks[:n]) for n, i in enumerate(blocks)}

    def p_at(i, j):
        return pl.ds((before[i] + j) % P_TILES * TILE, TILE)

    def dp_at(i, j):
        return pl.ds((before[i] + j) % DP_TILES * TILE, TILE)

    def scores(i, state):
        q_split = split_rows(q_t[:, tile_at(i)])
        top = None
        for j in range(i + 1):
            s = dot(k_n[tile_at(j), :], q_split)
            if j == i:
                s = jnp.where(query >= key, s, -1e30)
            p_s[p_at(i, j), :] = s
            top = gather(top, fold(s, jnp.maximum), jnp.maximum)
            if j == i:
                state['max'] = jnp.max(top, axis=0, keepdims=True)
            yield

    def weights(i, state):
        do_split = split_rows(dctx_ref[:, tile_at(i)])
        total = both = None
        for j in range(i + 1):
            dp = dot(v_n[tile_at(j), :], do_split).astype(BF16)
            dp_s[dp_at(i, j), :] = dp
            p = jnp.exp2((p_s[p_at(i, j), :] - state['max']) * LOG2E)
            p_s[p_at(i, j), :] = p
            total = gather(total, fold(p, jnp.add), jnp.add)
            both = gather(both, fold(p * dp.astype(F32), jnp.add), jnp.add)
            if j == i:
                state['inv'] = 1.0 / jnp.sum(total, axis=0, keepdims=True)
                state['delta'] = jnp.sum(both, axis=0, keepdims=True) * state['inv']
            yield

    def grads(i, state):
        cols = tile_at(i)
        q_pair, do_pair = split_lanes(q_n[cols, :]), split_lanes(do_n[cols, :])
        ctx, dq = [None] * 2, [None] * 2
        for j in range(i + 1):
            keys = tile_at(j)
            p = p_s[p_at(i, j), :] * state['inv']
            p_bf = p.astype(BF16)
            ds_bf = (p * (dp_s[dp_at(i, j), :].astype(F32) - state['delta'])).astype(BF16)
            for head in range(2):
                side = slice(head * TILE, (head + 1) * TILE)
                ctx[head] = gather(ctx[head], dot(qkv_ref[head_rows(head, 2), keys], p_bf[:, side]), jnp.add)
                dq[head] = gather(dq[head], dot(k_t[pl.ds(head * HEAD, HEAD), keys], ds_bf[:, side]), jnp.add)
            for acc, new in ((dv_acc, dot(p_bf, do_pair)), (dk_acc, dot(ds_bf, q_pair))):
                acc[keys, :] = new if i == blocks[0] else acc[keys, :] + new
            if j == i:
                dk, dv = dk_acc[cols, :].astype(BF16).T, dv_acc[cols, :].astype(BF16).T
                for head in range(2):
                    rows = pl.ds(head * HEAD, HEAD)
                    side = slice(head * HEAD, (head + 1) * HEAD)
                    ctx_ref[rows, cols] = ctx[head].astype(BF16)
                    dqkv_ref[head_rows(head, 0), cols] = rotate((dq[head] * HEAD ** -0.5).astype(BF16), cols, -1.0)
                    dqkv_ref[head_rows(head, 1), cols] = rotate(dk[side], cols, -1.0)
                    dqkv_ref[head_rows(head, 2), cols] = dv[side]
            yield

    slot(0)
    for j in range(T // TILE):
        prepare(j)
    states = {i: {} for i in blocks}
    for n in range(len(blocks) + 2):
        work = []
        for stage, make in ((n - 2, grads), (n - 1, weights), (n, scores)):
            if 0 <= stage < len(blocks):
                i = blocks[stage]
                run = make(i, states[i])
                work += [((j + 0.5) / (i + 1), run) for j in range(i + 1)]
        for _, run in sorted(work, key=lambda item: item[0]):
            next(run)
        if n in SLOT_AFTER:
            slot(SLOT_AFTER[n])


P_TILES, DP_TILES = 21, 15
SLOT_AFTER = {2: 1, 4: 2, 6: 3, 9: 4}
HEAD, PAIR = 64, 128


def attention_scratch():
    V = pltpu.VMEM
    return [V((PAIR, T), BF16)] * 2 + [V((T, PAIR), BF16)] * 4 + [V((P_TILES * TILE, 2 * TILE), F32), V((DP_TILES * TILE, 2 * TILE), BF16)] \
        + [V((T, PAIR), F32)] * 2


SCHEDULE = {
    (0, 0): (('start', 0),),
    (1, 3): (('add', 0), ('pass_on', 0)),
    (2, 3): (('finish', 0), ('start', 1)),
    (3, 1): (('add', 1), ('pass_on', 1)),
    (3, 2): (('finish', 1), ('start', 2)),
    (3, 3): (('add', 2), ('pass_on', 2)),
    (3, 4): (('finish', 2),),
}


def attention_kernel(qkv_ref, dctx_ref, cos_ref, sin_ref, up_ref, down_ref, dqkv_ref, ctx_ref, up_out, down_out, *refs):
    count = len(attention_scratch())
    groups = plan_sums((up_ref, down_ref), (PLAN_UP, PLAN_DOWN), refs[count:])
    every = groups[0] + groups[1]

    def slot(place):
        for (pair, at), stages in SCHEDULE.items():
            if at != place:
                continue

            @pl.when(pl.program_id(0) == pair)
            def _(pair=pair, stages=stages):
                if (pair, place) == (0, 0):
                    greet([ring_chip(axis, ahead) for axis in AXES for ahead in (1, 3)])
                for stage, phase in stages:
                    for one in every:
                        getattr(one, stage)(phase)
                if (pair, place) == list(SCHEDULE)[-1]:
                    for out, sums in zip((up_out, down_out), groups):
                        for one in sums:
                            out[:, one.cols] = one.result[:]
                            one.drain()

    attention_pair(qkv_ref, dctx_ref, cos_ref, sin_ref, dqkv_ref, ctx_ref, *refs[:count], slot)


def attention(qkv_t, dctx_t, cos_t, sin_t, g_up, g_down):
    pairs = dctx_t.shape[0] // PAIR
    S = jax.ShapeDtypeStruct
    shares = [(g.shape[0] // 64, g.shape[1]) for g in (g_up, g_down)]
    hbm = pl.BlockSpec(memory_space=pl.ANY)

    def by_pair(rows):
        return pl.BlockSpec((rows, T), lambda p: (p, 0))

    def fixed(shape):
        return pl.BlockSpec(shape, lambda p: (0, 0), pipeline_mode=pl.Buffered(1))

    return pl.pallas_call(
        attention_kernel,
        grid=(pairs,),
        in_specs=[by_pair(3 * PAIR), by_pair(PAIR), fixed(cos_t.shape), fixed(sin_t.shape), hbm, hbm],
        out_specs=[by_pair(3 * PAIR), by_pair(PAIR)] + [fixed(share) for share in shares],
        out_shape=[S(qkv_t.shape, BF16), S(dctx_t.shape, BF16)] + [S(share, F32) for share in shares],
        scratch_shapes=attention_scratch() + plan_scratch((PLAN_UP, PLAN_DOWN)),
        compiler_params=pltpu.CompilerParams(dimension_semantics=("arbitrary",), vmem_limit_bytes=VMEM_LIMIT,
                                             collective_id=0, has_side_effects=True),
        cost_estimate=pl.CostEstimate(flops=80 * 10**9, bytes_accessed=20 << 20, transcendentals=8 * T * T // 2),
        name="attention",
    )(qkv_t, dctx_t, cos_t, sin_t, *(g.reshape((RING,) * 3 + (-1, g.shape[1])) for g in (g_up, g_down)))


def tail_kernel(hat_hbm, dqkv_hbm, ctx_hbm, dy_hbm, w_hbm, x_hbm, dhm_hbm, ln_ref, gx_ref, gln_ref, gqkv_ref, gout_ref,
                hat, dqkv, ctx, dy, w, x, dhm_own, dhm_in, dha_s, dha_in, g_qkv, g_out, pair_s, ring_s,
                load, send, recv, ring_send, ring_recv, *sum_refs):
    core = lax.axis_index('tp')
    own, away = core * HALF, (1 - core) * HALF
    qkv_sums, out_sums = plan_sums((g_qkv, g_out), (PLAN_QKV, PLAN_OUT), sum_refs, True)
    every = qkv_sums + out_sums
    block = dqkv.shape[0] // len(qkv_sums)

    def rows_of(ref, start, size):
        return ref.at[pl.ds(start, size)]

    pieces = [(hat_hbm, hat)] + [(rows_of(dqkv_hbm, n * block, block), rows_of(dqkv, n * block, block)) for n in range(3)]
    pieces += [(ctx_hbm, ctx), (dy_hbm, dy), (w_hbm, w), (x_hbm, x), (rows_of(dhm_hbm, own, HALF), dhm_own)]
    loads = [pltpu.make_async_copy(src, dst, load.at[n]) for n, (src, dst) in enumerate(pieces)]
    for copy in loads:
        copy.start()
    greet([ring_chip(axis, ahead) for axis in AXES for ahead in (1, 2, 3)] + [other_core()])
    dhm_copy = send_to(other_core(), rows_of(dhm_hbm, away, HALF), dhm_in, send.at[0], recv.at[0])
    dha_copy = send_to(other_core(), dha_s.at[0], dha_in, send.at[1], recv.at[1])
    pair_copy = send_to(other_core(), pair_s.at[0], pair_s.at[1], send.at[2], recv.at[2])
    dhm_copy.start()

    loads[0].wait()
    per_group = block // TILE

    def columns(k, carry):
        for n in range(len(qkv_sums)):
            @pl.when(k == n * per_group)
            def _(n=n):
                loads[1 + n].wait()
        cols = pl.ds(pl.multiple_of(k * TILE, TILE), TILE)
        g_qkv[:, :, :, :, cols] = dot_nt(hat[:], dqkv[cols, :]).reshape(g_qkv.shape[:4] + (TILE,))
        for n, one in enumerate(qkv_sums):
            @pl.when(k == (n + 1) * per_group - 1)
            def _(one=one):
                one.start(0)
        return carry
    lax.fori_loop(0, len(qkv_sums) * per_group, columns, 0)
    loads[4].wait()
    loads[5].wait()

    def out_columns(k, carry):
        cols = pl.ds(pl.multiple_of(k * TILE, TILE), TILE)
        g_out[:, :, :, :, cols] = dot(ctx[:], dy[:, cols]).reshape(g_out.shape[:4] + (TILE,))
        return carry
    lax.fori_loop(0, dy.shape[1] // TILE, out_columns, 0)
    for one in out_sums:
        one.start(0)

    loads[6].wait()
    tiles = HALF // TILE

    def tokens(k, carry):
        mine = lax.div(k, tiles)
        at = lax.rem(k, tiles) * TILE
        cols = pl.ds(pl.multiple_of(jnp.where(mine == 0, away, own) + at, TILE), TILE)
        dha_s[mine, pl.ds(pl.multiple_of(at, TILE), TILE), :] = dot(dqkv[:, cols].T, w[:]).astype(BF16)

        @pl.when(k == tiles - 1)
        def _():
            dha_copy.start()
        return carry
    lax.fori_loop(0, 2 * tiles, tokens, 0)

    def stages(sums, phase, *names):
        for name in names:
            for one in sums:
                getattr(one, name)(phase)

    stages(qkv_sums, 0, 'add', 'pass_on')
    loads[7].wait()
    loads[8].wait()
    dhm_copy.wait_recv()
    dha_copy.wait_recv()
    pair_s[0] = jnp.zeros_like(pair_s[0])

    def norm_back(k, carry):
        at = pl.ds(pl.multiple_of(k * SMALL, SMALL), SMALL)
        norm, rstd = normed(x[at, :])
        da = (dha_s[1, at, :].astype(F32) + dha_in[at, :].astype(F32)).astype(BF16).astype(F32)
        dm = (dhm_own[at, :].astype(F32) + dhm_in[at, :].astype(F32)).astype(BF16).astype(F32)
        g = da * ln_ref[pl.ds(0, 1), :] + dm * ln_ref[pl.ds(2, 1), :]
        mean_g = jnp.mean(g, axis=-1, keepdims=True)
        mean_gn = jnp.mean(g * norm, axis=-1, keepdims=True)
        residual = dy[pl.ds(pl.multiple_of(own + k * SMALL, SMALL), SMALL), :].astype(F32)
        gx_ref[at, :] = (residual + rstd * (g - mean_g - norm * mean_gn)).astype(BF16)
        for row, value in enumerate((da * norm, da, dm * norm, dm)):
            pair_s[0, pl.ds(row, 1), :] += jnp.sum(value, axis=0, keepdims=True)
        return carry

    steps = HALF // SMALL

    def norm_step(k, carry):
        @pl.when(k == steps // 2)
        def _():
            stages(out_sums, 0, 'add', 'pass_on')
            stages(qkv_sums, 0, 'finish')
            stages(qkv_sums, 1, 'start')
        return norm_back(k, carry)
    lax.fori_loop(0, steps, norm_step, 0)
    pair_copy.start()
    stages(out_sums, 0, 'finish')
    stages(out_sums, 1, 'start')
    stages(qkv_sums, 1, 'add', 'pass_on')
    stages(out_sums, 1, 'add', 'pass_on')

    def ring_copies(phase):
        place = ring_place(AXES[phase])
        return [send_to(ring_chip(AXES[phase], ahead), ring_s.at[phase, place], ring_s.at[phase, place],
                        ring_send.at[phase, ahead], ring_recv.at[phase, ahead]) for ahead in (1, 2, 3)]

    def ring_start(phase, value):
        ring_s[phase, ring_place(AXES[phase])] = value
        for copy in ring_copies(phase):
            copy.start()

    def ring_sum(phase):
        for copy in ring_copies(phase):
            copy.wait_recv()
        return ring_s[phase, 0] + ring_s[phase, 1] + ring_s[phase, 2] + ring_s[phase, 3]

    pair_copy.wait_recv()
    ring_start(0, pair_s[0] + pair_s[1])
    stages(every, 1, 'finish')
    stages(every, 2, 'start')
    ring_start(1, ring_sum(0))
    stages(every, 2, 'add', 'pass_on')
    ring_start(2, ring_sum(1))
    stages(every, 2, 'finish')
    gln_ref[:] = ring_sum(2)[:gln_ref.shape[0]]
    for out, sums in ((gqkv_ref, qkv_sums), (gout_ref, out_sums)):
        for one in sums:
            out[:, one.cols] = one.result[:]
            one.drain()
    for copy in (dhm_copy, dha_copy, pair_copy):
        copy.wait_send()
    for phase in range(3):
        for copy in ring_copies(phase):
            copy.wait_send()


def tail(ha_t, dqkv_t, ctx_t, dy, wqkv_t, x, dhm, ln):
    D, C = ha_t.shape[0], ctx_t.shape[0]
    S, V = jax.ShapeDtypeStruct, pltpu.VMEM
    hbm, vmem = pl.BlockSpec(memory_space=pl.ANY), pl.BlockSpec(memory_space=pltpu.VMEM)
    own = V((HALF, D), BF16)
    chips = (RING,) * 3
    dma = pltpu.SemaphoreType.DMA
    return pl.pallas_call(
        tail_kernel,
        in_specs=[hbm] * 7 + [vmem],
        out_specs=[vmem] * 4,
        out_shape=[S((HALF, D), BF16), S(ln.shape, F32), S((D // 64, 3 * C), F32), S((C // 64, D), F32)],
        scratch_shapes=[V(a.shape, BF16) for a in (ha_t, dqkv_t, ctx_t, dy, wqkv_t)] + [own] * 3 + [V((2, HALF, D), BF16), own]
        + [V(chips + (D // 64, 3 * C), F32), V(chips + (C // 64, D), F32), V((2, 8, D), F32), V((3, RING, 8, D), F32)]
        + [dma((9,)), dma((3,)), dma((3,)), dma((3, RING)), dma((3, RING))] + plan_scratch((PLAN_QKV, PLAN_OUT)),
        compiler_params=pltpu.CompilerParams(vmem_limit_bytes=VMEM_LIMIT, collective_id=1, has_side_effects=True),
        cost_estimate=pl.CostEstimate(flops=15 * 10**9, bytes_accessed=30 << 20, transcendentals=0),
        name="tail",
    )(ha_t, dqkv_t, ctx_t, dy, wqkv_t, x, dhm, ln)


def output_kernel(*refs):
    ins, outs = refs[:len(refs) // 2], refs[len(refs) // 2:]
    outs[0][:] = ins[0][:]

    @pl.when(pl.program_id(0) == 0)
    def _():
        for src, dst in zip(ins[2:], outs[2:]):
            dst[:] = src[:]
        wide, split = ins[1], outs[1]
        for group in range(split.shape[2]):
            for part in range(3):
                split[:, part, group, :] = wide[:, pl.ds((3 * group + part) * HEAD, HEAD)]


def outputs(grad_x, grad_wqkv, *rest):
    rows, cols = grad_wqkv.shape
    split = jax.ShapeDtypeStruct((rows, 3, cols // (3 * HEAD), HEAD), F32)
    shapes = [grad_x, split, *rest]
    steps = 4

    def fixed(a):
        return pl.BlockSpec(a.shape, lambda i: (0,) * len(a.shape), pipeline_mode=pl.Buffered(1))

    tok = pl.BlockSpec((grad_x.shape[0] // steps, grad_x.shape[1]), lambda i: (i, 0))
    return pl.pallas_call(
        output_kernel, grid=(steps,),
        in_specs=[tok, fixed(grad_wqkv)] + [fixed(a) for a in rest],
        out_specs=[tok, fixed(split)] + [fixed(a) for a in rest],
        out_shape=[jax.ShapeDtypeStruct(a.shape, a.dtype) for a in shapes],
        compiler_params=pltpu.CompilerParams(dimension_semantics=("arbitrary",)),
        name="outputs",
    )(grad_x, grad_wqkv, *rest)


def solution(mesh):
    def local_step(x_loc, dy_loc, ln_params, w_qkv, w_out, w_up, w_down):
        x_loc, dy_loc = x_loc[0], dy_loc[0]
        wqkv_t = w_qkv.transpose(1, 2, 3, 0).reshape(-1, x_loc.shape[1])
        cos_t, sin_t = rope_tables()
        ha_t, qkv_t, dctx_t, dhm, dy, g_wup, g_wdown = token_part(x_loc, dy_loc, ln_params, wqkv_t, w_out, w_up, w_down)
        dqkv_t, ctx_t, grad_wup, grad_wdown = attention(qkv_t, dctx_t, cos_t, sin_t, g_wup, g_wdown)
        grad_x, grad_ln, grad_wqkv, grad_wout = tail(ha_t, dqkv_t, ctx_t, dy, wqkv_t, x_loc, dhm, ln_params)
        grad_x, grad_wqkv, *rest = outputs(grad_x, grad_wqkv, grad_ln, grad_wout, grad_wup, grad_wdown)
        return grad_x[None], rest[0], grad_wqkv.swapaxes(1, 2), *rest[1:]

    act_spec = P('dp', 'tp')
    in_specs = (act_spec, act_spec, P(), P(None, 'tp'), P('tp'), P(None, 'tp'), P('tp'))
    out_specs = (act_spec, P(), P('dp', 'tp'), P(('tp', 'dp')), P('dp', 'tp'), P(('tp', 'dp')))
    return jax.shard_map(local_step, mesh=mesh, in_specs=in_specs, out_specs=out_specs, check_vma=False)
```

```python
import math

import jax
import jax.numpy as jnp
import numpy as np
from jax import lax
from jax.experimental import pallas as pl
from jax.experimental.pallas import tpu as pltpu
from jax.sharding import PartitionSpec as P

NORM_EPS = 1e-5
ROPE_BASE = 10000.0
F32, BF16 = jnp.float32, jnp.bfloat16
LOG2E = math.log2(math.e)
T = 2048
HALF = T // 2
TILE = 256
SMALL = 128
TT = 512
FC = 1024
LANES = 128
HEAD, PAIR = 64, 128
VMEM_LIMIT = 63 << 20
AXES = ('z', 'y', 'x')
AXIS_STRIDE = {'z': 16, 'y': 4, 'x': 1}
RING = 4


def dot(a, b):
    return jnp.dot(a, b, preferred_element_type=F32)


def dot_nt(a, b):
    return lax.dot_general(a, b, (((1,), (1,)), ((), ())), preferred_element_type=F32)


def ring_place(axis):
    return lax.rem(lax.div(lax.axis_index('dp'), AXIS_STRIDE[axis]), RING)


def ring_chip(axis, ahead):
    place = ring_place(axis)
    return {'dp': lax.axis_index('dp') + (lax.rem(place + ahead, RING) - place) * AXIS_STRIDE[axis]}


def other_core():
    return {'tp': 1 - lax.axis_index('tp')}


def send_to(device, src, dst, send_sem, recv_sem):
    return pltpu.make_async_remote_copy(src_ref=src, dst_ref=dst, send_sem=send_sem, recv_sem=recv_sem,
                                        device_id=device, device_id_type=pl.DeviceIdType.MESH)


def greet(devices):
    barrier = pltpu.get_barrier_semaphore()
    for device in devices:
        pl.semaphore_signal(barrier, inc=1, device_id=device, device_id_type=pl.DeviceIdType.MESH)
    pl.semaphore_wait(barrier, len(devices))


class TorusSum:
    COUNT = 30

    @staticmethod
    def half_shape(rows, width, by_cols):
        return (rows, width // 2) if by_cols else (rows // 2, width)

    @staticmethod
    def scratch(rows, width, by_cols=False):
        half, whole = TorusSum.half_shape(rows, width, by_cols), (rows, width)
        shapes = []
        for lead in ((RING, RING), (RING,), ()):
            shapes += [pltpu.VMEM(lead + half, F32)] * 8 + [pltpu.VMEM(lead + whole, F32)]
        return shapes + [pltpu.SemaphoreType.DMA((18,)), pltpu.SemaphoreType.DMA((18,)), pltpu.SemaphoreType.DMA((3,))]

    def __init__(self, grad, order, rows, col, width, refs, by_cols=False, in_vmem=False):
        self.grad, self.order, self.col, self.by_cols, self.in_vmem = grad, order, col, by_cols, in_vmem
        self.whole, self.half = (rows, width), TorusSum.half_shape(rows, width, by_cols)
        self.cols = pl.ds(col, width)
        self.refs, (self.send, self.recv, self.load) = refs, refs[27:]
        self.kept = [[axis for axis in AXES if axis not in order[:n]] for n in range(3)]

    def bufs(self, phase):
        return self.refs[9 * phase:9 * phase + 9]

    def part(self, which, col=0):
        shape = self.whole if which == 2 else self.half
        start = [0, col]
        if which == 1:
            start[self.by_cols] += self.half[self.by_cols]
        return tuple(pl.ds(first, size) for first, size in zip(start, shape))

    def block(self, phase, ahead, which):
        index = lax.rem(ring_place(self.order[phase]) + ahead, RING)
        lead = tuple(index if axis == self.order[phase] else slice(None) for axis in self.kept[phase])
        if phase == 0:
            return self.grad.at[lead + self.part(which, self.col)]
        return self.refs[9 * phase - 1].at[lead + self.part(which)]

    def load_copy(self, n):
        ahead, which = ((1, 0), (3, 1), (0, 2))[n]
        return pltpu.make_async_copy(self.block(0, ahead, which), self.bufs(0)[6 + n], self.load.at[n])

    def copy(self, phase, n):
        bufs = self.bufs(phase)
        src = bufs[2 + n] if n >= 4 else self.block(phase, *((2, 0), (1, 1), (2, 1), (3, 0))[n])
        chip = ring_chip(self.order[phase], (1, 1, 3, 3, 1, 3)[n])
        return send_to(chip, src, bufs[n], self.send.at[6 * phase + n], self.recv.at[6 * phase + n])

    def loads(self, phase):
        return phase == 0 and not self.in_vmem

    def start(self, phase):
        for n in (0, 2, 1, 3):
            self.copy(phase, n).start()
        if self.loads(phase):
            for n in range(3):
                self.load_copy(n).start()

    def add(self, phase):
        bufs = self.bufs(phase)
        own = self.block(phase, 1, 0), self.block(phase, 3, 1)
        if self.loads(phase):
            own = bufs[6], bufs[7]
            self.load_copy(0).wait()
            self.load_copy(1).wait()
        self.copy(phase, 0).wait_recv()
        self.copy(phase, 2).wait_recv()

        def rows(at):
            bufs[6][at] = own[0][at] + bufs[0][at]
            bufs[7][at] = own[1][at] + bufs[2][at]
        self.each(phase, rows)

    def each(self, phase, body):
        if phase == 0:
            def step(n, carry):
                body(n)
                return carry
            lax.fori_loop(0, RING, step, 0)
        else:
            body(slice(None))

    def pass_on(self, phase):
        self.copy(phase, 4).start()
        self.copy(phase, 5).start()

    def finish(self, phase):
        bufs = self.bufs(phase)
        lead = (slice(None),) * (2 - phase)
        low, high = bufs[8].at[lead + self.part(0)], bufs[8].at[lead + self.part(1)]
        own = self.block(phase, 0, 0), self.block(phase, 0, 1)
        if self.loads(phase):
            own = low, high
            self.load_copy(2).wait()
        for n in (1, 3, 4, 5):
            self.copy(phase, n).wait_recv()

        def rows(at):
            low[at] = own[0][at] + bufs[3][at] + bufs[4][at]
            high[at] = own[1][at] + bufs[1][at] + bufs[5][at]
        self.each(phase, rows)

    def drain(self):
        for phase in range(3):
            for n in range(6):
                self.copy(phase, n).wait_send()

    @property
    def result(self):
        return self.refs[26]


def plan_columns(rows, tiles, by_cols=False):
    plan, col = [], 0
    for order, count in zip((('x', 'y', 'z'), ('y', 'z', 'x'), ('z', 'x', 'y')), tiles):
        plan.append((order, rows, col, count * LANES, by_cols))
        col += count * LANES
    return plan


def plan_scratch(plans):
    return [shape for plan in plans for _, rows, _, width, by_cols in plan for shape in TorusSum.scratch(rows, width, by_cols)]


def plan_sums(grads, plans, refs, in_vmem=False):
    groups = []
    for grad, plan in zip(grads, plans):
        groups.append([])
        for order, rows, col, width, by_cols in plan:
            groups[-1].append(TorusSum(grad, order, rows, col, width, refs[:TorusSum.COUNT], by_cols, in_vmem))
            refs = refs[TorusSum.COUNT:]
    return groups


PLAN_UP = plan_columns(16, (5, 5, 6))
PLAN_DOWN = plan_columns(32, (3, 3, 2))
PLAN_QKV = plan_columns(16, (4, 4, 4))
PLAN_OUT = plan_columns(8, (4, 2, 2), True)


def normed(x):
    x = x.astype(F32)
    centered = x - jnp.mean(x, axis=-1, keepdims=True)
    rstd = lax.rsqrt(jnp.mean(centered * centered, axis=-1, keepdims=True) + NORM_EPS)
    return centered * rstd, rstd


def token_tile(step):
    core, halves = lax.axis_index('tp'), HALF // TT
    return jnp.where(step < halves, core * halves + step, (1 - core) * halves + step - halves)


def token_kernel(x_hbm, dy_hbm, ln_ref, freq_ref, wqkv_hbm, wout_hbm, wup_hbm, wdown_hbm,
                 ha_ref, qkv_ref, dctx_ref, dhm_ref, cos_ref, sin_ref, dy_ref, gup_ref, gdown_ref,
                 xs, dys, wqkv, wout, wup, wdown, ha_s, hm_s, hm_t, dh_s, up_acc, down_acc,
                 row_load, w_load, chunk_load, flush_sem, dy_sem, send, recv):
    step = pl.program_id(0)
    first, last = step == 0, step == pl.num_programs(0) - 1
    width = wup.shape[1]
    chunks = width // FC
    rows = pl.ds(pl.multiple_of(step * TT, TT), TT)

    def chunk(c):
        return pl.ds(pl.multiple_of(c * FC, FC), FC)

    def flush(c):
        return (pltpu.make_async_copy(up_acc.at[:, chunk(c)], gup_ref.at[:, chunk(c)], flush_sem.at[0, c]),
                pltpu.make_async_copy(down_acc.at[chunk(c), :], gdown_ref.at[chunk(c), :], flush_sem.at[1, c]))

    def row_loads(n):
        part = pl.ds(n * TT, TT)
        return [pltpu.make_async_copy(src.at[part], dst.at[part], row_load.at[k, n]) for k, (src, dst) in enumerate(((x_hbm, xs), (dy_hbm, dys)))]

    def chunk_loads(c):
        return (pltpu.make_async_copy(wup_hbm.at[:, chunk(c)], wup.at[:, chunk(c)], chunk_load.at[0, c]),
                pltpu.make_async_copy(wdown_hbm.at[chunk(c), :], wdown.at[chunk(c), :], chunk_load.at[1, c]))

    core = lax.axis_index('tp')
    dy_saves = [pltpu.make_async_copy(dys.at[pl.ds(n * HALF, HALF)], dy_ref.at[pl.ds(place * HALF, HALF)], dy_sem.at[n])
                for n, place in enumerate((core, 1 - core))]
    w_loads = [pltpu.make_async_copy(src, dst, w_load.at[k]) for k, (src, dst) in enumerate(((wqkv_hbm, wqkv), (wout_hbm, wout)))]
    swaps = [send_to(other_core(), src, dst.at[pl.ds(HALF, HALF)], send.at[k], recv.at[k]) for k, (src, dst) in enumerate(((x_hbm, xs), (dy_hbm, dys)))]

    @pl.when(first)
    def _():
        for copy in [*row_loads(0), *(copy for c in range(chunks) for copy in chunk_loads(c)), *w_loads, *row_loads(1)]:
            copy.start()
        up_acc[:] = jnp.zeros_like(up_acc)
        down_acc[:] = jnp.zeros_like(down_acc)
        greet([other_core()])
        for copy in swaps:
            copy.start()

    def norms(n):
        norm, _ = normed(xs[pl.ds(pl.multiple_of(n * TT, TT), TT), :])
        hm = (norm * ln_ref[pl.ds(2, 1), :] + ln_ref[pl.ds(3, 1), :]).astype(BF16)
        ha_s[:] = (norm * ln_ref[pl.ds(0, 1), :] + ln_ref[pl.ds(1, 1), :]).astype(BF16).T
        hm_s[:] = hm
        hm_t[:] = hm.T

    @pl.when(first)
    def _():
        for copy in row_loads(0):
            copy.wait()
        norms(0)

    ha_ref[:] = ha_s[:]

    def columns(c, carry):
        @pl.when(first)
        def _():
            for copy in chunk_loads(c):
                copy.wait()
        cols = chunk(c)
        u = dot(hm_s[:], wup[:, cols]).astype(BF16).astype(F32)
        dg = dot_nt(dys[rows, :], wdown[cols, :]).astype(BF16).astype(F32)
        cdf = 0.5 * (1.0 + lax.erf(u * math.sqrt(0.5)))
        gelu = (u * cdf).astype(BF16)
        pdf = jnp.exp(-0.5 * u * u) * (1.0 / math.sqrt(2.0 * math.pi))
        dh = (dg * (cdf + u * pdf)).astype(BF16)
        dh_s[:, cols] = dh
        down_acc[cols, :] += dot(gelu.T, dys[rows, :])
        up_acc[:, cols] += dot(hm_t[:], dh)

        @pl.when(last)
        def _():
            for copy in flush(c):
                copy.start()
        return carry
    lax.fori_loop(0, chunks, columns, 0)
    @pl.when(first)
    def _():
        for copy in w_loads:
            copy.wait()
    for n in range(1, HALF // TT):
        @pl.when(step == n - 1)
        def _(n=n):
            for copy in row_loads(n):
                copy.wait()

    @pl.when(step == HALF // TT - 1)
    def _():
        for copy in swaps:
            copy.wait_recv()
        for copy in dy_saves:
            copy.start()

    dhm_ref[:] = dot_nt(dh_s[:], wup[:]).astype(BF16)
    norms(jnp.minimum(step + 1, pl.num_programs(0) - 1))
    qkv_ref[:] = dot(wqkv[:], ha_ref[:]).astype(BF16)
    dctx_ref[:] = dot_nt(wout[:], dys[rows, :]).astype(BF16)
    position = token_tile(step) * TT + lax.broadcasted_iota(jnp.int32, cos_ref.shape, 1)
    angles = position.astype(F32) * freq_ref[:, pl.ds(0, 1)]
    cos_ref[:] = jnp.cos(angles)
    sin_ref[:] = jnp.sin(angles)

    @pl.when(last)
    def _():
        for copy in swaps:
            copy.wait_send()
        for copy in dy_saves:
            copy.wait()
        for c in range(chunks):
            for copy in flush(c):
                copy.wait()


def token_part(x, dy, ln, wqkv_t, wout, wup, wdown):
    D, width = wup.shape
    S, V, dma = jax.ShapeDtypeStruct, pltpu.VMEM, pltpu.SemaphoreType.DMA
    hbm, vmem = pl.BlockSpec(memory_space=pl.ANY), pl.BlockSpec(memory_space=pltpu.VMEM)
    steps, halves = T // TT, HALF // TT
    freq = np.tile((ROPE_BASE ** (np.arange(0, -HEAD, -2) / HEAD)).astype(np.float32)[:, None], LANES)

    def tok(size):
        return pl.BlockSpec((TT, size), lambda i: (token_tile(i), 0))

    def col(size):
        return pl.BlockSpec((size, TT), lambda i: (0, token_tile(i)))

    return pl.pallas_call(
        token_kernel,
        grid=(steps,),
        in_specs=[hbm, hbm, vmem, vmem] + [hbm] * 4,
        out_specs=[col(D), col(wqkv_t.shape[0]), col(wout.shape[0]), tok(D), col(HEAD // 2), col(HEAD // 2), hbm, hbm, hbm],
        out_shape=[S((D, T), BF16), S((wqkv_t.shape[0], T), BF16), S((wout.shape[0], T), BF16), S((T, D), BF16),
                   S((HEAD // 2, T), F32), S((HEAD // 2, T), F32), S((T, D), BF16),
                   S((D, width), F32), S((width, D), F32)],
        scratch_shapes=[V((T, D), BF16)] * 2 + [V(w.shape, BF16) for w in (wqkv_t, wout, wup, wdown)]
        + [V((D, TT), BF16), V((TT, D), BF16), V((D, TT), BF16), V((TT, width), BF16), V((D, width), F32), V((width, D), F32)]
        + [dma((2, halves)), dma((2,)), dma((2, width // FC)), dma((2, width // FC)), dma((2,)), dma((2,)), dma((2,))],
        compiler_params=pltpu.CompilerParams(dimension_semantics=("arbitrary",), vmem_limit_bytes=VMEM_LIMIT,
                                             collective_id=2, has_side_effects=True),
        cost_estimate=pl.CostEstimate(flops=52 * 10**9, bytes_accessed=60 << 20, transcendentals=2 * T * width),
        name="token_part",
    )(x, dy, ln, freq, wqkv_t, wout, wup, wdown)


def attention_pair(qkv_ref, dctx_ref, cos_ref, sin_ref, dqkv_ref, ctx_ref, q_t, k_t, q_n, k_n, v_n, do_n, p_s, dp_s, dk_acc, dv_acc, slot):
    lane = lax.broadcasted_iota(jnp.int32, (TILE, PAIR), 1)
    key = lax.broadcasted_iota(jnp.int32, (TILE, 2 * TILE), 0)
    query = lax.broadcasted_iota(jnp.int32, (TILE, 2 * TILE), 1) % TILE

    def tile_at(j):
        return pl.ds(j * TILE, TILE)

    def head_rows(head, part):
        return pl.ds((3 * head + part) * HEAD, HEAD)

    def halves(x):
        return x[:HEAD // 2].astype(F32), x[HEAD // 2:].astype(F32)

    def rotate(x, cols, sign):
        cos, sin = cos_ref[:, cols], sin_ref[:, cols] * sign
        lo, hi = halves(x)
        return jnp.concatenate([lo * cos - hi * sin, hi * cos + lo * sin], axis=0).astype(BF16)

    def prepare(j):
        cols = tile_at(j)
        for head in range(2):
            rows = pl.ds(head * HEAD, HEAD)
            q_t[rows, cols] = rotate(qkv_ref[head_rows(head, 0), cols], cols, 1.0) * jnp.asarray(HEAD ** -0.5, BF16)
            k_t[rows, cols] = rotate(qkv_ref[head_rows(head, 1), cols], cols, 1.0)
        q_n[cols, :] = q_t[:, cols].T
        k_n[cols, :] = k_t[:, cols].T
        v_n[cols, :] = jnp.concatenate([qkv_ref[head_rows(head, 2), cols] for head in range(2)], axis=0).T
        do_n[cols, :] = dctx_ref[:, cols].T

    def split_lanes(x):
        zero = jnp.zeros_like(x)
        return jnp.concatenate([jnp.where(lane < HEAD, x, zero), jnp.where(lane < HEAD, zero, x)], axis=0)

    def split_rows(x):
        zero = jnp.zeros((HEAD, TILE), x.dtype)
        return jnp.concatenate([jnp.concatenate([x[:HEAD], zero], axis=1), jnp.concatenate([zero, x[HEAD:]], axis=1)], axis=0)

    def fold(x, op):
        parts = [x[r:r + 8] for r in range(0, TILE, 8)]
        while len(parts) > 1:
            parts = [op(a, b) for a, b in zip(parts[::2], parts[1::2])]
        return parts[0]

    def gather(old, new, op):
        return new if old is None else op(old, new)

    blocks = list(reversed(range(T // TILE)))
    before = {i: sum(b + 1 for b in blocks[:n]) for n, i in enumerate(blocks)}

    def p_at(i, j):
        return pl.ds((before[i] + j) % P_TILES * TILE, TILE)

    def dp_at(i, j):
        return pl.ds((before[i] + j) % DP_TILES * TILE, TILE)

    def scores(i, state):
        q_split = split_rows(q_t[:, tile_at(i)])
        top = None
        for j in range(i + 1):
            s = dot(k_n[tile_at(j), :], q_split)
            if j == i:
                s = jnp.where(query >= key, s, -1e30)
            p_s[p_at(i, j), :] = s
            top = gather(top, fold(s, jnp.maximum), jnp.maximum)
            if j == i:
                state['max'] = jnp.max(top, axis=0, keepdims=True)
            yield

    def weights(i, state):
        do_split = split_rows(dctx_ref[:, tile_at(i)])
        total = both = None
        for j in range(i + 1):
            dp = dot(v_n[tile_at(j), :], do_split).astype(BF16)
            dp_s[dp_at(i, j), :] = dp
            p = jnp.exp2((p_s[p_at(i, j), :] - state['max']) * LOG2E)
            p_s[p_at(i, j), :] = p
            total = gather(total, fold(p, jnp.add), jnp.add)
            both = gather(both, fold(p * dp.astype(F32), jnp.add), jnp.add)
            if j == i:
                state['inv'] = 1.0 / jnp.sum(total, axis=0, keepdims=True)
                state['delta'] = jnp.sum(both, axis=0, keepdims=True) * state['inv']
            yield

    def grads(i, state):
        cols = tile_at(i)
        q_pair, do_pair = split_lanes(q_n[cols, :]), split_lanes(do_n[cols, :])
        ctx, dq = [None] * 2, [None] * 2
        for j in range(i + 1):
            keys = tile_at(j)
            p = p_s[p_at(i, j), :] * state['inv']
            p_bf = p.astype(BF16)
            ds_bf = (p * (dp_s[dp_at(i, j), :].astype(F32) - state['delta'])).astype(BF16)
            for head in range(2):
                side = slice(head * TILE, (head + 1) * TILE)
                ctx[head] = gather(ctx[head], dot(qkv_ref[head_rows(head, 2), keys], p_bf[:, side]), jnp.add)
                dq[head] = gather(dq[head], dot(k_t[pl.ds(head * HEAD, HEAD), keys], ds_bf[:, side]), jnp.add)
            for acc, new in ((dv_acc, dot(p_bf, do_pair)), (dk_acc, dot(ds_bf, q_pair))):
                acc[keys, :] = new if i == blocks[0] else acc[keys, :] + new
            if j == i:
                dk, dv = dk_acc[cols, :].astype(BF16).T, dv_acc[cols, :].astype(BF16).T
                for head in range(2):
                    rows = pl.ds(head * HEAD, HEAD)
                    side = slice(head * HEAD, (head + 1) * HEAD)
                    ctx_ref[rows, cols] = ctx[head].astype(BF16)
                    dqkv_ref[head_rows(head, 0), cols] = rotate((dq[head] * HEAD ** -0.5).astype(BF16), cols, -1.0)
                    dqkv_ref[head_rows(head, 1), cols] = rotate(dk[side], cols, -1.0)
                    dqkv_ref[head_rows(head, 2), cols] = dv[side]
            yield

    slot(0)
    for j in range(T // TILE):
        prepare(j)
    states = {i: {} for i in blocks}
    for n in range(len(blocks) + 2):
        work = []
        for stage, make in ((n - 2, grads), (n - 1, weights), (n, scores)):
            if 0 <= stage < len(blocks):
                i = blocks[stage]
                run = make(i, states[i])
                work += [((j + 0.5) / (i + 1), run) for j in range(i + 1)]
        for _, run in sorted(work, key=lambda item: item[0]):
            next(run)
        if n in SLOT_AFTER:
            slot(SLOT_AFTER[n])


P_TILES, DP_TILES = 21, 15
SLOT_AFTER = {2: 1, 4: 2, 6: 3, 9: 4}


def attention_scratch():
    V = pltpu.VMEM
    return [V((PAIR, T), BF16)] * 2 + [V((T, PAIR), BF16)] * 4 + [V((P_TILES * TILE, 2 * TILE), F32), V((DP_TILES * TILE, 2 * TILE), BF16)] \
        + [V((T, PAIR), F32)] * 2


SCHEDULE = {
    (0, 0): (('start', 0),),
    (1, 3): (('add', 0), ('pass_on', 0)),
    (2, 3): (('finish', 0), ('start', 1)),
    (3, 1): (('add', 1), ('pass_on', 1)),
    (3, 2): (('finish', 1), ('start', 2)),
    (3, 3): (('add', 2), ('pass_on', 2)),
    (3, 4): (('finish', 2),),
}


def attention_kernel(qkv_ref, dctx_ref, cos_ref, sin_ref, up_ref, down_ref, dqkv_ref, ctx_ref, up_out, down_out, *refs):
    count = len(attention_scratch())
    groups = plan_sums((up_ref, down_ref), (PLAN_UP, PLAN_DOWN), refs[count:])
    every = groups[0] + groups[1]

    def slot(place):
        for (pair, at), stages in SCHEDULE.items():
            if at != place:
                continue

            @pl.when(pl.program_id(0) == pair)
            def _(pair=pair, stages=stages):
                if (pair, place) == (0, 0):
                    greet([ring_chip(axis, ahead) for axis in AXES for ahead in (1, 3)])
                for stage, phase in stages:
                    for one in every:
                        getattr(one, stage)(phase)
                if (pair, place) == list(SCHEDULE)[-1]:
                    for out, sums in zip((up_out, down_out), groups):
                        for one in sums:
                            out[:, one.cols] = one.result[:]
                            one.drain()

    attention_pair(qkv_ref, dctx_ref, cos_ref, sin_ref, dqkv_ref, ctx_ref, *refs[:count], slot)


def attention(qkv_t, dctx_t, cos_t, sin_t, g_up, g_down):
    pairs = dctx_t.shape[0] // PAIR
    S = jax.ShapeDtypeStruct
    shares = [(g.shape[0] // 64, g.shape[1]) for g in (g_up, g_down)]
    hbm = pl.BlockSpec(memory_space=pl.ANY)

    def by_pair(rows):
        return pl.BlockSpec((rows, T), lambda p: (p, 0))

    def fixed(shape):
        return pl.BlockSpec(shape, lambda p: (0, 0), pipeline_mode=pl.Buffered(1))

    return pl.pallas_call(
        attention_kernel,
        grid=(pairs,),
        in_specs=[by_pair(3 * PAIR), by_pair(PAIR), fixed(cos_t.shape), fixed(sin_t.shape), hbm, hbm],
        out_specs=[by_pair(3 * PAIR), by_pair(PAIR)] + [fixed(share) for share in shares],
        out_shape=[S(qkv_t.shape, BF16), S(dctx_t.shape, BF16)] + [S(share, F32) for share in shares],
        scratch_shapes=attention_scratch() + plan_scratch((PLAN_UP, PLAN_DOWN)),
        compiler_params=pltpu.CompilerParams(dimension_semantics=("arbitrary",), vmem_limit_bytes=VMEM_LIMIT,
                                             collective_id=0, has_side_effects=True),
        cost_estimate=pl.CostEstimate(flops=80 * 10**9, bytes_accessed=20 << 20, transcendentals=8 * T * T // 2),
        name="attention",
    )(qkv_t, dctx_t, cos_t, sin_t, *(g.reshape((RING,) * 3 + (-1, g.shape[1])) for g in (g_up, g_down)))


DURING_TOKENS = {2: ('B+0', 'b!0'), 5: ('C+0', 'c!0')}
DURING_NORMS = {2: ('A=0',), 5: ('B=0', 'a+0'), 7: ('b+0',)}
AFTER_NORMS = (
    ('C=0', 'A+1', 'c+0', 'B+1', 'a=0', 'b=0'),
    ('C+1', 'A=1', 'c=0', 'B=1', 'a+1', 'b+1'),
    ('A+2', 'B+2', 'C=1', 'c+1', 'a=1', 'b=1'),
    ('A=2', 'B=2', 'C+2', 'c=1', 'a+2', 'b+2'),
    ('C=2', 'a=2', 'b=2', 'c+2', 'c=2'),
)


def tail_kernel(hat_hbm, dqkv_hbm, ctx_hbm, dy_hbm, w_hbm, x_hbm, dhm_hbm, ln_ref, gx_ref, gln_ref, gqkv_ref, gout_ref,
                hat, dqkv, ctx, dy, w, x, dhm_own, dhm_in, dha_s, dha_in, g_qkv, g_out, pair_s, ring_s,
                load, send, recv, ring_send, ring_recv, *sum_refs):
    core = lax.axis_index('tp')
    own, away = core * HALF, (1 - core) * HALF
    groups = plan_sums((g_qkv, g_out), (PLAN_QKV, PLAN_OUT), sum_refs, True)
    qkv_sums = groups[0]
    sums = dict(zip('ABCabc', groups[0] + groups[1]))
    block = dqkv.shape[0] // len(qkv_sums)

    def rows_of(ref, start, size):
        return ref.at[pl.ds(start, size)]

    pieces = [(hat_hbm, hat)] + [(rows_of(dqkv_hbm, n * block, block), rows_of(dqkv, n * block, block)) for n in range(3)]
    pieces += [(ctx_hbm, ctx), (dy_hbm, dy), (w_hbm, w), (x_hbm, x), (rows_of(dhm_hbm, own, HALF), dhm_own)]
    loads = [pltpu.make_async_copy(src, dst, load.at[n]) for n, (src, dst) in enumerate(pieces)]
    for copy in loads:
        copy.start()
    greet([ring_chip(axis, ahead) for axis in AXES for ahead in (1, 2, 3)] + [other_core()])
    dhm_copy = send_to(other_core(), rows_of(dhm_hbm, away, HALF), dhm_in, send.at[0], recv.at[0])
    dha_copy = send_to(other_core(), dha_s.at[0], dha_in, send.at[1], recv.at[1])
    pair_copy = send_to(other_core(), pair_s.at[0], pair_s.at[1], send.at[2], recv.at[2])
    dhm_copy.start()

    def run(events):
        for name, act, ring in events:
            one, phase = sums[name], int(ring)
            if act == '!':
                one.start(phase)
            elif act == '+':
                one.add(phase)
                one.pass_on(phase)
            else:
                one.finish(phase)
                if phase < len(AXES) - 1:
                    one.start(phase + 1)
                elif name in 'abc':
                    gout_ref[:, one.cols] = one.result[:]
                else:
                    for k in range(one.whole[1] // HEAD):
                        group, part = divmod(one.col // HEAD + k, 3)
                        gqkv_ref[:, part, group, :] = one.result[:, pl.ds(k * HEAD, HEAD)]

    def run_at(k, table):
        for when, events in table.items():
            @pl.when(k == when)
            def _(events=events):
                run(events)

    loads[0].wait()
    per_group = block // TILE

    def columns(k, carry):
        for n in range(len(qkv_sums)):
            @pl.when(k == n * per_group)
            def _(n=n):
                loads[1 + n].wait()
        cols = pl.ds(pl.multiple_of(k * TILE, TILE), TILE)
        g_qkv[:, :, :, :, cols] = dot_nt(hat[:], dqkv[cols, :]).reshape(g_qkv.shape[:4] + (TILE,))
        for n, one in enumerate(qkv_sums):
            @pl.when(k == (n + 1) * per_group - 1)
            def _(one=one):
                one.start(0)
        return carry
    lax.fori_loop(0, len(qkv_sums) * per_group, columns, 0)
    loads[4].wait()
    loads[5].wait()

    def out_columns(k, carry):
        cols = pl.ds(pl.multiple_of(k * TILE, TILE), TILE)
        g_out[:, :, :, :, cols] = dot(ctx[:], dy[:, cols]).reshape(g_out.shape[:4] + (TILE,))
        return carry
    lax.fori_loop(0, dy.shape[1] // TILE, out_columns, 0)
    run(('A+0', 'a!0'))

    loads[6].wait()
    tiles = HALF // TILE

    def tokens(k, carry):
        mine = lax.div(k, tiles)
        at = lax.rem(k, tiles) * TILE
        cols = pl.ds(pl.multiple_of(jnp.where(mine == 0, away, own) + at, TILE), TILE)
        dha_s[mine, pl.ds(pl.multiple_of(at, TILE), TILE), :] = dot(dqkv[:, cols].T, w[:]).astype(BF16)

        @pl.when(k == tiles - 1)
        def _():
            dha_copy.start()
        run_at(k, DURING_TOKENS)
        return carry
    lax.fori_loop(0, 2 * tiles, tokens, 0)

    loads[7].wait()
    loads[8].wait()
    dhm_copy.wait_recv()
    dha_copy.wait_recv()
    pair_s[0] = jnp.zeros_like(pair_s[0])

    def norm_back(k, carry):
        at = pl.ds(pl.multiple_of(k * SMALL, SMALL), SMALL)
        norm, rstd = normed(x[at, :])
        da = (dha_s[1, at, :].astype(F32) + dha_in[at, :].astype(F32)).astype(BF16).astype(F32)
        dm = (dhm_own[at, :].astype(F32) + dhm_in[at, :].astype(F32)).astype(BF16).astype(F32)
        g = da * ln_ref[pl.ds(0, 1), :] + dm * ln_ref[pl.ds(2, 1), :]
        mean_g = jnp.mean(g, axis=-1, keepdims=True)
        mean_gn = jnp.mean(g * norm, axis=-1, keepdims=True)
        residual = dy[pl.ds(pl.multiple_of(own + k * SMALL, SMALL), SMALL), :].astype(F32)
        gx_ref[at, :] = (residual + rstd * (g - mean_g - norm * mean_gn)).astype(BF16)
        for row, value in enumerate((da * norm, da, dm * norm, dm)):
            pair_s[0, pl.ds(row, 1), :] += jnp.sum(value, axis=0, keepdims=True)
        return carry

    steps = HALF // SMALL

    def norm_step(k, carry):
        run_at(k, DURING_NORMS)
        return norm_back(k, carry)
    lax.fori_loop(0, steps, norm_step, 0)
    pair_copy.start()

    def ring_copies(phase):
        place = ring_place(AXES[phase])
        return [send_to(ring_chip(AXES[phase], ahead), ring_s.at[phase, place], ring_s.at[phase, place],
                        ring_send.at[phase, ahead], ring_recv.at[phase, ahead]) for ahead in (1, 2, 3)]

    def ring_start(phase, value):
        ring_s[phase, ring_place(AXES[phase])] = value
        for copy in ring_copies(phase):
            copy.start()

    def ring_sum(phase):
        for copy in ring_copies(phase):
            copy.wait_recv()
        return ring_s[phase, 0] + ring_s[phase, 1] + ring_s[phase, 2] + ring_s[phase, 3]

    for n, events in enumerate(AFTER_NORMS):
        run(events)
        if n == 0:
            pair_copy.wait_recv()
            ring_start(0, pair_s[0] + pair_s[1])
        elif n < len(AXES):
            ring_start(n, ring_sum(n - 1))
    gln_ref[:] = ring_sum(2)[:gln_ref.shape[0]]
    for one in sums.values():
        one.drain()
    for copy in (dhm_copy, dha_copy, pair_copy):
        copy.wait_send()
    for phase in range(3):
        for copy in ring_copies(phase):
            copy.wait_send()


def tail(ha_t, dqkv_t, ctx_t, dy, wqkv_t, x, dhm, ln):
    D, C = ha_t.shape[0], ctx_t.shape[0]
    S, V = jax.ShapeDtypeStruct, pltpu.VMEM
    hbm, vmem = pl.BlockSpec(memory_space=pl.ANY), pl.BlockSpec(memory_space=pltpu.VMEM)
    own = V((HALF, D), BF16)
    chips = (RING,) * 3
    dma = pltpu.SemaphoreType.DMA
    return pl.pallas_call(
        tail_kernel,
        in_specs=[hbm] * 7 + [vmem],
        out_specs=[vmem] * 4,
        out_shape=[S((HALF, D), BF16), S(ln.shape, F32), S((D // 64, 3, C // HEAD, HEAD), F32), S((C // 64, D), F32)],
        scratch_shapes=[V(a.shape, BF16) for a in (ha_t, dqkv_t, ctx_t, dy, wqkv_t)] + [own] * 3 + [V((2, HALF, D), BF16), own]
        + [V(chips + (D // 64, 3 * C), F32), V(chips + (C // 64, D), F32), V((2, 8, D), F32), V((3, RING, 8, D), F32)]
        + [dma((9,)), dma((3,)), dma((3,)), dma((3, RING)), dma((3, RING))] + plan_scratch((PLAN_QKV, PLAN_OUT)),
        compiler_params=pltpu.CompilerParams(vmem_limit_bytes=VMEM_LIMIT, collective_id=1, has_side_effects=True),
        cost_estimate=pl.CostEstimate(flops=15 * 10**9, bytes_accessed=30 << 20, transcendentals=0),
        name="tail",
    )(ha_t, dqkv_t, ctx_t, dy, wqkv_t, x, dhm, ln)


def output_kernel(*refs):
    ins, outs = refs[:len(refs) // 2], refs[len(refs) // 2:]
    outs[0][:] = ins[0][:]

    @pl.when(pl.program_id(0) == 0)
    def _():
        for src, dst in zip(ins[1:], outs[1:]):
            dst[:] = src[:]


def outputs(grad_x, *rest):
    steps = 2

    def fixed(a):
        return pl.BlockSpec(a.shape, lambda i: (0,) * len(a.shape), pipeline_mode=pl.Buffered(1))

    specs = [pl.BlockSpec((grad_x.shape[0] // steps, grad_x.shape[1]), lambda i: (i, 0))] + [fixed(a) for a in rest]
    return pl.pallas_call(
        output_kernel, grid=(steps,), in_specs=specs, out_specs=specs,
        out_shape=[jax.ShapeDtypeStruct(a.shape, a.dtype) for a in (grad_x, *rest)],
        compiler_params=pltpu.CompilerParams(dimension_semantics=("arbitrary",)),
        name="outputs",
    )(grad_x, *rest)


def solution(mesh):
    def local_step(x_loc, dy_loc, ln_params, w_qkv, w_out, w_up, w_down):
        x_loc, dy_loc = x_loc[0], dy_loc[0]
        wqkv_t = w_qkv.transpose(1, 2, 3, 0).reshape(-1, x_loc.shape[1])
        ha_t, qkv_t, dctx_t, dhm, cos_t, sin_t, dy, g_wup, g_wdown = token_part(x_loc, dy_loc, ln_params, wqkv_t, w_out, w_up, w_down)
        dqkv_t, ctx_t, grad_wup, grad_wdown = attention(qkv_t, dctx_t, cos_t, sin_t, g_wup, g_wdown)
        grad_x, grad_ln, grad_wqkv, grad_wout = tail(ha_t, dqkv_t, ctx_t, dy, wqkv_t, x_loc, dhm, ln_params)
        grad_x, grad_ln, grad_wqkv, *rest = outputs(grad_x, grad_ln, grad_wqkv, grad_wout, grad_wup, grad_wdown)
        return grad_x[None], grad_ln, grad_wqkv.swapaxes(1, 2), *rest

    act_spec = P('dp', 'tp')
    in_specs = (act_spec, act_spec, P(), P(None, 'tp'), P('tp'), P(None, 'tp'), P('tp'))
    out_specs = (act_spec, P(), P('dp', 'tp'), P(('tp', 'dp')), P('dp', 'tp'), P(('tp', 'dp')))
    return jax.shard_map(local_step, mesh=mesh, in_specs=in_specs, out_specs=out_specs, check_vma=False)
```

```python
import math

import jax
import jax.numpy as jnp
import numpy as np
from jax import lax
from jax.experimental import pallas as pl
from jax.experimental.pallas import tpu as pltpu
from jax.sharding import PartitionSpec as P

NORM_EPS = 1e-5
ROPE_BASE = 10000.0
F32, BF16 = jnp.float32, jnp.bfloat16
LOG2E = math.log2(math.e)
T = 2048
HALF = T // 2
TILE = 256
SMALL = 128
TT = 512
FC = 1024
LANES = 128
HEAD, PAIR = 64, 128
VMEM_LIMIT = 63 << 20
AXES = ('z', 'y', 'x')
AXIS_STRIDE = {'z': 16, 'y': 4, 'x': 1}
RING = 4


def dot(a, b):
    return jnp.dot(a, b, preferred_element_type=F32)


def dot_nt(a, b):
    return lax.dot_general(a, b, (((1,), (1,)), ((), ())), preferred_element_type=F32)


def ring_place(axis):
    return lax.rem(lax.div(lax.axis_index('dp'), AXIS_STRIDE[axis]), RING)


def ring_chip(axis, ahead):
    place = ring_place(axis)
    return {'dp': lax.axis_index('dp') + (lax.rem(place + ahead, RING) - place) * AXIS_STRIDE[axis]}


def other_core():
    return {'tp': 1 - lax.axis_index('tp')}


def send_to(device, src, dst, send_sem, recv_sem):
    return pltpu.make_async_remote_copy(src_ref=src, dst_ref=dst, send_sem=send_sem, recv_sem=recv_sem,
                                        device_id=device, device_id_type=pl.DeviceIdType.MESH)


def greet(devices):
    barrier = pltpu.get_barrier_semaphore()
    for device in devices:
        pl.semaphore_signal(barrier, inc=1, device_id=device, device_id_type=pl.DeviceIdType.MESH)
    pl.semaphore_wait(barrier, len(devices))


class TorusSum:
    @staticmethod
    def half_shape(rows, width, by_cols):
        return (rows, width // 2) if by_cols else (rows // 2, width)

    @staticmethod
    def scratch(rows, width, by_cols, in_vmem):
        half, whole = TorusSum.half_shape(rows, width, by_cols), (rows, width)
        leads = ((RING, RING), (RING,), ())
        shapes = [pltpu.VMEM(lead + shape, F32) for lead in leads for shape in (half,) * 6 + (whole,)]
        shapes += [] if in_vmem else [pltpu.VMEM(leads[0] + half, F32)] * 2
        return shapes + [pltpu.SemaphoreType.DMA((18,)), pltpu.SemaphoreType.DMA((18,)), pltpu.SemaphoreType.DMA((3,))]

    def __init__(self, grad, order, rows, col, width, refs, by_cols, in_vmem):
        self.grad, self.order, self.col, self.by_cols, self.in_vmem = grad, order, col, by_cols, in_vmem
        self.whole, self.half = (rows, width), TorusSum.half_shape(rows, width, by_cols)
        self.cols = pl.ds(col, width)
        self.sums = [refs[7 * n:7 * n + 7] for n in range(3)]
        self.loaded, (self.send, self.recv, self.load) = refs[21:-3], refs[-3:]
        self.kept = [[axis for axis in AXES if axis not in order[:n]] for n in range(3)]

    def part(self, which, col=0):
        shape = self.whole if which == 2 else self.half
        start = [0, col]
        if which == 1:
            start[self.by_cols] += self.half[self.by_cols]
        return tuple(pl.ds(first, size) for first, size in zip(start, shape))

    def block(self, phase, ahead, which):
        index = lax.rem(ring_place(self.order[phase]) + ahead, RING)
        lead = tuple(index if axis == self.order[phase] else slice(None) for axis in self.kept[phase])
        if phase == 0:
            return self.grad.at[lead + self.part(which, self.col)]
        return self.sums[phase - 1][6].at[lead + self.part(which)]

    def load_copy(self, n):
        ahead, which = ((1, 0), (3, 1), (0, 2))[n]
        dst = (*self.loaded, self.sums[0][6])[n]
        return pltpu.make_async_copy(self.block(0, ahead, which), dst, self.load.at[n])

    def copy(self, phase, n):
        bufs = self.sums[phase]
        src = bufs[2 * n - 8] if n >= 4 else self.block(phase, *((2, 0), (1, 1), (2, 1), (3, 0))[n])
        chip = ring_chip(self.order[phase], (1, 1, 3, 3, 1, 3)[n])
        return send_to(chip, src, bufs[n], self.send.at[6 * phase + n], self.recv.at[6 * phase + n])

    def loads(self, phase):
        return phase == 0 and not self.in_vmem

    def start(self, phase):
        for n in (0, 2, 1, 3):
            self.copy(phase, n).start()
        if self.loads(phase):
            for n in range(3):
                self.load_copy(n).start()

    def add(self, phase):
        bufs = self.sums[phase]
        own = self.block(phase, 1, 0), self.block(phase, 3, 1)
        if self.loads(phase):
            own = self.loaded
            self.load_copy(0).wait()
            self.load_copy(1).wait()
        self.copy(phase, 0).wait_recv()
        self.copy(phase, 2).wait_recv()

        def rows(at):
            bufs[0][at] = own[0][at] + bufs[0][at]
            bufs[2][at] = own[1][at] + bufs[2][at]
        self.each(phase, rows)

    def each(self, phase, body):
        if phase == 0:
            def step(n, carry):
                body(n)
                return carry
            lax.fori_loop(0, RING, step, 0)
        else:
            body(slice(None))

    def pass_on(self, phase):
        self.copy(phase, 4).start()
        self.copy(phase, 5).start()

    def finish(self, phase):
        bufs = self.sums[phase]
        lead = (slice(None),) * (2 - phase)
        low, high = bufs[6].at[lead + self.part(0)], bufs[6].at[lead + self.part(1)]
        own = self.block(phase, 0, 0), self.block(phase, 0, 1)
        if self.loads(phase):
            own = low, high
            self.load_copy(2).wait()
        for n in (1, 3, 4, 5):
            self.copy(phase, n).wait_recv()

        def rows(at):
            low[at] = own[0][at] + bufs[3][at] + bufs[4][at]
            high[at] = own[1][at] + bufs[1][at] + bufs[5][at]
        self.each(phase, rows)

    def drain(self):
        for phase in range(3):
            for n in range(6):
                self.copy(phase, n).wait_send()

    @property
    def result(self):
        return self.sums[2][6]


def plan_columns(rows, tiles, by_cols=False):
    plan, col, orders = [], 0, (('x', 'y', 'z'), ('y', 'z', 'x'), ('z', 'x', 'y'))
    for n, count in enumerate(tiles):
        plan.append((orders[n % len(orders)], rows, col, count * LANES, by_cols))
        col += count * LANES
    return plan


def plan_scratch(plans, in_vmem=False):
    return [shape for plan in plans for _, rows, _, width, by_cols in plan for shape in TorusSum.scratch(rows, width, by_cols, in_vmem)]


def plan_sums(grads, plans, refs, in_vmem=False):
    groups = []
    for grad, plan in zip(grads, plans):
        groups.append([])
        for order, rows, col, width, by_cols in plan:
            count = len(TorusSum.scratch(rows, width, by_cols, in_vmem))
            groups[-1].append(TorusSum(grad, order, rows, col, width, refs[:count], by_cols, in_vmem))
            refs = refs[count:]
    return groups


PLAN_UP = plan_columns(16, (5, 5, 6))
PLAN_DOWN = plan_columns(32, (3, 3, 2))
PLAN_QKV = plan_columns(16, (4, 4, 4))
PLAN_OUT = plan_columns(8, (4, 2, 2), True)


def lane_mean(x):
    return jnp.mean(x, axis=-1, keepdims=True)


def normed(x):
    x = x.astype(F32)
    centered = x - lane_mean(x)
    rstd = lax.rsqrt(lane_mean(centered * centered) + NORM_EPS)
    return centered * rstd, rstd


def token_tile(step):
    core, halves = lax.axis_index('tp'), HALF // TT
    return jnp.where(step < halves, core * halves + step, (1 - core) * halves + step - halves)


def token_kernel(x_hbm, dy_hbm, ln_ref, freq_ref, wout_hbm, wup_hbm, wdown_hbm,
                 ha_ref, dctx_ref, dh_ref, cos_ref, sin_ref, dy_ref, gup_ref, gdown_ref,
                 xs, dys, wout, wup, wdown, ha_s, hm_s, hm_t, up_acc, down_acc,
                 row_load, w_load, chunk_load, flush_sem, dy_sem, send, recv):
    step = pl.program_id(0)
    first, last = step == 0, step == pl.num_programs(0) - 1
    width = wup.shape[1]
    chunks = width // FC
    rows = pl.ds(pl.multiple_of(step * TT, TT), TT)

    def chunk(c):
        return pl.ds(pl.multiple_of(c * FC, FC), FC)

    def flush(c):
        return (pltpu.make_async_copy(up_acc.at[:, chunk(c)], gup_ref.at[:, chunk(c)], flush_sem.at[0, c]),
                pltpu.make_async_copy(down_acc.at[chunk(c), :], gdown_ref.at[chunk(c), :], flush_sem.at[1, c]))

    def row_loads(n):
        part = pl.ds(n * TT, TT)
        return [pltpu.make_async_copy(src.at[part], dst.at[part], row_load.at[k, n]) for k, (src, dst) in enumerate(((x_hbm, xs), (dy_hbm, dys)))]

    def chunk_loads(c):
        return (pltpu.make_async_copy(wup_hbm.at[:, chunk(c)], wup.at[:, chunk(c)], chunk_load.at[0, c]),
                pltpu.make_async_copy(wdown_hbm.at[chunk(c), :], wdown.at[chunk(c), :], chunk_load.at[1, c]))

    core = lax.axis_index('tp')
    dy_saves = [pltpu.make_async_copy(dys.at[pl.ds(n * HALF, HALF)], dy_ref.at[pl.ds(place * HALF, HALF)], dy_sem.at[n])
                for n, place in enumerate((core, 1 - core))]
    w_loads = [pltpu.make_async_copy(wout_hbm, wout, w_load.at[0])]
    swaps = [send_to(other_core(), src, dst.at[pl.ds(HALF, HALF)], send.at[k], recv.at[k]) for k, (src, dst) in enumerate(((x_hbm, xs), (dy_hbm, dys)))]

    @pl.when(first)
    def _():
        for copy in [*row_loads(0), *(copy for c in range(chunks) for copy in chunk_loads(c)), *w_loads, *row_loads(1)]:
            copy.start()
        up_acc[:] = jnp.zeros_like(up_acc)
        down_acc[:] = jnp.zeros_like(down_acc)
        greet([other_core()])
        for copy in swaps:
            copy.start()

    def norms(n, part):
        size = TT // chunks
        at = pl.ds(pl.multiple_of(part * size, size), size)
        norm, _ = normed(xs[pl.ds(pl.multiple_of(n * TT + part * size, size), size), :])
        hm = (norm * ln_ref[pl.ds(2, 1), :] + ln_ref[pl.ds(3, 1), :]).astype(BF16)
        ha_s[:, at] = (norm * ln_ref[pl.ds(0, 1), :] + ln_ref[pl.ds(1, 1), :]).astype(BF16).T
        slot = lax.rem(n, 2)
        hm_s[slot, at, :] = hm
        hm_t[slot, :, at] = hm.T

    @pl.when(first)
    def _():
        for copy in row_loads(0):
            copy.wait()
        for part in range(chunks):
            norms(0, part)
        for n in range(1, HALF // TT):
            for copy in row_loads(n):
                copy.wait()

    @pl.when(step == HALF // TT - 1)
    def _():
        for copy in swaps:
            copy.wait_recv()
        for copy in dy_saves:
            copy.start()

    ha_ref[:] = ha_s[:]
    now = lax.rem(step, 2)

    def columns(c, carry):
        @pl.when(first)
        def _():
            for copy in chunk_loads(c):
                copy.wait()
        norms(jnp.minimum(step + 1, pl.num_programs(0) - 1), c)
        cols = chunk(c)
        u = dot(hm_s[now], wup[:, cols]).astype(BF16).astype(F32)
        dg = dot_nt(dys[rows, :], wdown[cols, :]).astype(BF16).astype(F32)
        cdf = 0.5 * (1.0 + lax.erf(u * math.sqrt(0.5)))
        gelu = (u * cdf).astype(BF16)
        pdf = jnp.exp(-0.5 * u * u) * (1.0 / math.sqrt(2.0 * math.pi))
        dh = (dg * (cdf + u * pdf)).astype(BF16)
        dh_ref[:, cols] = dh
        down_acc[cols, :] += dot(gelu.T, dys[rows, :])
        up_acc[:, cols] += dot(hm_t[now], dh)

        @pl.when(last)
        def _():
            for copy in flush(c):
                copy.start()
        return carry
    lax.fori_loop(0, chunks, columns, 0)
    @pl.when(first)
    def _():
        for copy in w_loads:
            copy.wait()
    dctx_ref[:] = dot_nt(wout[:], dys[rows, :]).astype(BF16)
    position = token_tile(step) * TT + lax.broadcasted_iota(jnp.int32, cos_ref.shape, 1)
    angles = position.astype(F32) * freq_ref[:, pl.ds(0, 1)]
    cos_ref[:] = jnp.cos(angles)
    sin_ref[:] = jnp.sin(angles)

    @pl.when(last)
    def _():
        for copy in swaps:
            copy.wait_send()
        for copy in dy_saves:
            copy.wait()
        for c in range(chunks):
            for copy in flush(c):
                copy.wait()


def token_part(x, dy, ln, wout, wup, wdown):
    D, width = wup.shape
    S, V, dma = jax.ShapeDtypeStruct, pltpu.VMEM, pltpu.SemaphoreType.DMA
    hbm, vmem = pl.BlockSpec(memory_space=pl.ANY), pl.BlockSpec(memory_space=pltpu.VMEM)
    steps, halves = T // TT, HALF // TT
    freq = np.tile((ROPE_BASE ** (np.arange(0, -HEAD, -2) / HEAD)).astype(np.float32)[:, None], LANES)

    def tok(size):
        return pl.BlockSpec((TT, size), lambda i: (token_tile(i), 0))

    def col(size):
        return pl.BlockSpec((size, TT), lambda i: (0, token_tile(i)))

    return pl.pallas_call(
        token_kernel,
        grid=(steps,),
        in_specs=[hbm, hbm, vmem, vmem] + [hbm] * 3,
        out_specs=[col(D), col(wout.shape[0]), tok(width), col(HEAD // 2), col(HEAD // 2), hbm, hbm, hbm],
        out_shape=[S((D, T), BF16), S((wout.shape[0], T), BF16), S((T, width), BF16),
                   S((HEAD // 2, T), F32), S((HEAD // 2, T), F32), S((T, D), BF16),
                   S((D, width), F32), S((width, D), F32)],
        scratch_shapes=[V((T, D), BF16)] * 2 + [V(w.shape, BF16) for w in (wout, wup, wdown)]
        + [V((D, TT), BF16), V((2, TT, D), BF16), V((2, D, TT), BF16), V((D, width), F32), V((width, D), F32)]
        + [dma((2, halves)), dma((1,)), dma((2, width // FC)), dma((2, width // FC)), dma((2,)), dma((2,)), dma((2,))],
        compiler_params=pltpu.CompilerParams(dimension_semantics=("arbitrary",), vmem_limit_bytes=VMEM_LIMIT,
                                             collective_id=2, has_side_effects=True),
        name="token_part",
    )(x, dy, ln, freq, wout, wup, wdown)


def attention_pair(ha_ref, w_ref, dctx_ref, cos_ref, sin_ref, dqkv_ref, ctx_ref, qkv_ref, q_t, k_t, k_n, v_n, do_n, p_s, dp_s, dk_acc, dv_acc, slot):
    lane = lax.broadcasted_iota(jnp.int32, (TILE, PAIR), 1)
    key = lax.broadcasted_iota(jnp.int32, (TILE, 2 * TILE), 0)
    query = lax.broadcasted_iota(jnp.int32, (TILE, 2 * TILE), 1) % TILE

    def tile_at(j):
        return pl.ds(j * TILE, TILE)

    def head_rows(head, part):
        return pl.ds((3 * head + part) * HEAD, HEAD)

    def halves(x):
        return x[:HEAD // 2].astype(F32), x[HEAD // 2:].astype(F32)

    def rotate(x, cols, sign):
        cos, sin = cos_ref[:, cols], sin_ref[:, cols] * sign
        lo, hi = halves(x)
        return jnp.concatenate([lo * cos - hi * sin, hi * cos + lo * sin], axis=0).astype(BF16)

    def prepare(j):
        cols = tile_at(j)
        qkv_ref[:, cols] = dot(w_ref[:], ha_ref[:, cols]).astype(BF16)
        for head in range(2):
            rows = pl.ds(head * HEAD, HEAD)
            q_t[rows, cols] = rotate(qkv_ref[head_rows(head, 0), cols], cols, 1.0) * jnp.asarray(HEAD ** -0.5, BF16)
            k_t[rows, cols] = rotate(qkv_ref[head_rows(head, 1), cols], cols, 1.0)
        k_n[cols, :] = k_t[:, cols].T
        v_n[cols, :] = jnp.concatenate([qkv_ref[head_rows(head, 2), cols] for head in range(2)], axis=0).T
        do_n[cols, :] = dctx_ref[:, cols].T

    def split_lanes(x):
        zero = jnp.zeros_like(x)
        return jnp.concatenate([jnp.where(lane < HEAD, x, zero), jnp.where(lane < HEAD, zero, x)], axis=0)

    def split_rows(x):
        zero = jnp.zeros((HEAD, TILE), x.dtype)
        return jnp.concatenate([jnp.concatenate([x[:HEAD], zero], axis=1), jnp.concatenate([zero, x[HEAD:]], axis=1)], axis=0)

    def fold(x, op):
        parts = [x[r:r + 8] for r in range(0, TILE, 8)]
        while len(parts) > 1:
            parts = [op(a, b) for a, b in zip(parts[::2], parts[1::2])]
        return parts[0]

    def gather(old, new, op):
        return new if old is None else op(old, new)

    blocks = list(reversed(range(T // TILE)))
    before = {i: sum(b + 1 for b in blocks[:n]) for n, i in enumerate(blocks)}

    def p_at(i, j):
        return pl.ds((before[i] + j) % P_TILES * TILE, TILE)

    def dp_at(i, j):
        return pl.ds((before[i] + j) % DP_TILES * TILE, TILE)

    def scores(i, state):
        q_split = split_rows(q_t[:, tile_at(i)])
        top = None
        for j in range(i + 1):
            s = dot(k_n[tile_at(j), :], q_split)
            if j == i:
                s = jnp.where(query >= key, s, -1e30)
            p_s[p_at(i, j), :] = s
            top = gather(top, fold(s, jnp.maximum), jnp.maximum)
            if j == i:
                state['max'] = jnp.max(top, axis=0, keepdims=True)
            yield

    def weights(i, state):
        do_split = split_rows(dctx_ref[:, tile_at(i)])
        total = both = None
        for j in range(i + 1):
            dp = dot(v_n[tile_at(j), :], do_split).astype(BF16)
            dp_s[dp_at(i, j), :] = dp
            p = jnp.exp2((p_s[p_at(i, j), :] - state['max']) * LOG2E)
            p_s[p_at(i, j), :] = p
            total = gather(total, fold(p, jnp.add), jnp.add)
            both = gather(both, fold(p * dp.astype(F32), jnp.add), jnp.add)
            if j == i:
                state['inv'] = 1.0 / jnp.sum(total, axis=0, keepdims=True)
                state['delta'] = jnp.sum(both, axis=0, keepdims=True) * state['inv']
            yield

    def grads(i, state):
        cols = tile_at(i)
        do_pair = split_lanes(do_n[cols, :])
        ctx, dq = [None] * 2, [None] * 2
        for j in range(i + 1):
            keys = tile_at(j)
            p = p_s[p_at(i, j), :] * state['inv']
            p_bf = p.astype(BF16)
            ds_bf = (p * (dp_s[dp_at(i, j), :].astype(F32) - state['delta'])).astype(BF16)
            for head in range(2):
                side = slice(head * TILE, (head + 1) * TILE)
                ctx[head] = gather(ctx[head], dot(qkv_ref[head_rows(head, 2), keys], p_bf[:, side]), jnp.add)
                dq[head] = gather(dq[head], dot(k_t[pl.ds(head * HEAD, HEAD), keys], ds_bf[:, side]), jnp.add)
            dv = dot(p_bf, do_pair)
            dv_acc[keys, :] = dv if i == blocks[0] else dv_acc[keys, :] + dv
            for head in range(2):
                rows = pl.ds(head * HEAD, HEAD)
                dk = dot_nt(q_t[rows, cols], ds_bf[:, head * TILE:(head + 1) * TILE])
                dk_acc[rows, keys] = dk if i == blocks[0] else dk_acc[rows, keys] + dk
            if j == i:
                dk, dv = dk_acc[:, cols].astype(BF16), dv_acc[cols, :].astype(BF16).T
                for head in range(2):
                    rows = pl.ds(head * HEAD, HEAD)
                    side = slice(head * HEAD, (head + 1) * HEAD)
                    ctx_ref[rows, cols] = ctx[head].astype(BF16)
                    dqkv_ref[head_rows(head, 0), cols] = rotate((dq[head] * HEAD ** -0.5).astype(BF16), cols, -1.0)
                    dqkv_ref[head_rows(head, 1), cols] = rotate(dk[side], cols, -1.0)
                    dqkv_ref[head_rows(head, 2), cols] = dv[side]
            yield

    slot(0)
    for j in range(T // TILE):
        prepare(j)
    states = {i: {} for i in blocks}
    for n in range(len(blocks) + 2):
        work = []
        for stage, make in ((n - 2, grads), (n - 1, weights), (n, scores)):
            if 0 <= stage < len(blocks):
                i = blocks[stage]
                run = make(i, states[i])
                work += [((j + 0.5) / (i + 1), run) for j in range(i + 1)]
        for _, run in sorted(work, key=lambda item: item[0]):
            next(run)
        if n in SLOT_AFTER:
            slot(SLOT_AFTER[n])


P_TILES, DP_TILES = 16, 9
SLOT_AFTER = {2: 1, 4: 2, 6: 3, 9: 4}


def attention_scratch():
    V = pltpu.VMEM
    return [V((3 * PAIR, T), BF16)] + [V((PAIR, T), BF16)] * 2 + [V((T, PAIR), BF16)] * 3 + [V((P_TILES * TILE, 2 * TILE), F32), V((DP_TILES * TILE, 2 * TILE), BF16)] \
        + [V((PAIR, T), F32), V((T, PAIR), F32)]


SCHEDULE = {
    (0, 0): (('start', 0),),
    (1, 2): (('add', 0), ('pass_on', 0)),
    (2, 2): (('finish', 0), ('start', 1)),
    (3, 1): (('add', 1), ('pass_on', 1)),
    (3, 2): (('finish', 1), ('start', 2)),
    (3, 3): (('add', 2), ('pass_on', 2)),
    (3, 4): (('finish', 2),),
}


def attention_kernel(ha_ref, w_ref, dctx_ref, cos_ref, sin_ref, up_ref, down_ref, dqkv_ref, ctx_ref, up_out, down_out, *refs):
    count = len(attention_scratch())
    groups = plan_sums((up_ref, down_ref), (PLAN_UP, PLAN_DOWN), refs[count:])
    every = groups[0] + groups[1]

    def slot(place):
        for (pair, at), stages in SCHEDULE.items():
            if at != place:
                continue

            @pl.when(pl.program_id(0) == pair)
            def _(pair=pair, stages=stages):
                if (pair, place) == (0, 0):
                    greet([ring_chip(axis, ahead) for axis in AXES for ahead in (1, 3)])
                for stage, phase in stages:
                    for one in every:
                        getattr(one, stage)(phase)
                if (pair, place) == list(SCHEDULE)[-1]:
                    for out, sums in zip((up_out, down_out), groups):
                        for one in sums:
                            out[:, one.cols] = one.result[:]
                            one.drain()

    attention_pair(ha_ref, w_ref, dctx_ref, cos_ref, sin_ref, dqkv_ref, ctx_ref, *refs[:count], slot)


def attention(ha_t, wqkv_t, dctx_t, cos_t, sin_t, g_up, g_down):
    pairs = dctx_t.shape[0] // PAIR
    S = jax.ShapeDtypeStruct
    shares = [(g.shape[0] // 64, g.shape[1]) for g in (g_up, g_down)]
    hbm = pl.BlockSpec(memory_space=pl.ANY)

    def by_pair(rows):
        return pl.BlockSpec((rows, T), lambda p: (p, 0))

    def fixed(shape):
        return pl.BlockSpec(shape, lambda p: (0, 0), pipeline_mode=pl.Buffered(1))

    return pl.pallas_call(
        attention_kernel,
        grid=(pairs,),
        in_specs=[fixed(ha_t.shape), pl.BlockSpec((3 * PAIR, wqkv_t.shape[1]), lambda p: (p, 0)), by_pair(PAIR), fixed(cos_t.shape), fixed(sin_t.shape), hbm, hbm],
        out_specs=[by_pair(3 * PAIR), by_pair(PAIR)] + [fixed(share) for share in shares],
        out_shape=[S((wqkv_t.shape[0], T), BF16), S(dctx_t.shape, BF16)] + [S(share, F32) for share in shares],
        scratch_shapes=attention_scratch() + plan_scratch((PLAN_UP, PLAN_DOWN)),
        compiler_params=pltpu.CompilerParams(dimension_semantics=("arbitrary",), vmem_limit_bytes=VMEM_LIMIT,
                                             collective_id=0, has_side_effects=True),
        name="attention",
    )(ha_t, wqkv_t, dctx_t, cos_t, sin_t, *(g.reshape((RING,) * 3 + (-1, g.shape[1])) for g in (g_up, g_down)))


DURING_TOKENS = {4: ('B+0', 'b!0')}
DURING_MLP = {0: ('C+0', 'c!0'), 3: ('A=0', 'a+0')}
DURING_NORMS = {0: ('B=0', 'b+0'), 2: ('C=0',), 4: ('c+0',), 5: ('A+1', 'a=0')}
AFTER_NORMS = (
    ('B+1', 'b=0', 'c=0', 'C+1', 'a+1', 'A=1'),
    ('b+1', 'c+1', 'B=1', 'a=1', 'C=1', 'A+2'),
    ('b=1', 'c=1', 'B+2', 'a+2', 'C+2', 'A=2'),
    ('b+2', 'c+2', 'B=2', 'a=2', 'C=2'),
    ('b=2', 'c=2'),
)


def tail_kernel(hat_hbm, dqkv_hbm, ctx_hbm, dy_hbm, w_hbm, x_hbm, wup_hbm, dh_hbm, ln_ref, gx_ref, gln_ref, gqkv_ref, gout_ref,
                hat, dqkv, ctx, dy, w, x, wup, dhm_s, dhm_in, dha_s, dha_in, g_qkv, g_out, pair_s, ring_s,
                load, mlp_sem, send, recv, ring_send, ring_recv, *sum_refs):
    core = lax.axis_index('tp')
    own, away = core * HALF, (1 - core) * HALF
    groups = plan_sums((g_qkv, g_out), (PLAN_QKV, PLAN_OUT), sum_refs, True)
    qkv_sums = groups[0]
    sums = dict(zip('ABCabc', groups[0] + groups[1]))
    block = dqkv.shape[0] // len(qkv_sums)

    def rows_of(ref, start, size):
        return ref.at[pl.ds(start, size)]

    pieces = [(hat_hbm, hat)] + [(rows_of(dqkv_hbm, n * block, block), rows_of(dqkv, n * block, block)) for n in range(3)]
    pieces += [(ctx_hbm, ctx), (dy_hbm, dy), (w_hbm, w), (x_hbm, x), (wup_hbm, wup)]
    loads = [pltpu.make_async_copy(src, dst, load.at[n]) for n, (src, dst) in enumerate(pieces)]
    for copy in loads:
        copy.start()
    greet([ring_chip(axis, ahead) for axis in AXES for ahead in (1, 2, 3)] + [other_core()])
    dhm_copy = send_to(other_core(), dhm_s.at[0], dhm_in, send.at[0], recv.at[0])
    dha_copy = send_to(other_core(), dha_s.at[0], dha_in, send.at[1], recv.at[1])
    pair_copy = send_to(other_core(), pair_s.at[0], pair_s.at[1], send.at[2], recv.at[2])

    def run(events):
        for name, act, ring in events:
            one, phase = sums[name], int(ring)
            if act == '!':
                one.start(phase)
            elif act == '+':
                one.add(phase)
                one.pass_on(phase)
            else:
                one.finish(phase)
                if phase < len(AXES) - 1:
                    one.start(phase + 1)
                elif name in 'abc':
                    gout_ref[:, one.cols] = one.result[:]
                else:
                    for k in range(one.whole[1] // HEAD):
                        group, part = divmod(one.col // HEAD + k, 3)
                        gqkv_ref[:, part, group, :] = one.result[:, pl.ds(k * HEAD, HEAD)]

    def run_at(k, table):
        for when, events in table.items():
            @pl.when(k == when)
            def _(events=events):
                run(events)

    loads[0].wait()
    per_group = block // TILE

    def columns(k, carry):
        for n in range(len(qkv_sums)):
            @pl.when(k == n * per_group)
            def _(n=n):
                loads[1 + n].wait()
        cols = pl.ds(pl.multiple_of(k * TILE, TILE), TILE)
        g_qkv[:, :, :, :, cols] = dot_nt(hat[:], dqkv[cols, :]).reshape(g_qkv.shape[:4] + (TILE,))
        for n, one in enumerate(qkv_sums):
            @pl.when(k == (n + 1) * per_group - 1)
            def _(one=one):
                one.start(0)
        return carry
    lax.fori_loop(0, len(qkv_sums) * per_group, columns, 0)
    loads[4].wait()
    loads[5].wait()

    def out_columns(k, carry):
        cols = pl.ds(pl.multiple_of(k * TILE, TILE), TILE)
        g_out[:, :, :, :, cols] = dot(ctx[:], dy[:, cols]).reshape(g_out.shape[:4] + (TILE,))
        return carry
    lax.fori_loop(0, dy.shape[1] // TILE, out_columns, 0)
    run(('A+0', 'a!0'))

    def mlp_load(k):
        start = pl.multiple_of(jnp.where(k < 2, away, own) + lax.rem(k, 2) * TT, TT)
        return pltpu.make_async_copy(rows_of(dh_hbm, start, TT), rows_of(hat, lax.rem(k, 2) * TT, TT), mlp_sem.at[lax.rem(k, 2)])

    loads[6].wait()
    mlp_load(0).start()
    mlp_load(1).start()
    tiles = HALF // TILE

    def tokens(k, carry):
        mine = lax.div(k, tiles)
        at = lax.rem(k, tiles) * TILE
        cols = pl.ds(pl.multiple_of(jnp.where(mine == 0, away, own) + at, TILE), TILE)
        dha_s[mine, pl.ds(pl.multiple_of(at, TILE), TILE), :] = dot(dqkv[:, cols].T, w[:]).astype(BF16)

        @pl.when(k == tiles - 1)
        def _():
            dha_copy.start()
        run_at(k, DURING_TOKENS)
        return carry
    lax.fori_loop(0, 2 * tiles, tokens, 0)

    def mlp_tokens(k, carry):
        run_at(k, DURING_MLP)
        mlp_load(k).wait()
        half, mine = lax.rem(k, 2) * TT, lax.div(k, 2)
        at = pl.ds(pl.multiple_of(half, TT), TT)
        dhm_s[mine, at, :] = dot_nt(hat[at, :], wup[:]).astype(BF16)

        @pl.when(k < 2)
        def _():
            mlp_load(k + 2).start()

        @pl.when(k == 1)
        def _():
            dhm_copy.start()
        return carry
    loads[8].wait()
    lax.fori_loop(0, T // TT, mlp_tokens, 0)

    loads[7].wait()
    dhm_copy.wait_recv()
    dha_copy.wait_recv()
    pair_s[0] = jnp.zeros_like(pair_s[0])

    def norm_back(k, carry):
        at = pl.ds(pl.multiple_of(k * SMALL, SMALL), SMALL)
        norm, rstd = normed(x[at, :])
        da = (dha_s[1, at, :].astype(F32) + dha_in[at, :].astype(F32)).astype(BF16).astype(F32)
        dm = (dhm_s[1, at, :].astype(F32) + dhm_in[at, :].astype(F32)).astype(BF16).astype(F32)
        g = da * ln_ref[pl.ds(0, 1), :] + dm * ln_ref[pl.ds(2, 1), :]
        mean_g = lane_mean(g)
        mean_gn = lane_mean(g * norm)
        residual = dy[pl.ds(pl.multiple_of(own + k * SMALL, SMALL), SMALL), :].astype(F32)
        gx_ref[at, :] = (residual + rstd * (g - mean_g - norm * mean_gn)).astype(BF16)
        for row, value in enumerate((da * norm, da, dm * norm, dm)):
            pair_s[0, pl.ds(row, 1), :] += jnp.sum(value, axis=0, keepdims=True)
        return carry

    steps = HALF // SMALL

    def norm_step(k, carry):
        run_at(k, DURING_NORMS)
        return norm_back(k, carry)
    lax.fori_loop(0, steps, norm_step, 0)
    pair_copy.start()

    def ring_copies(phase):
        place = ring_place(AXES[phase])
        return [send_to(ring_chip(AXES[phase], ahead), ring_s.at[phase, place], ring_s.at[phase, place],
                        ring_send.at[phase, ahead], ring_recv.at[phase, ahead]) for ahead in (1, 2, 3)]

    def ring_start(phase, value):
        ring_s[phase, ring_place(AXES[phase])] = value
        for copy in ring_copies(phase):
            copy.start()

    def ring_sum(phase):
        for copy in ring_copies(phase):
            copy.wait_recv()
        return ring_s[phase, 0] + ring_s[phase, 1] + ring_s[phase, 2] + ring_s[phase, 3]

    for n, events in enumerate(AFTER_NORMS):
        run(events)
        if n == 0:
            pair_copy.wait_recv()
            ring_start(0, pair_s[0] + pair_s[1])
        elif n < len(AXES):
            ring_start(n, ring_sum(n - 1))
    gln_ref[:] = ring_sum(2)[:gln_ref.shape[0]]
    for one in sums.values():
        one.drain()
    for copy in (dhm_copy, dha_copy, pair_copy):
        copy.wait_send()
    for phase in range(3):
        for copy in ring_copies(phase):
            copy.wait_send()


def tail(ha_t, dqkv_t, ctx_t, dy, wqkv_t, x, wup, dh, ln):
    D, C = ha_t.shape[0], ctx_t.shape[0]
    S, V = jax.ShapeDtypeStruct, pltpu.VMEM
    hbm, vmem = pl.BlockSpec(memory_space=pl.ANY), pl.BlockSpec(memory_space=pltpu.VMEM)
    own = V((HALF, D), BF16)
    chips = (RING,) * 3
    dma = pltpu.SemaphoreType.DMA
    return pl.pallas_call(
        tail_kernel,
        in_specs=[hbm] * 8 + [vmem],
        out_specs=[vmem] * 4,
        out_shape=[S((HALF, D), BF16), S(ln.shape, F32), S((D // 64, 3, C // HEAD, HEAD), F32), S((C // 64, D), F32)],
        scratch_shapes=[V(a.shape, BF16) for a in (ha_t, dqkv_t, ctx_t, dy, wqkv_t, x, wup)] + [V((2, HALF, D), BF16), own] * 2
        + [V(chips + (D // 64, 3 * C), F32), V(chips + (C // 64, D), F32), V((2, 8, D), F32), V((3, RING, 8, D), F32)]
        + [dma((9,)), dma((2,)), dma((3,)), dma((3,)), dma((3, RING)), dma((3, RING))] + plan_scratch((PLAN_QKV, PLAN_OUT), True),
        compiler_params=pltpu.CompilerParams(vmem_limit_bytes=VMEM_LIMIT, collective_id=1, has_side_effects=True),
        name="tail",
    )(ha_t, dqkv_t, ctx_t, dy, wqkv_t, x, wup, dh, ln)


def output_kernel(*refs):
    ins, outs = refs[:len(refs) // 2], refs[len(refs) // 2:]
    outs[0][:] = ins[0][:]

    @pl.when(pl.program_id(0) == 0)
    def _():
        for src, dst in zip(ins[1:], outs[1:]):
            dst[:] = src[:]


def outputs(grad_x, *rest):
    steps = 2

    def fixed(a):
        return pl.BlockSpec(a.shape, lambda i: (0,) * len(a.shape), pipeline_mode=pl.Buffered(1))

    specs = [pl.BlockSpec((grad_x.shape[0] // steps, grad_x.shape[1]), lambda i: (i, 0))] + [fixed(a) for a in rest]
    return pl.pallas_call(
        output_kernel, grid=(steps,), in_specs=specs, out_specs=specs,
        out_shape=[jax.ShapeDtypeStruct(a.shape, a.dtype) for a in (grad_x, *rest)],
        compiler_params=pltpu.CompilerParams(dimension_semantics=("arbitrary",)),
        name="outputs",
    )(grad_x, *rest)


def solution(mesh):
    def local_step(x_loc, dy_loc, ln_params, w_qkv, w_out, w_up, w_down):
        x_loc, dy_loc = x_loc[0], dy_loc[0]
        wqkv_t = w_qkv.transpose(1, 2, 3, 0).reshape(-1, x_loc.shape[1])
        ha_t, dctx_t, dh, cos_t, sin_t, dy, g_wup, g_wdown = token_part(x_loc, dy_loc, ln_params, w_out, w_up, w_down)
        dqkv_t, ctx_t, grad_wup, grad_wdown = attention(ha_t, wqkv_t, dctx_t, cos_t, sin_t, g_wup, g_wdown)
        grad_x, grad_ln, grad_wqkv, grad_wout = tail(ha_t, dqkv_t, ctx_t, dy, wqkv_t, x_loc, w_up, dh, ln_params)
        grad_x, grad_ln, grad_wqkv, *rest = outputs(grad_x, grad_ln, grad_wqkv, grad_wout, grad_wup, grad_wdown)
        return grad_x[None], grad_ln, grad_wqkv.swapaxes(1, 2), *rest

    act_spec = P('dp', 'tp')
    in_specs = (act_spec, act_spec, P(), P(None, 'tp'), P('tp'), P(None, 'tp'), P('tp'))
    out_specs = (act_spec, P(), P('dp', 'tp'), P(('tp', 'dp')), P('dp', 'tp'), P(('tp', 'dp')))
    return jax.shard_map(local_step, mesh=mesh, in_specs=in_specs, out_specs=out_specs, check_vma=False)
```

```python
import math

import jax
import jax.numpy as jnp
import numpy as np
from jax import lax
from jax.experimental import pallas as pl
from jax.experimental.pallas import tpu as pltpu
from jax.sharding import PartitionSpec as P

NORM_EPS = 1e-5
ROPE_BASE = 10000.0
F32, BF16 = jnp.float32, jnp.bfloat16
LOG2E = math.log2(math.e)
T = 2048
HALF = T // 2
TILE = 256
SMALL = 256
TT = 512
FC = 1024
LANES = 128
HEAD, PAIR = 64, 128
VMEM_LIMIT = 63 << 20
AXES = ('z', 'y', 'x')
AXIS_STRIDE = {'z': 16, 'y': 4, 'x': 1}
RING = 4


def dot(a, b):
    return jnp.dot(a, b, preferred_element_type=F32)


def dot_nt(a, b):
    return lax.dot_general(a, b, (((1,), (1,)), ((), ())), preferred_element_type=F32)


def row_of(ref, n):
    return ref[pl.ds(n, 1), :]


def ring_place(axis):
    return lax.rem(lax.div(lax.axis_index('dp'), AXIS_STRIDE[axis]), RING)


def ring_chip(axis, ahead):
    place = ring_place(axis)
    return {'dp': lax.axis_index('dp') + (lax.rem(place + ahead, RING) - place) * AXIS_STRIDE[axis]}


def other_core():
    return {'tp': 1 - lax.axis_index('tp')}


def send_to(device, src, dst, send_sem, recv_sem):
    return pltpu.make_async_remote_copy(src_ref=src, dst_ref=dst, send_sem=send_sem, recv_sem=recv_sem,
                                        device_id=device, device_id_type=pl.DeviceIdType.MESH)


def greet(devices):
    barrier = pltpu.get_barrier_semaphore()
    for device in devices:
        pl.semaphore_signal(barrier, inc=1, device_id=device, device_id_type=pl.DeviceIdType.MESH)
    pl.semaphore_wait(barrier, len(devices))


class TorusSum:
    @staticmethod
    def half_shape(rows, width, by_cols):
        return (rows, width // 2) if by_cols else (rows // 2, width)

    @staticmethod
    def scratch(rows, width, by_cols, in_vmem):
        half, whole = TorusSum.half_shape(rows, width, by_cols), (rows, width)
        leads = ((RING, RING), (RING,), ())
        shapes = [pltpu.VMEM(lead + shape, F32) for lead in leads for shape in (half,) * 6 + (whole,)]
        shapes += [] if in_vmem else [pltpu.VMEM(leads[0] + half, F32)] * 2
        return shapes + [pltpu.SemaphoreType.DMA((18,)), pltpu.SemaphoreType.DMA((18,)), pltpu.SemaphoreType.DMA((3,))]

    def __init__(self, grad, order, rows, col, width, refs, by_cols, in_vmem):
        self.grad, self.order, self.col, self.by_cols, self.in_vmem = grad, order, col, by_cols, in_vmem
        self.whole, self.half = (rows, width), TorusSum.half_shape(rows, width, by_cols)
        self.cols = pl.ds(col, width)
        self.sums = [refs[7 * n:7 * n + 7] for n in range(3)]
        self.loaded, (self.send, self.recv, self.load) = refs[21:-3], refs[-3:]
        self.kept = [[axis for axis in AXES if axis not in order[:n]] for n in range(3)]

    def part(self, which, col=0):
        shape = self.whole if which == 2 else self.half
        start = [0, col]
        if which == 1:
            start[self.by_cols] += self.half[self.by_cols]
        return tuple(pl.ds(first, size) for first, size in zip(start, shape))

    def block(self, phase, ahead, which):
        index = lax.rem(ring_place(self.order[phase]) + ahead, RING)
        lead = tuple(index if axis == self.order[phase] else slice(None) for axis in self.kept[phase])
        if phase == 0:
            return self.grad.at[lead + self.part(which, self.col)]
        return self.sums[phase - 1][6].at[lead + self.part(which)]

    def load_copy(self, n):
        ahead, which = ((1, 0), (3, 1), (0, 2))[n]
        dst = (*self.loaded, self.sums[0][6])[n]
        return pltpu.make_async_copy(self.block(0, ahead, which), dst, self.load.at[n])

    def copy(self, phase, n):
        bufs = self.sums[phase]
        src = bufs[2 * n - 8] if n >= 4 else self.block(phase, *((2, 0), (1, 1), (2, 1), (3, 0))[n])
        chip = ring_chip(self.order[phase], (1, 1, 3, 3, 1, 3)[n])
        return send_to(chip, src, bufs[n], self.send.at[6 * phase + n], self.recv.at[6 * phase + n])

    def loads(self, phase):
        return phase == 0 and not self.in_vmem

    def start(self, phase):
        for n in (0, 2, 1, 3):
            self.copy(phase, n).start()
        if self.loads(phase):
            for n in range(3):
                self.load_copy(n).start()

    def add(self, phase):
        bufs = self.sums[phase]
        own = self.block(phase, 1, 0), self.block(phase, 3, 1)
        if self.loads(phase):
            own = self.loaded
            self.load_copy(0).wait()
            self.load_copy(1).wait()
        self.copy(phase, 0).wait_recv()
        self.copy(phase, 2).wait_recv()

        def rows(at):
            bufs[0][at] = own[0][at] + bufs[0][at]
            bufs[2][at] = own[1][at] + bufs[2][at]
        self.each(phase, rows)

    def each(self, phase, body):
        if phase == 0:
            def step(n, carry):
                body(n)
                return carry
            lax.fori_loop(0, RING, step, 0)
        else:
            body(slice(None))

    def pass_on(self, phase):
        self.copy(phase, 4).start()
        self.copy(phase, 5).start()

    def finish(self, phase):
        bufs = self.sums[phase]
        lead = (slice(None),) * (2 - phase)
        low, high = bufs[6].at[lead + self.part(0)], bufs[6].at[lead + self.part(1)]
        own = self.block(phase, 0, 0), self.block(phase, 0, 1)
        if self.loads(phase):
            own = low, high
            self.load_copy(2).wait()
        for n in (1, 3, 4, 5):
            self.copy(phase, n).wait_recv()

        def rows(at):
            low[at] = own[0][at] + bufs[3][at] + bufs[4][at]
            high[at] = own[1][at] + bufs[1][at] + bufs[5][at]
        self.each(phase, rows)

    def drain(self):
        for phase in range(3):
            for n in range(6):
                self.copy(phase, n).wait_send()

    @property
    def result(self):
        return self.sums[2][6]


def plan_columns(rows, tiles, by_cols=False):
    plan, col, orders = [], 0, (('x', 'y', 'z'), ('y', 'z', 'x'), ('z', 'x', 'y'))
    for n, count in enumerate(tiles):
        plan.append((orders[n % len(orders)], rows, col, count * LANES, by_cols))
        col += count * LANES
    return plan


def plan_scratch(plans, in_vmem=False):
    return [shape for plan in plans for _, rows, _, width, by_cols in plan for shape in TorusSum.scratch(rows, width, by_cols, in_vmem)]


def plan_sums(grads, plans, refs, in_vmem=False):
    groups = []
    for grad, plan in zip(grads, plans):
        groups.append([])
        for order, rows, col, width, by_cols in plan:
            count = len(TorusSum.scratch(rows, width, by_cols, in_vmem))
            groups[-1].append(TorusSum(grad, order, rows, col, width, refs[:count], by_cols, in_vmem))
            refs = refs[count:]
    return groups


PLAN_UP = plan_columns(16, (5, 5, 6))
PLAN_DOWN = plan_columns(32, (3, 3, 2))
PLAN_QKV = plan_columns(16, (4, 4, 4))
PLAN_OUT = plan_columns(8, (4, 2, 2), True)


def lane_mean(x):
    return jnp.mean(x, axis=-1, keepdims=True)


def normed(x):
    x = x.astype(F32)
    centered = x - lane_mean(x)
    rstd = lax.rsqrt(lane_mean(centered * centered) + NORM_EPS)
    return centered * rstd, rstd


def token_tile(step):
    core, halves = lax.axis_index('tp'), HALF // TT
    return jnp.where(step < halves, core * halves + step, (1 - core) * halves + step - halves)


def token_kernel(x_hbm, dy_hbm, ln_ref, freq_ref, wout_hbm, wup_hbm, wdown_hbm,
                 ha_ref, dctx_ref, dh_ref, cos_ref, sin_ref, dy_ref, gup_ref, gdown_ref,
                 xs, dys, wout, wup, wdown, ha_s, hm_s, hm_t, up_acc, down_acc,
                 row_load, w_load, chunk_load, flush_sem, dy_sem, send, recv):
    step = pl.program_id(0)
    first, last = step == 0, step == pl.num_programs(0) - 1
    width = wup.shape[1]
    chunks = width // FC
    rows = pl.ds(pl.multiple_of(step * TT, TT), TT)

    def chunk(c):
        return pl.ds(pl.multiple_of(c * FC, FC), FC)

    def flush(c):
        return (pltpu.make_async_copy(up_acc.at[:, chunk(c)], gup_ref.at[:, chunk(c)], flush_sem.at[0, c]),
                pltpu.make_async_copy(down_acc.at[chunk(c), :], gdown_ref.at[chunk(c), :], flush_sem.at[1, c]))

    def row_loads(n):
        part = pl.ds(n * TT, TT)
        return [pltpu.make_async_copy(src.at[part], dst.at[part], row_load.at[k, n]) for k, (src, dst) in enumerate(((x_hbm, xs), (dy_hbm, dys)))]

    def chunk_loads(c):
        return (pltpu.make_async_copy(wup_hbm.at[:, chunk(c)], wup.at[:, chunk(c)], chunk_load.at[0, c]),
                pltpu.make_async_copy(wdown_hbm.at[chunk(c), :], wdown.at[chunk(c), :], chunk_load.at[1, c]))

    core = lax.axis_index('tp')
    dy_saves = [pltpu.make_async_copy(dys.at[pl.ds(n * HALF, HALF)], dy_ref.at[pl.ds(place * HALF, HALF)], dy_sem.at[n])
                for n, place in enumerate((core, 1 - core))]
    w_loads = [pltpu.make_async_copy(wout_hbm, wout, w_load.at[0])]
    swaps = [send_to(other_core(), src, dst.at[pl.ds(HALF, HALF)], send.at[k], recv.at[k]) for k, (src, dst) in enumerate(((x_hbm, xs), (dy_hbm, dys)))]

    @pl.when(first)
    def _():
        for copy in [*row_loads(0), *(copy for c in range(chunks) for copy in chunk_loads(c)), *w_loads, *row_loads(1)]:
            copy.start()
        up_acc[:] = jnp.zeros_like(up_acc)
        down_acc[:] = jnp.zeros_like(down_acc)
        greet([other_core()])
        for copy in swaps:
            copy.start()

    def norms(n, part):
        size = TT // chunks
        at = pl.ds(pl.multiple_of(part * size, size), size)
        norm, _ = normed(xs[pl.ds(pl.multiple_of(n * TT + part * size, size), size), :])
        hm = (norm * row_of(ln_ref, 2) + row_of(ln_ref, 3)).astype(BF16)
        ha_s[:, at] = (norm * row_of(ln_ref, 0) + row_of(ln_ref, 1)).astype(BF16).T
        slot = lax.rem(n, 2)
        hm_s[slot, at, :] = hm
        hm_t[slot, :, at] = hm.T

    @pl.when(first)
    def _():
        for copy in row_loads(0):
            copy.wait()
        for part in range(chunks):
            norms(0, part)
        for n in range(1, HALF // TT):
            for copy in row_loads(n):
                copy.wait()

    @pl.when(step == HALF // TT - 1)
    def _():
        for copy in swaps:
            copy.wait_recv()
        for copy in dy_saves:
            copy.start()

    ha_ref[:] = ha_s[:]
    now = lax.rem(step, 2)

    def columns(c, carry):
        @pl.when(first)
        def _():
            for copy in chunk_loads(c):
                copy.wait()
        norms(jnp.minimum(step + 1, pl.num_programs(0) - 1), c)
        cols = chunk(c)
        u = dot(hm_s[now], wup[:, cols]).astype(BF16).astype(F32)
        dg = dot_nt(dys[rows, :], wdown[cols, :]).astype(BF16).astype(F32)
        cdf = 0.5 * (1.0 + lax.erf(u * math.sqrt(0.5)))
        gelu = (u * cdf).astype(BF16)
        pdf = jnp.exp(-0.5 * u * u) * (1.0 / math.sqrt(2.0 * math.pi))
        dh = (dg * (cdf + u * pdf)).astype(BF16)
        dh_ref[:, cols] = dh
        down_acc[cols, :] += dot(gelu.T, dys[rows, :])
        up_acc[:, cols] += dot(hm_t[now], dh)

        @pl.when(last)
        def _():
            for copy in flush(c):
                copy.start()
        return carry
    lax.fori_loop(0, chunks, columns, 0)
    @pl.when(first)
    def _():
        for copy in w_loads:
            copy.wait()
    dctx_ref[:] = dot_nt(wout[:], dys[rows, :]).astype(BF16)
    position = token_tile(step) * TT + lax.broadcasted_iota(jnp.int32, cos_ref.shape, 1)
    angles = position.astype(F32) * freq_ref[:, pl.ds(0, 1)]
    cos_ref[:] = jnp.cos(angles)
    sin_ref[:] = jnp.sin(angles)

    @pl.when(last)
    def _():
        for copy in swaps:
            copy.wait_send()
        for copy in dy_saves:
            copy.wait()
        for c in range(chunks):
            for copy in flush(c):
                copy.wait()


def token_part(x, dy, ln, wout, wup, wdown):
    D, width = wup.shape
    S, V, dma = jax.ShapeDtypeStruct, pltpu.VMEM, pltpu.SemaphoreType.DMA
    hbm, vmem = pl.BlockSpec(memory_space=pl.ANY), pl.BlockSpec(memory_space=pltpu.VMEM)
    steps, halves = T // TT, HALF // TT
    freq = np.tile((ROPE_BASE ** (np.arange(0, -HEAD, -2) / HEAD)).astype(np.float32)[:, None], LANES)

    def tok(size):
        return pl.BlockSpec((TT, size), lambda i: (token_tile(i), 0))

    def col(size):
        return pl.BlockSpec((size, TT), lambda i: (0, token_tile(i)))

    return pl.pallas_call(
        token_kernel,
        grid=(steps,),
        in_specs=[hbm, hbm, vmem, vmem] + [hbm] * 3,
        out_specs=[col(D), col(wout.shape[0]), tok(width), col(HEAD // 2), col(HEAD // 2), hbm, hbm, hbm],
        out_shape=[S((D, T), BF16), S((wout.shape[0], T), BF16), S((T, width), BF16),
                   S((HEAD // 2, T), F32), S((HEAD // 2, T), F32), S((T, D), BF16),
                   S((D, width), F32), S((width, D), F32)],
        scratch_shapes=[V((T, D), BF16)] * 2 + [V(w.shape, BF16) for w in (wout, wup, wdown)]
        + [V((D, TT), BF16), V((2, TT, D), BF16), V((2, D, TT), BF16), V((D, width), F32), V((width, D), F32)]
        + [dma((2, halves)), dma((1,)), dma((2, width // FC)), dma((2, width // FC)), dma((2,)), dma((2,)), dma((2,))],
        compiler_params=pltpu.CompilerParams(dimension_semantics=("arbitrary",), vmem_limit_bytes=VMEM_LIMIT,
                                             collective_id=2, has_side_effects=True),
        name="token_part",
    )(x, dy, ln, freq, wout, wup, wdown)


def attention_pair(ha_ref, w_ref, dctx_ref, cos_ref, sin_ref, dqkv_ref, ctx_ref, qkv_ref, q_t, k_t, k_n, v_n, do_n, p_s, dp_s, dk_acc, dv_acc, slot):
    lane = lax.broadcasted_iota(jnp.int32, (TILE, PAIR), 1)
    key = lax.broadcasted_iota(jnp.int32, (TILE, 2 * TILE), 0)
    query = lax.broadcasted_iota(jnp.int32, (TILE, 2 * TILE), 1) % TILE

    def tile_at(j):
        return pl.ds(j * TILE, TILE)

    def head_rows(head, part):
        return pl.ds((3 * head + part) * HEAD, HEAD)

    def halves(x):
        return x[:HEAD // 2].astype(F32), x[HEAD // 2:].astype(F32)

    def rotate(x, cols, sign):
        cos, sin = cos_ref[:, cols], sin_ref[:, cols] * sign
        lo, hi = halves(x)
        return jnp.concatenate([lo * cos - hi * sin, hi * cos + lo * sin], axis=0).astype(BF16)

    def prepare(j):
        cols = tile_at(j)
        qkv_ref[:, cols] = dot(w_ref[:], ha_ref[:, cols]).astype(BF16)
        for head in range(2):
            rows = pl.ds(head * HEAD, HEAD)
            q_t[rows, cols] = rotate(qkv_ref[head_rows(head, 0), cols], cols, 1.0) * jnp.asarray(HEAD ** -0.5, BF16)
            k_t[rows, cols] = rotate(qkv_ref[head_rows(head, 1), cols], cols, 1.0)
        k_n[cols, :] = k_t[:, cols].T
        v_n[cols, :] = jnp.concatenate([qkv_ref[head_rows(head, 2), cols] for head in range(2)], axis=0).T
        do_n[cols, :] = dctx_ref[:, cols].T

    def split_lanes(x):
        zero = jnp.zeros_like(x)
        return jnp.concatenate([jnp.where(lane < HEAD, x, zero), jnp.where(lane < HEAD, zero, x)], axis=0)

    def split_rows(x):
        zero = jnp.zeros((HEAD, TILE), x.dtype)
        return jnp.concatenate([jnp.concatenate([x[:HEAD], zero], axis=1), jnp.concatenate([zero, x[HEAD:]], axis=1)], axis=0)

    def fold(x, op):
        parts = [x[r:r + 8] for r in range(0, TILE, 8)]
        while len(parts) > 1:
            parts = [op(a, b) for a, b in zip(parts[::2], parts[1::2])]
        return parts[0]

    def gather(old, new, op):
        return new if old is None else op(old, new)

    blocks = list(reversed(range(T // TILE)))
    before = {i: sum(b + 1 for b in blocks[:n]) for n, i in enumerate(blocks)}

    def p_at(i, j):
        return pl.ds((before[i] + j) % P_TILES * TILE, TILE)

    def dp_at(i, j):
        return pl.ds((before[i] + j) % DP_TILES * TILE, TILE)

    def scores(i, state):
        q_split = split_rows(q_t[:, tile_at(i)])
        top = None
        for j in range(i + 1):
            s = dot(k_n[tile_at(j), :], q_split)
            if j == i:
                s = jnp.where(query >= key, s, -1e30)
            p_s[p_at(i, j), :] = s
            top = gather(top, fold(s, jnp.maximum), jnp.maximum)
            if j == i:
                state['max'] = jnp.max(top, axis=0, keepdims=True)
            yield

    def weights(i, state):
        do_split = split_rows(dctx_ref[:, tile_at(i)])
        total = both = None
        for j in range(i + 1):
            dp = dot(v_n[tile_at(j), :], do_split).astype(BF16)
            dp_s[dp_at(i, j), :] = dp
            p = jnp.exp2((p_s[p_at(i, j), :] - state['max']) * LOG2E)
            p_s[p_at(i, j), :] = p
            total = gather(total, fold(p, jnp.add), jnp.add)
            both = gather(both, fold(p * dp.astype(F32), jnp.add), jnp.add)
            if j == i:
                state['inv'] = 1.0 / jnp.sum(total, axis=0, keepdims=True)
                state['delta'] = jnp.sum(both, axis=0, keepdims=True) * state['inv']
            yield

    def grads(i, state):
        cols = tile_at(i)
        do_pair = split_lanes(do_n[cols, :])
        ctx, dq = [None] * 2, [None] * 2
        for j in range(i + 1):
            keys = tile_at(j)
            p = p_s[p_at(i, j), :] * state['inv']
            p_bf = p.astype(BF16)
            ds_bf = (p * (dp_s[dp_at(i, j), :].astype(F32) - state['delta'])).astype(BF16)
            for head in range(2):
                side = slice(head * TILE, (head + 1) * TILE)
                ctx[head] = gather(ctx[head], dot(qkv_ref[head_rows(head, 2), keys], p_bf[:, side]), jnp.add)
                dq[head] = gather(dq[head], dot(k_t[pl.ds(head * HEAD, HEAD), keys], ds_bf[:, side]), jnp.add)
            dv = dot(p_bf, do_pair)
            dv_acc[keys, :] = dv if i == blocks[0] else dv_acc[keys, :] + dv
            for head in range(2):
                rows = pl.ds(head * HEAD, HEAD)
                dk = dot_nt(q_t[rows, cols], ds_bf[:, head * TILE:(head + 1) * TILE])
                dk_acc[rows, keys] = dk if i == blocks[0] else dk_acc[rows, keys] + dk
            if j == i:
                dk, dv = dk_acc[:, cols].astype(BF16), dv_acc[cols, :].astype(BF16).T
                for head in range(2):
                    rows = pl.ds(head * HEAD, HEAD)
                    side = slice(head * HEAD, (head + 1) * HEAD)
                    ctx_ref[rows, cols] = ctx[head].astype(BF16)
                    dqkv_ref[head_rows(head, 0), cols] = rotate((dq[head] * HEAD ** -0.5).astype(BF16), cols, -1.0)
                    dqkv_ref[head_rows(head, 1), cols] = rotate(dk[side], cols, -1.0)
                    dqkv_ref[head_rows(head, 2), cols] = dv[side]
            yield

    slot(0)
    for j in range(T // TILE):
        prepare(j)
    states = {i: {} for i in blocks}
    for n in range(len(blocks) + 2):
        work = []
        for stage, make in ((n - 2, grads), (n - 1, weights), (n, scores)):
            if 0 <= stage < len(blocks):
                i = blocks[stage]
                run = make(i, states[i])
                work += [((j + 0.5) / (i + 1), run) for j in range(i + 1)]
        for _, run in sorted(work, key=lambda item: item[0]):
            next(run)
        if n in SLOT_AFTER:
            slot(SLOT_AFTER[n])


P_TILES, DP_TILES = 16, 9
SLOT_AFTER = {2: 1, 4: 2, 6: 3, 9: 4}


def attention_scratch():
    V = pltpu.VMEM
    return [V((3 * PAIR, T), BF16)] + [V((PAIR, T), BF16)] * 2 + [V((T, PAIR), BF16)] * 3 + [V((P_TILES * TILE, 2 * TILE), F32), V((DP_TILES * TILE, 2 * TILE), BF16)] \
        + [V((PAIR, T), F32), V((T, PAIR), F32)]


SCHEDULE = {
    (0, 0): (('start', 0),),
    (1, 3): (('add', 0), ('pass_on', 0)),
    (2, 3): (('finish', 0), ('start', 1)),
    (3, 1): (('add', 1), ('pass_on', 1)),
    (3, 2): (('finish', 1), ('start', 2)),
    (3, 3): (('add', 2), ('pass_on', 2)),
    (3, 4): (('finish', 2),),
}


def attention_kernel(ha_ref, w_ref, dctx_ref, cos_ref, sin_ref, up_ref, down_ref, dqkv_ref, ctx_ref, up_out, down_out, *refs):
    count = len(attention_scratch())
    groups = plan_sums((up_ref, down_ref), (PLAN_UP, PLAN_DOWN), refs[count:])
    every = groups[0] + groups[1]

    def slot(place):
        for (pair, at), stages in SCHEDULE.items():
            if at != place:
                continue

            @pl.when(pl.program_id(0) == pair)
            def _(pair=pair, stages=stages):
                if (pair, place) == (0, 0):
                    greet([ring_chip(axis, ahead) for axis in AXES for ahead in (1, 3)])
                for stage, phase in stages:
                    for one in every:
                        getattr(one, stage)(phase)
                if (pair, place) == list(SCHEDULE)[-1]:
                    for out, sums in zip((up_out, down_out), groups):
                        for one in sums:
                            out[:, one.cols] = one.result[:]
                            one.drain()

    attention_pair(ha_ref, w_ref, dctx_ref, cos_ref, sin_ref, dqkv_ref, ctx_ref, *refs[:count], slot)


def attention(ha_t, wqkv_t, dctx_t, cos_t, sin_t, g_up, g_down):
    pairs = dctx_t.shape[0] // PAIR
    S = jax.ShapeDtypeStruct
    shares = [(g.shape[0] // 64, g.shape[1]) for g in (g_up, g_down)]
    hbm = pl.BlockSpec(memory_space=pl.ANY)

    def by_pair(rows):
        return pl.BlockSpec((rows, T), lambda p: (p, 0))

    def fixed(shape):
        return pl.BlockSpec(shape, lambda p: (0, 0), pipeline_mode=pl.Buffered(1))

    return pl.pallas_call(
        attention_kernel,
        grid=(pairs,),
        in_specs=[fixed(ha_t.shape), pl.BlockSpec((3 * PAIR, wqkv_t.shape[1]), lambda p: (p, 0)), by_pair(PAIR), fixed(cos_t.shape), fixed(sin_t.shape), hbm, hbm],
        out_specs=[by_pair(3 * PAIR), by_pair(PAIR)] + [fixed(share) for share in shares],
        out_shape=[S((wqkv_t.shape[0], T), BF16), S(dctx_t.shape, BF16)] + [S(share, F32) for share in shares],
        scratch_shapes=attention_scratch() + plan_scratch((PLAN_UP, PLAN_DOWN)),
        compiler_params=pltpu.CompilerParams(dimension_semantics=("arbitrary",), vmem_limit_bytes=VMEM_LIMIT,
                                             collective_id=0, has_side_effects=True),
        name="attention",
    )(ha_t, wqkv_t, dctx_t, cos_t, sin_t, *(g.reshape((RING,) * 3 + (-1, g.shape[1])) for g in (g_up, g_down)))


DURING_TOKENS = {2: ('B+0', 'b!0'), 5: ('C+0', 'c!0')}
DURING_MLP = {2: ('A=0', 'a+0'), 3: ('B=0', 'b+0')}
DURING_NORMS = {0: ('C=0', 'c+0'), 1: ('A+1', 'a=0'), 2: ('B+1', 'b=0'), 3: ('c=0', 'C+1')}
AFTER_NORMS = (
    ('a+1', 'A=1', 'B=1', 'b+1'),
    ('c+1', 'C=1', 'A+2', 'a=1', 'B+2', 'b=1'),
    ('c=1', 'C+2', 'A=2', 'a+2', 'b+2', 'B=2'),
    ('c+2', 'a=2', 'b=2', 'C=2'),
    ('c=2',),
)


def tail_kernel(hat_hbm, dqkv_hbm, ctx_hbm, dy_hbm, w_hbm, x_hbm, wup_hbm, dh_hbm, ln_ref, gx_ref, gln_ref, gqkv_ref, gout_ref,
                gx_s, hat, dqkv, ctx, dy, w, x, wup, dhm_s, dhm_in, dha_s, dha_in, g_qkv, g_out, pair_s, ring_s,
                load, mlp_sem, send, recv, ring_send, ring_recv, *sum_refs):
    core = lax.axis_index('tp')
    own, away = core * HALF, (1 - core) * HALF
    groups = plan_sums((g_qkv, g_out), (PLAN_QKV, PLAN_OUT), sum_refs, True)
    qkv_sums = groups[0]
    sums = dict(zip('ABCabc', groups[0] + groups[1]))
    block = dqkv.shape[0] // len(qkv_sums)

    def rows_of(ref, start, size):
        return ref.at[pl.ds(start, size)]

    pieces = [(hat_hbm, hat)] + [(rows_of(dqkv_hbm, n * block, block), rows_of(dqkv, n * block, block)) for n in range(3)]
    pieces += [(ctx_hbm, ctx), (dy_hbm, dy), (w_hbm, w), (x_hbm, x), (wup_hbm, wup)]
    loads = [pltpu.make_async_copy(src, dst, load.at[n]) for n, (src, dst) in enumerate(pieces)]
    for copy in loads:
        copy.start()
    greet([ring_chip(axis, ahead) for axis in AXES for ahead in (1, 2, 3)] + [other_core()])
    dhm_copy = send_to(other_core(), dhm_s.at[0], dhm_in, send.at[0], recv.at[0])
    dha_copy = send_to(other_core(), dha_s.at[0], dha_in, send.at[1], recv.at[1])
    pair_copy = send_to(other_core(), pair_s.at[0], pair_s.at[1], send.at[2], recv.at[2])

    def run(events):
        for name, act, ring in events:
            one, phase = sums[name], int(ring)
            if act == '!':
                one.start(phase)
            elif act == '+':
                one.add(phase)
                one.pass_on(phase)
            else:
                one.finish(phase)
                if phase < len(AXES) - 1:
                    one.start(phase + 1)
                elif name in 'abc':
                    gout_ref[:, one.cols] = one.result[:]
                else:
                    for k in range(one.whole[1] // HEAD):
                        group, part = divmod(one.col // HEAD + k, 3)
                        gqkv_ref[:, part, group, :] = one.result[:, pl.ds(k * HEAD, HEAD)]

    def run_at(k, table):
        for when, events in table.items():
            @pl.when(k == when)
            def _(events=events):
                run(events)

    loads[0].wait()
    per_group = block // TILE

    def columns(k, carry):
        for n in range(len(qkv_sums)):
            @pl.when(k == n * per_group)
            def _(n=n):
                loads[1 + n].wait()
        cols = pl.ds(pl.multiple_of(k * TILE, TILE), TILE)
        g_qkv[:, :, :, :, cols] = dot_nt(hat[:], dqkv[cols, :]).reshape(g_qkv.shape[:4] + (TILE,))
        for n, one in enumerate(qkv_sums):
            @pl.when(k == (n + 1) * per_group - 1)
            def _(one=one):
                one.start(0)
        return carry
    lax.fori_loop(0, len(qkv_sums) * per_group, columns, 0)
    loads[4].wait()
    loads[5].wait()

    def out_columns(k, carry):
        cols = pl.ds(pl.multiple_of(k * TILE, TILE), TILE)
        g_out[:, :, :, :, cols] = dot(ctx[:], dy[:, cols]).reshape(g_out.shape[:4] + (TILE,))
        return carry
    lax.fori_loop(0, dy.shape[1] // TILE, out_columns, 0)
    run(('A+0', 'a!0'))

    def mlp_load(k):
        start = pl.multiple_of(jnp.where(k < 2, away, own) + lax.rem(k, 2) * TT, TT)
        return pltpu.make_async_copy(rows_of(dh_hbm, start, TT), rows_of(hat, lax.rem(k, 2) * TT, TT), mlp_sem.at[lax.rem(k, 2)])

    loads[6].wait()
    mlp_load(0).start()
    mlp_load(1).start()
    tiles = HALF // TILE

    def tokens(k, carry):
        mine = lax.div(k, tiles)
        at = lax.rem(k, tiles) * TILE
        cols = pl.ds(pl.multiple_of(jnp.where(mine == 0, away, own) + at, TILE), TILE)
        dha_s[mine, pl.ds(pl.multiple_of(at, TILE), TILE), :] = dot(dqkv[:, cols].T, w[:]).astype(BF16)

        @pl.when(k == tiles - 1)
        def _():
            dha_copy.start()
        run_at(k, DURING_TOKENS)
        return carry
    lax.fori_loop(0, 2 * tiles, tokens, 0)

    def mlp_tokens(k, carry):
        run_at(k, DURING_MLP)
        mlp_load(k).wait()
        half, mine = lax.rem(k, 2) * TT, lax.div(k, 2)
        at = pl.ds(pl.multiple_of(half, TT), TT)
        dhm_s[mine, at, :] = dot_nt(hat[at, :], wup[:]).astype(BF16)

        @pl.when(k < 2)
        def _():
            mlp_load(k + 2).start()

        @pl.when(k == 1)
        def _():
            dhm_copy.start()
        return carry
    loads[8].wait()
    lax.fori_loop(0, T // TT, mlp_tokens, 0)

    loads[7].wait()
    dhm_copy.wait_recv()
    dha_copy.wait_recv()
    pair_s[0] = jnp.zeros_like(pair_s[0])
    wide = pair_s.shape[2]

    def norm_back(k, carry):
        at = pl.ds(pl.multiple_of(k * SMALL, SMALL), SMALL)
        norm, rstd = normed(x[at, :])
        da = (dha_s[1, at, :].astype(F32) + dha_in[at, :].astype(F32)).astype(BF16).astype(F32)
        dm = (dhm_s[1, at, :].astype(F32) + dhm_in[at, :].astype(F32)).astype(BF16).astype(F32)
        g = da * row_of(ln_ref, 0) + dm * row_of(ln_ref, 2)
        mean_g = lane_mean(g)
        mean_gn = lane_mean(g * norm)
        residual = dy[pl.ds(pl.multiple_of(own + k * SMALL, SMALL), SMALL), :].astype(F32)
        gx_s[at, :] = (residual + rstd * (g - mean_g - norm * mean_gn)).astype(BF16)
        for row, value in enumerate((da * norm, da, dm * norm, dm)):
            total = jnp.sum(value, axis=0, keepdims=True)
            for side in range(2):
                pair_s[0, pl.ds(2 * row + side, 1), :] += total[:, side * wide:(side + 1) * wide]
        return carry

    steps = HALF // SMALL

    def norm_step(k, carry):
        run_at(k, DURING_NORMS)
        return norm_back(k, carry)
    lax.fori_loop(0, steps, norm_step, 0)
    pair_copy.start()
    gx_copy = pltpu.make_async_copy(gx_s, gx_ref, load.at[9])
    gx_copy.start()

    def ring_copies(phase):
        place = ring_place(AXES[phase])
        return [send_to(ring_chip(AXES[phase], ahead), ring_s.at[phase, place], ring_s.at[phase, place],
                        ring_send.at[phase, ahead], ring_recv.at[phase, ahead]) for ahead in (1, 2, 3)]

    def ring_start(phase, value):
        ring_s[phase, ring_place(AXES[phase])] = value
        for copy in ring_copies(phase):
            copy.start()

    def ring_sum(phase):
        for copy in ring_copies(phase):
            copy.wait_recv()
        return ring_s[phase, 0] + ring_s[phase, 1] + ring_s[phase, 2] + ring_s[phase, 3]

    for n, events in enumerate(AFTER_NORMS):
        run(events)
        if n == 0:
            pair_copy.wait_recv()
            ring_start(0, pair_s[0] + pair_s[1])
        elif n < len(AXES):
            ring_start(n, ring_sum(n - 1))
    pair_copy.wait_send()
    pair_s[0] = ring_sum(2)
    for row in range(gln_ref.shape[0]):
        for side in range(2):
            gln_ref[pl.ds(row, 1), pl.ds(side * wide, wide)] = row_of(pair_s.at[0], 2 * row + side)
    for one in sums.values():
        one.drain()
    gx_copy.wait()
    for copy in (dhm_copy, dha_copy):
        copy.wait_send()
    for phase in range(3):
        for copy in ring_copies(phase):
            copy.wait_send()


def tail(ha_t, dqkv_t, ctx_t, dy, wqkv_t, x, wup, dh, ln):
    D, C = ha_t.shape[0], ctx_t.shape[0]
    S, V = jax.ShapeDtypeStruct, pltpu.VMEM
    hbm, vmem = pl.BlockSpec(memory_space=pl.ANY), pl.BlockSpec(memory_space=pltpu.VMEM)
    own = V((HALF, D), BF16)
    chips = (RING,) * 3
    dma = pltpu.SemaphoreType.DMA
    return pl.pallas_call(
        tail_kernel,
        in_specs=[hbm] * 8 + [vmem],
        out_specs=[hbm] + [vmem] * 3,
        out_shape=[S((HALF, D), BF16), S(ln.shape, F32), S((D // 64, 3, C // HEAD, HEAD), F32), S((C // 64, D), F32)],
        scratch_shapes=[own] + [V(a.shape, BF16) for a in (ha_t, dqkv_t, ctx_t, dy, wqkv_t, x, wup)] + [V((2, HALF, D), BF16), own] * 2
        + [V(chips + (D // 64, 3 * C), F32), V(chips + (C // 64, D), F32), V((2, 8, D // 2), F32), V((3, RING, 8, D // 2), F32)]
        + [dma((10,)), dma((2,)), dma((3,)), dma((3,)), dma((3, RING)), dma((3, RING))] + plan_scratch((PLAN_QKV, PLAN_OUT), True),
        compiler_params=pltpu.CompilerParams(vmem_limit_bytes=VMEM_LIMIT, collective_id=1, has_side_effects=True),
        name="tail",
    )(ha_t, dqkv_t, ctx_t, dy, wqkv_t, x, wup, dh, ln)


def output_kernel(*refs):
    ins, outs = refs[:len(refs) // 2], refs[len(refs) // 2:]
    outs[0][:] = ins[0][:]

    @pl.when(pl.program_id(0) == 0)
    def _():
        for src, dst in zip(ins[1:], outs[1:]):
            dst[:] = src[:]


def outputs(grad_x, *rest):
    steps = 2

    def fixed(a):
        return pl.BlockSpec(a.shape, lambda i: (0,) * len(a.shape), pipeline_mode=pl.Buffered(1))

    specs = [pl.BlockSpec((grad_x.shape[0] // steps, grad_x.shape[1]), lambda i: (i, 0))] + [fixed(a) for a in rest]
    return pl.pallas_call(
        output_kernel, grid=(steps,), in_specs=specs, out_specs=specs,
        out_shape=[jax.ShapeDtypeStruct(a.shape, a.dtype) for a in (grad_x, *rest)],
        compiler_params=pltpu.CompilerParams(dimension_semantics=("arbitrary",)),
        name="outputs",
    )(grad_x, *rest)


def solution(mesh):
    def local_step(x_loc, dy_loc, ln_params, w_qkv, w_out, w_up, w_down):
        x_loc, dy_loc = x_loc[0], dy_loc[0]
        wqkv_t = w_qkv.transpose(1, 2, 3, 0).reshape(-1, x_loc.shape[1])
        ha_t, dctx_t, dh, cos_t, sin_t, dy, g_wup, g_wdown = token_part(x_loc, dy_loc, ln_params, w_out, w_up, w_down)
        dqkv_t, ctx_t, grad_wup, grad_wdown = attention(ha_t, wqkv_t, dctx_t, cos_t, sin_t, g_wup, g_wdown)
        grad_x, grad_ln, grad_wqkv, grad_wout = tail(ha_t, dqkv_t, ctx_t, dy, wqkv_t, x_loc, w_up, dh, ln_params)
        grad_x, grad_ln, grad_wqkv, *rest = outputs(grad_x, grad_ln, grad_wqkv, grad_wout, grad_wup, grad_wdown)
        return grad_x[None], grad_ln, grad_wqkv.swapaxes(1, 2), *rest

    act_spec = P('dp', 'tp')
    in_specs = (act_spec, act_spec, P(), P(None, 'tp'), P('tp'), P(None, 'tp'), P('tp'))
    out_specs = (act_spec, P(), P('dp', 'tp'), P(('tp', 'dp')), P('dp', 'tp'), P(('tp', 'dp')))
    return jax.shard_map(local_step, mesh=mesh, in_specs=in_specs, out_specs=out_specs, check_vma=False)
```

```python
import math

import jax
import jax.numpy as jnp
import numpy as np
from jax import lax
from jax.experimental import pallas as pl
from jax.experimental.pallas import tpu as pltpu
from jax.sharding import PartitionSpec as P

NORM_EPS = 1e-5
ROPE_BASE = 10000.0
F32, BF16 = jnp.float32, jnp.bfloat16
LOG2E = math.log2(math.e)
T = 2048
HALF = T // 2
TILE = 256
SMALL = 256
TT = 512
FC = 1024
LANES = 128
HEAD, PAIR = 64, 128
VMEM_LIMIT = 63 << 20
AXES = ('z', 'y', 'x')
AXIS_STRIDE = {'z': 16, 'y': 4, 'x': 1}
RING = 4


def dot(a, b):
    return jnp.dot(a, b, preferred_element_type=F32)


def dot_nt(a, b):
    return lax.dot_general(a, b, (((1,), (1,)), ((), ())), preferred_element_type=F32)


def row_of(ref, n):
    return ref[pl.ds(n, 1), :]


def ring_place(axis):
    return lax.rem(lax.div(lax.axis_index('dp'), AXIS_STRIDE[axis]), RING)


def ring_chip(axis, ahead):
    place = ring_place(axis)
    return {'dp': lax.axis_index('dp') + (lax.rem(place + ahead, RING) - place) * AXIS_STRIDE[axis]}


def other_core():
    return {'tp': 1 - lax.axis_index('tp')}


def send_to(device, src, dst, send_sem, recv_sem):
    return pltpu.make_async_remote_copy(src_ref=src, dst_ref=dst, send_sem=send_sem, recv_sem=recv_sem,
                                        device_id=device, device_id_type=pl.DeviceIdType.MESH)


def greet(devices):
    barrier = pltpu.get_barrier_semaphore()
    for device in devices:
        pl.semaphore_signal(barrier, inc=1, device_id=device, device_id_type=pl.DeviceIdType.MESH)
    pl.semaphore_wait(barrier, len(devices))


class TorusSum:
    @staticmethod
    def half_shape(rows, width, by_cols):
        return (rows, width // 2) if by_cols else (rows // 2, width)

    @staticmethod
    def scratch(rows, width, by_cols, in_vmem):
        half, whole = TorusSum.half_shape(rows, width, by_cols), (rows, width)
        leads = ((RING, RING), (RING,), ())
        shapes = [pltpu.VMEM(lead + shape, F32) for lead in leads for shape in (half,) * 6 + (whole,)]
        shapes += [] if in_vmem else [pltpu.VMEM(leads[0] + half, F32)] * 2
        return shapes + [pltpu.SemaphoreType.DMA((18,)), pltpu.SemaphoreType.DMA((18,)), pltpu.SemaphoreType.DMA((3,))]

    def __init__(self, grad, order, rows, col, width, refs, by_cols, in_vmem):
        self.grad, self.order, self.col, self.by_cols, self.in_vmem = grad, order, col, by_cols, in_vmem
        self.whole, self.half = (rows, width), TorusSum.half_shape(rows, width, by_cols)
        self.cols = pl.ds(col, width)
        self.sums = [refs[7 * n:7 * n + 7] for n in range(3)]
        self.loaded, (self.send, self.recv, self.load) = refs[21:-3], refs[-3:]
        self.kept = [[axis for axis in AXES if axis not in order[:n]] for n in range(3)]

    def part(self, which, col=0):
        shape = self.whole if which == 2 else self.half
        start = [0, col]
        if which == 1:
            start[self.by_cols] += self.half[self.by_cols]
        return tuple(pl.ds(first, size) for first, size in zip(start, shape))

    def block(self, phase, ahead, which):
        index = lax.rem(ring_place(self.order[phase]) + ahead, RING)
        lead = tuple(index if axis == self.order[phase] else slice(None) for axis in self.kept[phase])
        if phase == 0:
            return self.grad.at[lead + self.part(which, self.col)]
        return self.sums[phase - 1][6].at[lead + self.part(which)]

    def load_copy(self, n):
        ahead, which = ((1, 0), (3, 1), (0, 2))[n]
        dst = (*self.loaded, self.sums[0][6])[n]
        return pltpu.make_async_copy(self.block(0, ahead, which), dst, self.load.at[n])

    def copy(self, phase, n):
        bufs = self.sums[phase]
        src = bufs[2 * n - 8] if n >= 4 else self.block(phase, *((2, 0), (1, 1), (2, 1), (3, 0))[n])
        chip = ring_chip(self.order[phase], (1, 1, 3, 3, 1, 3)[n])
        return send_to(chip, src, bufs[n], self.send.at[6 * phase + n], self.recv.at[6 * phase + n])

    def loads(self, phase):
        return phase == 0 and not self.in_vmem

    def start(self, phase):
        for n in (0, 2, 1, 3):
            self.copy(phase, n).start()
        if self.loads(phase):
            for n in range(3):
                self.load_copy(n).start()

    def add(self, phase):
        bufs = self.sums[phase]
        own = self.block(phase, 1, 0), self.block(phase, 3, 1)
        if self.loads(phase):
            own = self.loaded
            self.load_copy(0).wait()
            self.load_copy(1).wait()
        self.copy(phase, 0).wait_recv()
        self.copy(phase, 2).wait_recv()

        def rows(at):
            bufs[0][at] = own[0][at] + bufs[0][at]
            bufs[2][at] = own[1][at] + bufs[2][at]
        self.each(phase, rows)

    def each(self, phase, body):
        if phase == 0:
            def step(n, carry):
                body(n)
                return carry
            lax.fori_loop(0, RING, step, 0)
        else:
            body(slice(None))

    def pass_on(self, phase):
        self.copy(phase, 4).start()
        self.copy(phase, 5).start()

    def finish(self, phase):
        bufs = self.sums[phase]
        lead = (slice(None),) * (2 - phase)
        low, high = bufs[6].at[lead + self.part(0)], bufs[6].at[lead + self.part(1)]
        own = self.block(phase, 0, 0), self.block(phase, 0, 1)
        if self.loads(phase):
            own = low, high
            self.load_copy(2).wait()
        for n in (1, 3, 4, 5):
            self.copy(phase, n).wait_recv()

        def rows(at):
            low[at] = own[0][at] + bufs[3][at] + bufs[4][at]
            high[at] = own[1][at] + bufs[1][at] + bufs[5][at]
        self.each(phase, rows)

    def drain(self):
        for phase in range(3):
            for n in range(6):
                self.copy(phase, n).wait_send()

    @property
    def result(self):
        return self.sums[2][6]


def plan_columns(rows, tiles, by_cols=False):
    plan, col, orders = [], 0, (('x', 'y', 'z'), ('y', 'z', 'x'), ('z', 'x', 'y'))
    for n, count in enumerate(tiles):
        plan.append((orders[n % len(orders)], rows, col, count * LANES, by_cols))
        col += count * LANES
    return plan


def plan_scratch(plans, in_vmem=False):
    return [shape for plan in plans for _, rows, _, width, by_cols in plan for shape in TorusSum.scratch(rows, width, by_cols, in_vmem)]


def plan_sums(grads, plans, refs, in_vmem=False):
    groups = []
    for grad, plan in zip(grads, plans):
        groups.append([])
        for order, rows, col, width, by_cols in plan:
            count = len(TorusSum.scratch(rows, width, by_cols, in_vmem))
            groups[-1].append(TorusSum(grad, order, rows, col, width, refs[:count], by_cols, in_vmem))
            refs = refs[count:]
    return groups


PLAN_UP = plan_columns(16, (5, 5, 6))
PLAN_DOWN = plan_columns(32, (3, 3, 2))
PLAN_QKV = plan_columns(16, (4, 4, 4))
PLAN_OUT = plan_columns(8, (4, 2, 2), True)


def lane_mean(x):
    return jnp.mean(x, axis=-1, keepdims=True)


def normed(x):
    x = x.astype(F32)
    centered = x - lane_mean(x)
    rstd = lax.rsqrt(lane_mean(centered * centered) + NORM_EPS)
    return centered * rstd, rstd


def token_tile(step):
    core, halves = lax.axis_index('tp'), HALF // TT
    return jnp.where(step < halves, core * halves + step, (1 - core) * halves + step - halves)


def token_kernel(x_hbm, dy_hbm, ln_ref, freq_ref, wout_hbm, wup_hbm, wdown_hbm,
                 ha_ref, dctx_ref, dh_ref, cos_ref, sin_ref, dy_ref, gup_ref, gdown_ref,
                 xs, dys, wout, wup, wdown, ha_s, hm_s, hm_t, up_acc, down_acc,
                 row_load, w_load, chunk_load, flush_sem, dy_sem, send, recv):
    step = pl.program_id(0)
    first, last = step == 0, step == pl.num_programs(0) - 1
    width = wup.shape[1]
    chunks = width // FC
    rows = pl.ds(pl.multiple_of(step * TT, TT), TT)

    def chunk(c):
        return pl.ds(pl.multiple_of(c * FC, FC), FC)

    def flush(c):
        return (pltpu.make_async_copy(up_acc.at[:, chunk(c)], gup_ref.at[:, chunk(c)], flush_sem.at[0, c]),
                pltpu.make_async_copy(down_acc.at[chunk(c), :], gdown_ref.at[chunk(c), :], flush_sem.at[1, c]))

    def row_loads(n):
        part = pl.ds(n * TT, TT)
        return [pltpu.make_async_copy(src.at[part], dst.at[part], row_load.at[k, n]) for k, (src, dst) in enumerate(((x_hbm, xs), (dy_hbm, dys)))]

    def chunk_loads(c):
        return (pltpu.make_async_copy(wup_hbm.at[:, chunk(c)], wup.at[:, chunk(c)], chunk_load.at[0, c]),
                pltpu.make_async_copy(wdown_hbm.at[chunk(c), :], wdown.at[chunk(c), :], chunk_load.at[1, c]))

    core = lax.axis_index('tp')
    dy_saves = [pltpu.make_async_copy(dys.at[pl.ds(n * HALF, HALF)], dy_ref.at[pl.ds(place * HALF, HALF)], dy_sem.at[n])
                for n, place in enumerate((core, 1 - core))]
    w_loads = [pltpu.make_async_copy(wout_hbm, wout, w_load.at[0])]
    swaps = [send_to(other_core(), src, dst.at[pl.ds(HALF, HALF)], send.at[k], recv.at[k]) for k, (src, dst) in enumerate(((x_hbm, xs), (dy_hbm, dys)))]

    @pl.when(first)
    def _():
        for copy in [*row_loads(0), *(copy for c in range(chunks) for copy in chunk_loads(c)), *w_loads, *row_loads(1)]:
            copy.start()
        up_acc[:] = jnp.zeros_like(up_acc)
        down_acc[:] = jnp.zeros_like(down_acc)
        greet([other_core()])
        for copy in swaps:
            copy.start()

    def norms(n, part):
        size = TT // chunks
        at = pl.ds(pl.multiple_of(part * size, size), size)
        norm, _ = normed(xs[pl.ds(pl.multiple_of(n * TT + part * size, size), size), :])
        hm = (norm * row_of(ln_ref, 2) + row_of(ln_ref, 3)).astype(BF16)
        ha_s[:, at] = (norm * row_of(ln_ref, 0) + row_of(ln_ref, 1)).astype(BF16).T
        slot = lax.rem(n, 2)
        hm_s[slot, at, :] = hm
        hm_t[slot, :, at] = hm.T

    @pl.when(first)
    def _():
        for copy in row_loads(0):
            copy.wait()
        for part in range(chunks):
            norms(0, part)
        for n in range(1, HALF // TT):
            for copy in row_loads(n):
                copy.wait()

    @pl.when(step == HALF // TT - 1)
    def _():
        for copy in swaps:
            copy.wait_recv()
        for copy in dy_saves:
            copy.start()

    ha_ref[:] = ha_s[:]
    now = lax.rem(step, 2)

    def columns(c, carry):
        @pl.when(first)
        def _():
            for copy in chunk_loads(c):
                copy.wait()
        cols = chunk(c)
        u = dot(hm_s[now], wup[:, cols]).astype(BF16).astype(F32)
        dg = dot_nt(dys[rows, :], wdown[cols, :]).astype(BF16).astype(F32)
        cdf = 0.5 * (1.0 + lax.erf(u * math.sqrt(0.5)))
        gelu = (u * cdf).astype(BF16)
        pdf = jnp.exp(-0.5 * u * u) * (1.0 / math.sqrt(2.0 * math.pi))
        dh = (dg * (cdf + u * pdf)).astype(BF16)
        dh_ref[:, cols] = dh
        up_acc[:, cols] += dot(hm_t[now], dh)
        down_acc[cols, :] += dot(gelu.T, dys[rows, :])
        norms(jnp.minimum(step + 1, pl.num_programs(0) - 1), c)

        @pl.when(last)
        def _():
            for copy in flush(c):
                copy.start()
        return carry
    lax.fori_loop(0, chunks, columns, 0)
    @pl.when(first)
    def _():
        for copy in w_loads:
            copy.wait()
    dctx_ref[:] = dot_nt(wout[:], dys[rows, :]).astype(BF16)
    position = token_tile(step) * TT + lax.broadcasted_iota(jnp.int32, cos_ref.shape, 1)
    angles = position.astype(F32) * freq_ref[:, pl.ds(0, 1)]
    cos_ref[:] = jnp.cos(angles)
    sin_ref[:] = jnp.sin(angles)

    @pl.when(last)
    def _():
        for copy in swaps:
            copy.wait_send()
        for copy in dy_saves:
            copy.wait()
        for c in range(chunks):
            for copy in flush(c):
                copy.wait()


def token_part(x, dy, ln, wout, wup, wdown):
    D, width = wup.shape
    S, V, dma = jax.ShapeDtypeStruct, pltpu.VMEM, pltpu.SemaphoreType.DMA
    hbm, vmem = pl.BlockSpec(memory_space=pl.ANY), pl.BlockSpec(memory_space=pltpu.VMEM)
    steps, halves = T // TT, HALF // TT
    freq = np.tile((ROPE_BASE ** (np.arange(0, -HEAD, -2) / HEAD)).astype(np.float32)[:, None], LANES)

    def tok(size):
        return pl.BlockSpec((TT, size), lambda i: (token_tile(i), 0))

    def col(size):
        return pl.BlockSpec((size, TT), lambda i: (0, token_tile(i)))

    return pl.pallas_call(
        token_kernel,
        grid=(steps,),
        in_specs=[hbm, hbm, vmem, vmem] + [hbm] * 3,
        out_specs=[col(D), col(wout.shape[0]), tok(width), col(HEAD // 2), col(HEAD // 2), hbm, hbm, hbm],
        out_shape=[S((D, T), BF16), S((wout.shape[0], T), BF16), S((T, width), BF16),
                   S((HEAD // 2, T), F32), S((HEAD // 2, T), F32), S((T, D), BF16),
                   S((D, width), F32), S((width, D), F32)],
        scratch_shapes=[V((T, D), BF16)] * 2 + [V(w.shape, BF16) for w in (wout, wup, wdown)]
        + [V((D, TT), BF16), V((2, TT, D), BF16), V((2, D, TT), BF16), V((D, width), F32), V((width, D), F32)]
        + [dma((2, halves)), dma((1,)), dma((2, width // FC)), dma((2, width // FC)), dma((2,)), dma((2,)), dma((2,))],
        compiler_params=pltpu.CompilerParams(dimension_semantics=("arbitrary",), vmem_limit_bytes=VMEM_LIMIT,
                                             collective_id=2, has_side_effects=True),
        name="token_part",
    )(x, dy, ln, freq, wout, wup, wdown)


def attention_pair(ha_ref, w_ref, dctx_ref, cos_ref, sin_ref, dqkv_ref, ctx_ref, qkv_ref, q_t, k_t, k_n, v_n, do_n, p_s, dp_s, dk_acc, dv_acc, slot):
    lane = lax.broadcasted_iota(jnp.int32, (TILE, PAIR), 1)
    key = lax.broadcasted_iota(jnp.int32, (TILE, 2 * TILE), 0)
    query = lax.broadcasted_iota(jnp.int32, (TILE, 2 * TILE), 1) % TILE

    def tile_at(j):
        return pl.ds(j * TILE, TILE)

    def head_rows(head, part):
        return pl.ds((3 * head + part) * HEAD, HEAD)

    def halves(x):
        return x[:HEAD // 2].astype(F32), x[HEAD // 2:].astype(F32)

    def rotate(x, cols, sign):
        cos, sin = cos_ref[:, cols], sin_ref[:, cols] * sign
        lo, hi = halves(x)
        return jnp.concatenate([lo * cos - hi * sin, hi * cos + lo * sin], axis=0).astype(BF16)

    def prepare(j):
        cols = tile_at(j)
        qkv_ref[:, cols] = dot(w_ref[:], ha_ref[:, cols]).astype(BF16)
        for head in range(2):
            rows = pl.ds(head * HEAD, HEAD)
            q_t[rows, cols] = rotate(qkv_ref[head_rows(head, 0), cols], cols, 1.0) * jnp.asarray(HEAD ** -0.5, BF16)
            k_t[rows, cols] = rotate(qkv_ref[head_rows(head, 1), cols], cols, 1.0)
        k_n[cols, :] = k_t[:, cols].T
        v_n[cols, :] = jnp.concatenate([qkv_ref[head_rows(head, 2), cols] for head in range(2)], axis=0).T
        do_n[cols, :] = dctx_ref[:, cols].T

    def split_lanes(x):
        zero = jnp.zeros_like(x)
        return jnp.concatenate([jnp.where(lane < HEAD, x, zero), jnp.where(lane < HEAD, zero, x)], axis=0)

    def split_rows(x):
        zero = jnp.zeros((HEAD, TILE), x.dtype)
        return jnp.concatenate([jnp.concatenate([x[:HEAD], zero], axis=1), jnp.concatenate([zero, x[HEAD:]], axis=1)], axis=0)

    def fold(x, op):
        parts = [x[r:r + 8] for r in range(0, TILE, 8)]
        while len(parts) > 1:
            parts = [op(a, b) for a, b in zip(parts[::2], parts[1::2])]
        return parts[0]

    def gather(old, new, op):
        return new if old is None else op(old, new)

    blocks = list(reversed(range(T // TILE)))
    before = {i: sum(b + 1 for b in blocks[:n]) for n, i in enumerate(blocks)}

    def p_at(i, j):
        return pl.ds((before[i] + j) % P_TILES * TILE, TILE)

    def dp_at(i, j):
        return pl.ds((before[i] + j) % DP_TILES * TILE, TILE)

    def scores(i, state):
        q_split = split_rows(q_t[:, tile_at(i)])
        top = None
        for j in range(i + 1):
            s = dot(k_n[tile_at(j), :], q_split)
            if j == i:
                s = jnp.where(query >= key, s, -1e30)
            p_s[p_at(i, j), :] = s
            top = gather(top, fold(s, jnp.maximum), jnp.maximum)
            if j == i:
                state['max'] = jnp.max(top, axis=0, keepdims=True)
            yield

    def weights(i, state):
        do_split = split_rows(dctx_ref[:, tile_at(i)])
        total = both = None
        for j in range(i + 1):
            dp = dot(v_n[tile_at(j), :], do_split).astype(BF16)
            dp_s[dp_at(i, j), :] = dp
            p = jnp.exp2((p_s[p_at(i, j), :] - state['max']) * LOG2E)
            p_s[p_at(i, j), :] = p
            total = gather(total, fold(p, jnp.add), jnp.add)
            both = gather(both, fold(p * dp.astype(F32), jnp.add), jnp.add)
            if j == i:
                state['inv'] = 1.0 / jnp.sum(total, axis=0, keepdims=True)
                state['delta'] = jnp.sum(both, axis=0, keepdims=True) * state['inv']
            yield

    def grads(i, state):
        cols = tile_at(i)
        do_pair = split_lanes(do_n[cols, :])
        ctx, dq = [None] * 2, [None] * 2
        for j in range(i + 1):
            keys = tile_at(j)
            p = p_s[p_at(i, j), :] * state['inv']
            p_bf = p.astype(BF16)
            ds_bf = (p * (dp_s[dp_at(i, j), :].astype(F32) - state['delta'])).astype(BF16)
            for head in range(2):
                side = slice(head * TILE, (head + 1) * TILE)
                ctx[head] = gather(ctx[head], dot(qkv_ref[head_rows(head, 2), keys], p_bf[:, side]), jnp.add)
                dq[head] = gather(dq[head], dot(k_t[pl.ds(head * HEAD, HEAD), keys], ds_bf[:, side]), jnp.add)
            dv = dot(p_bf, do_pair)
            dv_acc[keys, :] = dv if i == blocks[0] else dv_acc[keys, :] + dv
            for head in range(2):
                rows = pl.ds(head * HEAD, HEAD)
                dk = dot_nt(q_t[rows, cols], ds_bf[:, head * TILE:(head + 1) * TILE])
                dk_acc[rows, keys] = dk if i == blocks[0] else dk_acc[rows, keys] + dk
            if j == i:
                dk, dv = dk_acc[:, cols].astype(BF16), dv_acc[cols, :].astype(BF16).T
                for head in range(2):
                    rows = pl.ds(head * HEAD, HEAD)
                    side = slice(head * HEAD, (head + 1) * HEAD)
                    ctx_ref[rows, cols] = ctx[head].astype(BF16)
                    dqkv_ref[head_rows(head, 0), cols] = rotate((dq[head] * HEAD ** -0.5).astype(BF16), cols, -1.0)
                    dqkv_ref[head_rows(head, 1), cols] = rotate(dk[side], cols, -1.0)
                    dqkv_ref[head_rows(head, 2), cols] = dv[side]
            yield

    slot(0)
    for j in range(T // TILE):
        prepare(j)
    states = {i: {} for i in blocks}
    for n in range(len(blocks) + 2):
        work = []
        for stage, make in ((n - 2, grads), (n - 1, weights), (n, scores)):
            if 0 <= stage < len(blocks):
                i = blocks[stage]
                run = make(i, states[i])
                work += [((j + 0.5) / (i + 1), run) for j in range(i + 1)]
        for _, run in sorted(work, key=lambda item: item[0]):
            next(run)
        if n in SLOT_AFTER:
            slot(SLOT_AFTER[n])


P_TILES, DP_TILES = 16, 9
SLOT_AFTER = {2: 1, 4: 2, 6: 3, 9: 4}


def attention_scratch():
    V = pltpu.VMEM
    return [V((3 * PAIR, T), BF16)] + [V((PAIR, T), BF16)] * 2 + [V((T, PAIR), BF16)] * 3 + [V((P_TILES * TILE, 2 * TILE), F32), V((DP_TILES * TILE, 2 * TILE), BF16)] \
        + [V((PAIR, T), F32), V((T, PAIR), F32)]


SCHEDULE = {
    (0, 0): (('start', 0),),
    (1, 3): (('add', 0), ('pass_on', 0)),
    (2, 3): (('finish', 0), ('start', 1)),
    (3, 1): (('add', 1), ('pass_on', 1)),
    (3, 2): (('finish', 1), ('start', 2)),
    (3, 3): (('add', 2), ('pass_on', 2)),
    (3, 4): (('finish', 2),),
}


def attention_kernel(ha_ref, w_ref, dctx_ref, cos_ref, sin_ref, up_ref, down_ref, dqkv_ref, ctx_ref, up_out, down_out, *refs):
    count = len(attention_scratch())
    groups = plan_sums((up_ref, down_ref), (PLAN_UP, PLAN_DOWN), refs[count:])
    every = groups[0] + groups[1]

    def slot(place):
        for (pair, at), stages in SCHEDULE.items():
            if at != place:
                continue

            @pl.when(pl.program_id(0) == pair)
            def _(pair=pair, stages=stages):
                if (pair, place) == (0, 0):
                    greet([ring_chip(axis, ahead) for axis in AXES for ahead in (1, 3)])
                for stage, phase in stages:
                    for one in every:
                        getattr(one, stage)(phase)
                if (pair, place) == list(SCHEDULE)[-1]:
                    for out, sums in zip((up_out, down_out), groups):
                        for one in sums:
                            out[:, one.cols] = one.result[:]
                            one.drain()

    attention_pair(ha_ref, w_ref, dctx_ref, cos_ref, sin_ref, dqkv_ref, ctx_ref, *refs[:count], slot)


def attention(ha_t, wqkv_t, dctx_t, cos_t, sin_t, g_up, g_down):
    pairs = dctx_t.shape[0] // PAIR
    S = jax.ShapeDtypeStruct
    shares = [(g.shape[0] // 64, g.shape[1]) for g in (g_up, g_down)]
    hbm = pl.BlockSpec(memory_space=pl.ANY)

    def by_pair(rows):
        return pl.BlockSpec((rows, T), lambda p: (p, 0))

    def fixed(shape):
        return pl.BlockSpec(shape, lambda p: (0, 0), pipeline_mode=pl.Buffered(1))

    return pl.pallas_call(
        attention_kernel,
        grid=(pairs,),
        in_specs=[fixed(ha_t.shape), pl.BlockSpec((3 * PAIR, wqkv_t.shape[1]), lambda p: (p, 0)), by_pair(PAIR), fixed(cos_t.shape), fixed(sin_t.shape), hbm, hbm],
        out_specs=[by_pair(3 * PAIR), by_pair(PAIR)] + [fixed(share) for share in shares],
        out_shape=[S((wqkv_t.shape[0], T), BF16), S(dctx_t.shape, BF16)] + [S(share, F32) for share in shares],
        scratch_shapes=attention_scratch() + plan_scratch((PLAN_UP, PLAN_DOWN)),
        compiler_params=pltpu.CompilerParams(dimension_semantics=("arbitrary",), vmem_limit_bytes=VMEM_LIMIT,
                                             collective_id=0, has_side_effects=True),
        name="attention",
    )(ha_t, wqkv_t, dctx_t, cos_t, sin_t, *(g.reshape((RING,) * 3 + (-1, g.shape[1])) for g in (g_up, g_down)))


DURING_TOKENS = {2: ('B+0', 'b!0'), 5: ('C+0', 'c!0')}
DURING_MLP = {2: ('A=0', 'a+0'), 3: ('B=0', 'b+0')}
DURING_NORMS = {0: ('C=0', 'c+0'), 1: ('A+1', 'a=0'), 2: ('B+1', 'b=0'), 3: ('c=0', 'C+1')}
AFTER_NORMS = (
    ('a+1', 'A=1', 'B=1', 'b+1'),
    ('c+1', 'C=1', 'A+2', 'a=1', 'B+2', 'b=1'),
    ('c=1', 'C+2', 'A=2', 'a+2', 'b+2', 'B=2'),
    ('c+2', 'a=2', 'b=2', 'C=2'),
    ('c=2',),
)


def tail_kernel(hat_hbm, dqkv_hbm, ctx_hbm, dy_hbm, w_hbm, x_hbm, wup_hbm, dh_hbm, ln_ref, gx_ref, gln_ref, gqkv_ref, gout_ref,
                gx_s, hat, dqkv, ctx, dy, w, x, wup, dhm_s, dhm_in, dha_s, dha_in, g_qkv, g_out, pair_s, ring_s,
                load, mlp_sem, send, recv, ring_send, ring_recv, *sum_refs):
    core = lax.axis_index('tp')
    own, away = core * HALF, (1 - core) * HALF
    groups = plan_sums((g_qkv, g_out), (PLAN_QKV, PLAN_OUT), sum_refs, True)
    qkv_sums = groups[0]
    sums = dict(zip('ABCabc', groups[0] + groups[1]))
    block = dqkv.shape[0] // len(qkv_sums)

    def rows_of(ref, start, size):
        return ref.at[pl.ds(start, size)]

    pieces = [(hat_hbm, hat)] + [(rows_of(dqkv_hbm, n * block, block), rows_of(dqkv, n * block, block)) for n in range(3)]
    pieces += [(ctx_hbm, ctx), (dy_hbm, dy), (w_hbm, w), (x_hbm, x), (wup_hbm, wup)]
    loads = [pltpu.make_async_copy(src, dst, load.at[n]) for n, (src, dst) in enumerate(pieces)]
    for copy in loads:
        copy.start()
    greet([ring_chip(axis, ahead) for axis in AXES for ahead in (1, 2, 3)] + [other_core()])
    dhm_copy = send_to(other_core(), dhm_s.at[0], dhm_in, send.at[0], recv.at[0])
    dha_copy = send_to(other_core(), dha_s.at[0], dha_in, send.at[1], recv.at[1])
    pair_copy = send_to(other_core(), pair_s.at[0], pair_s.at[1], send.at[2], recv.at[2])

    def run(events):
        for name, act, ring in events:
            one, phase = sums[name], int(ring)
            if act == '!':
                one.start(phase)
            elif act == '+':
                one.add(phase)
                one.pass_on(phase)
            else:
                one.finish(phase)
                if phase < len(AXES) - 1:
                    one.start(phase + 1)
                elif name in 'abc':
                    gout_ref[:, one.cols] = one.result[:]
                else:
                    for k in range(one.whole[1] // HEAD):
                        group, part = divmod(one.col // HEAD + k, 3)
                        gqkv_ref[:, part, group, :] = one.result[:, pl.ds(k * HEAD, HEAD)]

    def run_at(k, table):
        for when, events in table.items():
            @pl.when(k == when)
            def _(events=events):
                run(events)

    loads[0].wait()
    per_group = block // TILE

    def columns(k, carry):
        for n in range(len(qkv_sums)):
            @pl.when(k == n * per_group)
            def _(n=n):
                loads[1 + n].wait()
        cols = pl.ds(pl.multiple_of(k * TILE, TILE), TILE)
        g_qkv[:, :, :, :, cols] = dot_nt(hat[:], dqkv[cols, :]).reshape(g_qkv.shape[:4] + (TILE,))
        for n, one in enumerate(qkv_sums):
            @pl.when(k == (n + 1) * per_group - 1)
            def _(one=one):
                one.start(0)
        return carry
    lax.fori_loop(0, len(qkv_sums) * per_group, columns, 0)
    loads[4].wait()
    loads[5].wait()

    def out_columns(k, carry):
        cols = pl.ds(pl.multiple_of(k * TILE, TILE), TILE)
        g_out[:, :, :, :, cols] = dot(ctx[:], dy[:, cols]).reshape(g_out.shape[:4] + (TILE,))
        return carry
    lax.fori_loop(0, dy.shape[1] // TILE, out_columns, 0)
    run(('A+0', 'a!0'))

    def mlp_load(k):
        start = pl.multiple_of(jnp.where(k < 2, away, own) + lax.rem(k, 2) * TT, TT)
        return pltpu.make_async_copy(rows_of(dh_hbm, start, TT), rows_of(hat, lax.rem(k, 2) * TT, TT), mlp_sem.at[lax.rem(k, 2)])

    loads[6].wait()
    mlp_load(0).start()
    mlp_load(1).start()
    tiles = HALF // TILE

    def tokens(k, carry):
        mine = lax.div(k, tiles)
        at = lax.rem(k, tiles) * TILE
        cols = pl.ds(pl.multiple_of(jnp.where(mine == 0, away, own) + at, TILE), TILE)
        dha_s[mine, pl.ds(pl.multiple_of(at, TILE), TILE), :] = dot(dqkv[:, cols].T, w[:]).astype(BF16)

        @pl.when(k == tiles - 1)
        def _():
            dha_copy.start()
        run_at(k, DURING_TOKENS)
        return carry
    lax.fori_loop(0, 2 * tiles, tokens, 0)

    def mlp_tokens(k, carry):
        run_at(k, DURING_MLP)
        mlp_load(k).wait()
        half, mine = lax.rem(k, 2) * TT, lax.div(k, 2)
        at = pl.ds(pl.multiple_of(half, TT), TT)
        dhm_s[mine, at, :] = dot_nt(hat[at, :], wup[:]).astype(BF16)

        @pl.when(k < 2)
        def _():
            mlp_load(k + 2).start()

        @pl.when(k == 1)
        def _():
            dhm_copy.start()
        return carry
    loads[8].wait()
    lax.fori_loop(0, T // TT, mlp_tokens, 0)

    loads[7].wait()
    dhm_copy.wait_recv()
    dha_copy.wait_recv()
    pair_s[0] = jnp.zeros_like(pair_s[0])
    wide = pair_s.shape[2]

    def norm_back(k, carry):
        at = pl.ds(pl.multiple_of(k * SMALL, SMALL), SMALL)
        norm, rstd = normed(x[at, :])
        da = (dha_s[1, at, :].astype(F32) + dha_in[at, :].astype(F32)).astype(BF16).astype(F32)
        dm = (dhm_s[1, at, :].astype(F32) + dhm_in[at, :].astype(F32)).astype(BF16).astype(F32)
        g = da * row_of(ln_ref, 0) + dm * row_of(ln_ref, 2)
        mean_g = lane_mean(g)
        mean_gn = lane_mean(g * norm)
        residual = dy[pl.ds(pl.multiple_of(own + k * SMALL, SMALL), SMALL), :].astype(F32)
        gx_s[at, :] = (residual + rstd * (g - mean_g - norm * mean_gn)).astype(BF16)
        for row, value in enumerate((da * norm, da, dm * norm, dm)):
            total = jnp.sum(value, axis=0, keepdims=True)
            for side in range(2):
                pair_s[0, pl.ds(2 * row + side, 1), :] += total[:, side * wide:(side + 1) * wide]
        return carry

    steps = HALF // SMALL

    def norm_step(k, carry):
        run_at(k, DURING_NORMS)
        return norm_back(k, carry)
    lax.fori_loop(0, steps, norm_step, 0)
    pair_copy.start()
    gx_copy = pltpu.make_async_copy(gx_s, gx_ref, load.at[9])
    gx_copy.start()

    def ring_copies(phase):
        place = ring_place(AXES[phase])
        return [send_to(ring_chip(AXES[phase], ahead), ring_s.at[phase, place], ring_s.at[phase, place],
                        ring_send.at[phase, ahead], ring_recv.at[phase, ahead]) for ahead in (1, 2, 3)]

    def ring_start(phase, value):
        ring_s[phase, ring_place(AXES[phase])] = value
        for copy in ring_copies(phase):
            copy.start()

    def ring_sum(phase):
        for copy in ring_copies(phase):
            copy.wait_recv()
        return ring_s[phase, 0] + ring_s[phase, 1] + ring_s[phase, 2] + ring_s[phase, 3]

    for n, events in enumerate(AFTER_NORMS):
        run(events)
        if n == 0:
            pair_copy.wait_recv()
            ring_start(0, pair_s[0] + pair_s[1])
        elif n < len(AXES):
            ring_start(n, ring_sum(n - 1))
    pair_copy.wait_send()
    pair_s[0] = ring_sum(2)
    for row in range(gln_ref.shape[0]):
        for side in range(2):
            gln_ref[pl.ds(row, 1), pl.ds(side * wide, wide)] = row_of(pair_s.at[0], 2 * row + side)
    for one in sums.values():
        one.drain()
    gx_copy.wait()
    for copy in (dhm_copy, dha_copy):
        copy.wait_send()
    for phase in range(3):
        for copy in ring_copies(phase):
            copy.wait_send()


def tail(ha_t, dqkv_t, ctx_t, dy, wqkv_t, x, wup, dh, ln):
    D, C = ha_t.shape[0], ctx_t.shape[0]
    S, V = jax.ShapeDtypeStruct, pltpu.VMEM
    hbm, vmem = pl.BlockSpec(memory_space=pl.ANY), pl.BlockSpec(memory_space=pltpu.VMEM)
    own = V((HALF, D), BF16)
    chips = (RING,) * 3
    dma = pltpu.SemaphoreType.DMA
    return pl.pallas_call(
        tail_kernel,
        in_specs=[hbm] * 8 + [vmem],
        out_specs=[hbm] + [vmem] * 3,
        out_shape=[S((HALF, D), BF16), S(ln.shape, F32), S((D // 64, 3, C // HEAD, HEAD), F32), S((C // 64, D), F32)],
        scratch_shapes=[own] + [V(a.shape, BF16) for a in (ha_t, dqkv_t, ctx_t, dy, wqkv_t, x, wup)] + [V((2, HALF, D), BF16), own] * 2
        + [V(chips + (D // 64, 3 * C), F32), V(chips + (C // 64, D), F32), V((2, 8, D // 2), F32), V((3, RING, 8, D // 2), F32)]
        + [dma((10,)), dma((2,)), dma((3,)), dma((3,)), dma((3, RING)), dma((3, RING))] + plan_scratch((PLAN_QKV, PLAN_OUT), True),
        compiler_params=pltpu.CompilerParams(vmem_limit_bytes=VMEM_LIMIT, collective_id=1, has_side_effects=True),
        name="tail",
    )(ha_t, dqkv_t, ctx_t, dy, wqkv_t, x, wup, dh, ln)


def output_kernel(*refs):
    ins, outs = refs[:len(refs) // 2], refs[len(refs) // 2:]
    outs[0][:] = ins[0][:]

    @pl.when(pl.program_id(0) == 0)
    def _():
        for src, dst in zip(ins[1:], outs[1:]):
            dst[:] = src[:]


def outputs(grad_x, *rest):
    steps = 2

    def fixed(a):
        return pl.BlockSpec(a.shape, lambda i: (0,) * len(a.shape), pipeline_mode=pl.Buffered(1))

    specs = [pl.BlockSpec((grad_x.shape[0] // steps, grad_x.shape[1]), lambda i: (i, 0))] + [fixed(a) for a in rest]
    return pl.pallas_call(
        output_kernel, grid=(steps,), in_specs=specs, out_specs=specs,
        out_shape=[jax.ShapeDtypeStruct(a.shape, a.dtype) for a in (grad_x, *rest)],
        compiler_params=pltpu.CompilerParams(dimension_semantics=("arbitrary",)),
        name="outputs",
    )(grad_x, *rest)


def solution(mesh):
    def local_step(x_loc, dy_loc, ln_params, w_qkv, w_out, w_up, w_down):
        x_loc, dy_loc = x_loc[0], dy_loc[0]
        wqkv_t = w_qkv.transpose(1, 2, 3, 0).reshape(-1, x_loc.shape[1])
        ha_t, dctx_t, dh, cos_t, sin_t, dy, g_wup, g_wdown = token_part(x_loc, dy_loc, ln_params, w_out, w_up, w_down)
        dqkv_t, ctx_t, grad_wup, grad_wdown = attention(ha_t, wqkv_t, dctx_t, cos_t, sin_t, g_wup, g_wdown)
        grad_x, grad_ln, grad_wqkv, grad_wout = tail(ha_t, dqkv_t, ctx_t, dy, wqkv_t, x_loc, w_up, dh, ln_params)
        grad_x, grad_ln, grad_wqkv, *rest = outputs(grad_x, grad_ln, grad_wqkv, grad_wout, grad_wup, grad_wdown)
        return grad_x[None], grad_ln, grad_wqkv.swapaxes(1, 2), *rest

    act_spec = P('dp', 'tp')
    in_specs = (act_spec, act_spec, P(), P(None, 'tp'), P('tp'), P(None, 'tp'), P('tp'))
    out_specs = (act_spec, P(), P('dp', 'tp'), P(('tp', 'dp')), P('dp', 'tp'), P(('tp', 'dp')))
    return jax.shard_map(local_step, mesh=mesh, in_specs=in_specs, out_specs=out_specs, check_vma=False)
```
